32 devices in a mesh: lon: 16 (over z, x, core), lat: 2 (over y).
Axes of the slice: x: 2, y: 2, z: 4, core: 2. Of those that a mesh axis runs over, the one named last changes fastest.
Arguments:
- zonal_state: float32 [4, 32, 3, 8, 2048], P(None, None, None, 'lat', 'lon'), may hold values from -6 to 6
- zonal_courant: float32 [32, 8, 2048], P(None, 'lat', 'lon'), may hold values from -0.5 to 0.5
- zonal_length: int32 [8], P('lat'), may hold values from 512 to 2048, as said below
- zonal_owner: int32 [8, 2048], P('lat', 'lon'), may hold values from 0 to 63, as said below
- merid_state: float32 [4, 32, 3, 64, 256], P(None, None, None, 'lon', 'lat'), may hold values from -6 to 6
- merid_courant: float32 [32, 64, 256], P(None, 'lon', 'lat'), may hold values from -0.5 to 0.5
- mixing: float32 [4, 32, 32], replicated, may hold values from -0.18 to 0.18
Outputs:
- zonal_next: float32 [4, 32, 3, 8, 2048], P(None, None, None, 'lat', 'lon')
- merid_next: float32 [4, 32, 3, 64, 256], P(None, None, None, 'lon', 'lat')
- coupling: float32 [64, 8, 128], P('lon', 'lat')
The draws below stay inside these ranges and needn't reach their ends.
Inputs may be any that keep to these rules, and one draw needn't show every extreme that they name: `zonal_owner`: non-decreasing along each row; each GCM column holds 16 to 48 consecutive cells of a row, and cell x belongs to a column g with |g - x // 32| <= 1. `zonal_length`: in each latitude sector (aligned blocks of 4 cycles) the first cycle holds 1088 cells and the second 2048.
All inputs are finite; a program needn't handle non-finite values.
Results may differ from the reference program's by a relative error of at most 0.0003.
Values sent between devices are 32-bit elements; how exact they have to be, the bound alone decides.
A program may use at most 64 MiB of HBM per device.

```python
import jax
import jax.numpy as jnp
from jax import lax

NV = 4
LEV = 32
WID = 3
SUB = 4
ZROWS_DEV = 4
CELLS_DEV = 128
GLON_DEV = 4
ZROWS = 8
ZCELLS = 2048
GLON = 64
MCOLS = 64
MY = 256


def draw_zonal_length(key, part):
    lengths = jax.random.randint(jax.random.fold_in(key, 5), (ZROWS,), ZCELLS // 4, ZCELLS + 1).astype(jnp.int32)
    rows = jnp.arange(ZROWS, dtype=jnp.int32)
    opposite = ZCELLS // 2 + CELLS_DEV // 2
    lengths = jnp.where(rows % ZROWS_DEV == 0, opposite, lengths)
    lengths = jnp.where(rows % ZROWS_DEV == 1, ZCELLS, lengths)
    return lengths.astype(jnp.int32)


def draw_zonal_owner(key, part):
    share = CELLS_DEV // GLON_DEV
    half = share // 2
    pairs = (GLON - 2) // 2
    shifts = jax.random.randint(jax.random.fold_in(key, 11), (ZROWS, pairs), -half, half + 1).astype(jnp.int32)
    shifts = shifts.at[0, 0].set(half)
    inner = jnp.stack([share + shifts, share - shifts], axis=-1).reshape(ZROWS, 2 * pairs)
    edge = jnp.full((ZROWS, 1), share, dtype=jnp.int32)
    widths = jnp.concatenate([edge, inner, edge], axis=1)
    ends = jnp.cumsum(widths, axis=1).astype(jnp.int32)
    cells = jnp.arange(ZCELLS, dtype=jnp.int32)

    def one_row(row_ends):
        return jnp.searchsorted(row_ends, cells, side='right').astype(jnp.int32)
    return jax.vmap(one_row)(ends).astype(jnp.int32)


def steps_of(own_key, shape, pieces, low, high):
    def one(axis_at, blocks):
        steps = jax.random.uniform(jax.random.fold_in(jax.random.fold_in(own_key, 6), axis_at), (blocks,), jnp.float32, low / len(pieces), high / len(pieces))
        return jnp.repeat(jnp.exp(steps), shape[axis_at] // blocks).reshape((-1,) + (1,) * (len(shape) - axis_at - 1))

    factor_of = one(*pieces[0])
    for cut in pieces[1:]:
        factor_of = factor_of * one(*cut)
    return factor_of


def normal_values(key, shape, deviation, bound, pieces=(), kind=jnp.bfloat16):
    entries = deviation * jax.random.normal(key, shape, jnp.float32)
    if pieces:
        entries = entries * steps_of(key, shape, pieces, -0.22, 0.18)
    return jnp.clip(entries, -bound, bound).astype(kind)


def setup_inputs(seed: int = 0) -> dict:
    key_of = jax.random.split(jax.random.key(seed), 8)
    zonal_state = normal_values(key_of[0], (NV, LEV, WID, ZROWS, ZCELLS), 1.0, 6.0, ((3, 2), (4, 16)), jnp.float32)
    zonal_courant = jnp.clip(jax.random.uniform(key_of[1], (LEV, ZROWS, ZCELLS), jnp.float32, -0.5, 0.5) * steps_of(key_of[1], (LEV, ZROWS, ZCELLS), ((1, 2), (2, 16)), -0.4, 0.0), -0.5, 0.5)
    zonal_length = draw_zonal_length(jax.random.fold_in(key_of[7], 71), 0)
    zonal_owner = draw_zonal_owner(jax.random.fold_in(key_of[7], 71), 0)
    merid_state = normal_values(key_of[4], (NV, LEV, WID, MCOLS, MY), 1.0, 6.0, ((3, 16), (4, 2)), jnp.float32)
    merid_courant = jnp.clip(jax.random.uniform(key_of[5], (LEV, MCOLS, MY), jnp.float32, -0.5, 0.5) * steps_of(key_of[5], (LEV, MCOLS, MY), ((1, 16), (2, 2)), -0.4, 0.0), -0.5, 0.5)
    mixing = normal_values(key_of[6], (NV, LEV, LEV), 0.03, 0.18, (), jnp.float32)
    return dict(zonal_state=zonal_state, zonal_courant=zonal_courant, zonal_length=zonal_length, zonal_owner=zonal_owner, merid_state=merid_state, merid_courant=merid_courant, mixing=mixing)


diffuse_along = 0.3
diffuse_across = 0.1


def across_terms(field_now):
    plus_side = jnp.concatenate([field_now[:, :, 1:], field_now[:, :, 2:3]], axis=2)
    minus_side = jnp.concatenate([field_now[:, :, 0:1], field_now[:, :, :2]], axis=2)
    return diffuse_across * (plus_side + minus_side - 2.0 * field_now)


def tendency(field_now, forward_side, backward_side, courant, mixing):
    vertical = jnp.einsum("vkj,vjwrx->vkwrx", mixing, field_now, precision=lax.Precision.HIGHEST)
    advect = -0.5 * courant * (forward_side - backward_side)
    spread = diffuse_along * (forward_side - 2.0 * field_now + backward_side)
    return advect + spread + across_terms(field_now) + vertical


def reference(zonal_state, zonal_courant, zonal_length, zonal_owner, merid_state, merid_courant, mixing):
    cells = jnp.arange(ZCELLS, dtype=jnp.int32)
    at_tail = cells[None, :] == (zonal_length[:, None] - 1)
    at_head = cells[None, :] == 0
    active = cells[None, :] < zonal_length[:, None]
    zonal_now = zonal_state
    for substep in range(SUB):
        head_cell = zonal_now[..., 0:1]
        tail_cell = jnp.sum(jnp.where(at_tail, zonal_now, 0.0), axis=-1, keepdims=True)
        forward_side = jnp.where(at_tail, head_cell, jnp.roll(zonal_now, -1, axis=-1))
        backward_side = jnp.where(at_head, tail_cell, jnp.roll(zonal_now, 1, axis=-1))
        change = tendency(zonal_now, forward_side, backward_side, zonal_courant[:, None], mixing)
        zonal_now = jnp.where(active, zonal_now + change, zonal_now)
    merid_now = merid_state
    half_turn = MCOLS // 2
    for substep in range(SUB):
        north_edge = jnp.roll(merid_now[:, :, ::-1, :, -1:], -half_turn, axis=3)
        south_edge = jnp.roll(merid_now[:, :, ::-1, :, 0:1], -half_turn, axis=3)
        forward_side = jnp.concatenate([merid_now[..., 1:], north_edge], axis=-1)
        backward_side = jnp.concatenate([south_edge, merid_now[..., :-1]], axis=-1)
        merid_now = merid_now + tendency(merid_now, forward_side, backward_side, merid_courant[:, None], mixing)
    scale = GLON_DEV / (3.0 * CELLS_DEV)
    change_sum = jnp.sum(zonal_now - zonal_state, axis=2) * scale
    flat = change_sum.reshape(NV * LEV, ZROWS, ZCELLS)
    columns = jnp.arange(GLON, dtype=jnp.int32)

    def one_row(paired):
        owner_row, change_row = paired
        onehot = (owner_row[:, None] == columns[None, :]).astype(jnp.float32)
        return jnp.einsum("xg,jx->gj", onehot, change_row, precision=lax.Precision.HIGHEST)

    rows_out = lax.map(one_row, (zonal_owner, jnp.moveaxis(flat, 1, 0)))
    coupling = jnp.transpose(rows_out, (1, 0, 2))
    return zonal_now, merid_now, coupling
```

```python
import functools

import jax
import jax.numpy as jnp
from jax import lax
from jax.experimental import pallas as pl
from jax.experimental.pallas import tpu as pltpu
from jax.sharding import PartitionSpec as P

SUB = 4
GLON_DEV = 4
PAD = 8
MESH = pl.DeviceIdType.MESH
F32 = jnp.float32


def mix_into(products, at, fields, weights):
    wide = jnp.concatenate(fields, axis=0)
    high = wide.astype(jnp.bfloat16)
    low = (wide - high.astype(F32)).astype(jnp.bfloat16)
    out = jnp.dot(jnp.concatenate([high, low], axis=1), weights[...], preferred_element_type=F32)
    half = out.shape[1] // 2
    products[pl.ds(at, wide.shape[0]), :] = out[:, :half] + out[:, half:]


def updated(now, ahead, behind, courant, product):
    c_ahead = 0.3 - 0.5 * courant
    c_behind = 0.3 + 0.5 * courant
    x0, x1, x2 = now
    local = (0.3 * x0 + 0.1 * x1, 0.2 * x1 + 0.1 * (x0 + x2), 0.3 * x2 + 0.1 * x1)
    return [
        local[w] + c_ahead * ahead[w] + c_behind * behind[w] + product[w] for w in range(3)
    ]


def advance(src, dst, courants, products, weights, cells, rows_dev, ends):
    rows = 3 * cells
    step = 32
    for r in range(rows_dev):
        mix_into(
            products,
            r * rows,
            [src[w * 4 + r, pl.ds(PAD, cells), :] for w in range(3)],
            weights,
        )
    for r in range(rows_dev):
        for at in range(0, cells, step):
            now = [src[w * 4 + r, pl.ds(PAD + at, step), :] for w in range(3)]
            ahead = [src[w * 4 + r, pl.ds(PAD + at + 1, step), :] for w in range(3)]
            behind = [src[w * 4 + r, pl.ds(PAD + at - 1, step), :] for w in range(3)]
            courant = courants[12 + r, pl.ds(PAD + at, step), :]
            product = [
                products[pl.ds(r * rows + w * cells + at, step), :] for w in range(3)
            ]
            new = updated(now, ahead, behind, courant, product)
            for w in range(3):
                value = new[w]
                if ends is not None:
                    index = at + lax.broadcasted_iota(jnp.int32, (step, 128), 0)
                    value = jnp.where(index < ends[r], value, now[w])
                dst[w * 4 + r, pl.ds(PAD + at, step), :] = value


def advance_strips(first, second, products, weights, rows_dev):
    rows = 32 * rows_dev
    step = 32
    for t in range(SUB):
        src, dst = (first, second) if t % 2 == 0 else (second, first)
        mix_into(products, 0, [src[w, pl.ds(PAD, rows), :] for w in range(3)], weights)
        for at in range(0, rows, step):
            now = [src[w, pl.ds(PAD + at, step), :] for w in range(3)]
            ahead = [src[w, pl.ds(PAD + at + 1, step), :] for w in range(3)]
            behind = [src[w, pl.ds(PAD + at - 1, step), :] for w in range(3)]
            courant = first[3, pl.ds(PAD + at, step), :]
            product = [products[pl.ds(w * rows + at, step), :] for w in range(3)]
            new = updated(now, ahead, behind, courant, product)
            for w in range(3):
                dst[w, pl.ds(PAD + at, step), :] = new[w]


def load_state(state, field, courant, cells, rows_dev):
    for r in range(rows_dev):
        for w in range(3):
            at = w * rows_dev + r
            block = field[pl.ds(at, 128, stride=3 * rows_dev), :]
            state[w * 4 + r, pl.ds(PAD, cells), :] = block.T
        levels = courant[pl.ds(r, 32, stride=rows_dev), :]
        state[12 + r, pl.ds(PAD, cells), :] = jnp.concatenate([levels] * 4, axis=0).T


def store_state(out, state, cells, rows_dev):
    for r in range(rows_dev):
        for w in range(3):
            at = w * rows_dev + r
            out[pl.ds(at, 128, stride=3 * rows_dev), :] = state[w * 4 + r, pl.ds(PAD, cells), :].T


def pack_ends(first, last, state, cells, rows_dev):
    for r in range(rows_dev):
        for ch in range(4):
            put = pl.ds((r % 2) * 4, 4)
            first[r // 2, ch, put, :] = state[ch * 4 + r, pl.ds(PAD, 4), :]
            last[r // 2, ch, put, :] = state[ch * 4 + r, pl.ds(PAD + cells - 4, 4), :]


def kernel(
    n, n_lat, cells, rows_dev,
    len_hbm, z_hbm, zc_hbm, own_hbm, m_hbm, mc_hbm, mix_hbm,
    zs2, mo, co_ref,
    len_ref, z_ref, zc_ref, own_ref, m_ref, mc_ref, mix_ref, in_sems,
    zs, zs1, ms, ms1, ms2, mh, mh1, zh, zh1, products, weights,
    z_first, z_last, z_tail, m_first, m_last,
    from_left, from_right, heads, tails_in, tail_zero, m_halo, head_rows,
    c_left, c_right, c_from_left, c_from_right,
    sends, recvs, tail_sends, tail_recvs, head_sends,
    hello_next, hello_merid, hello_far,
):
    me = lax.axis_index("lon")
    lat = lax.axis_index("lat")
    right, left = lax.rem(me + 1, n), lax.rem(me + n - 1, n)
    partner = lax.rem(me + n // 2, n)
    wrap_from = n // 4 - 1
    mid = n // 2
    last = n - 1
    start = me * cells
    loads = [
        pltpu.make_async_copy(src, dst, in_sems.at[i])
        for i, (src, dst) in enumerate(
            (
                (z_hbm, z_ref), (zc_hbm, zc_ref), (len_hbm, len_ref), (m_hbm, m_ref),
                (mc_hbm, mc_ref), (mix_hbm, mix_ref), (own_hbm, own_ref),
            )
        )
    ]
    for load in loads:
        load.start()
    barrier = pltpu.get_barrier_semaphore()

    def greet(lon_to, lat_to):
        pl.semaphore_signal(barrier, inc=1, device_id=(lon_to, lat_to), device_id_type=MESH)

    def hello(semaphore, lon_to, lat_to):
        pl.semaphore_signal(semaphore, inc=1, device_id=(lon_to, lat_to), device_id_type=MESH)

    at_south, at_north = lat == 0, lat == n_lat - 1
    south_lon = jnp.where(at_south, partner, me)
    south_lat = jnp.where(at_south, 0, lat - 1)
    north_lon = jnp.where(at_north, partner, me)
    north_lat = jnp.where(at_north, n_lat - 1, lat + 1)
    south_slot = jnp.where(at_south, 0, 1)
    north_slot = jnp.where(at_north, 1, 0)
    is_hub, is_far, has_left, has_right = me == 0, me >= wrap_from, me > 0, me < last
    south_later = jnp.logical_and(at_south, me < mid)
    north_later = jnp.logical_or(jnp.logical_not(at_north), me < mid)
    south_earlier, north_earlier = jnp.logical_not(south_later), jnp.logical_not(north_later)

    @pl.when(has_right)
    def _():
        greet(right, lat)

    @pl.when(south_later)
    def _():
        greet(south_lon, south_lat)

    @pl.when(north_later)
    def _():
        greet(north_lon, north_lat)

    @pl.when(is_hub)
    def _():
        for j in range(wrap_from, n):
            greet(j, lat)

    one = lambda flag: jnp.where(flag, 1, 0)
    peers = one(has_left) + one(south_earlier) + one(north_earlier) + one(is_far)

    @pl.when(peers > 0)
    def _():
        pl.semaphore_wait(barrier, peers)

    @pl.when(is_far)
    def _():
        hello(hello_far.at[me], 0, lat)

    @pl.when(has_left)
    def _():
        hello(hello_next.at[0], left, lat)

    @pl.when(south_earlier)
    def _():
        hello(hello_merid.at[south_slot], south_lon, south_lat)

    @pl.when(north_earlier)
    def _():
        hello(hello_merid.at[north_slot], north_lon, north_lat)

    for load in loads[:3]:
        load.wait()
    load_state(zs, z_ref, zc_ref, cells, rows_dev)
    pack_ends(z_first, z_last, zs, cells, rows_dev)
    lengths = [len_ref[r] for r in range(rows_dev)]
    index8 = lax.broadcasted_iota(jnp.int32, (8, 128), 0)
    for r in range(rows_dev):
        at = jnp.clip(lengths[r] - 4 - start, -4, cells)
        cell = lengths[r] - 4 - start + index8
        own = (cell >= 0) & (cell < cells)
        for ch in range(4):
            value = zs[ch * 4 + r, pl.ds(PAD + at, 8), :]
            z_tail[r // 2, ch, pl.ds((r % 2) * 4, 4), :] = jnp.where(own, value, 0.0)[:4]

    def copy(src, dst, send, recv, lon_to, lat_to):
        return pltpu.make_async_remote_copy(
            src_ref=src, dst_ref=dst, send_sem=send, recv_sem=recv,
            device_id=(lon_to, lat_to), device_id_type=MESH,
        )

    def head_copy(j):
        return copy(z_first.at[1], heads.at[1], head_sends.at[j], recvs.at[4], j, lat)

    head_mid = copy(z_first.at[0], heads.at[0], sends.at[5], recvs.at[5], mid, lat)
    head_last = copy(z_first.at[0], from_right.at[0], sends.at[8], recvs.at[9], last, lat)
    tail_mid = copy(z_tail.at[0], tail_zero, sends.at[5], recvs.at[6], 0, lat)
    tail_last = copy(z_last.at[0], from_left.at[0], sends.at[8], recvs.at[9], 0, lat)

    def tail_copy(j):
        return copy(z_tail.at[1], tails_in.at[j], sends.at[4], tail_recvs.at[j], 0, lat)

    to_right = copy(z_last, from_left, sends.at[0], recvs.at[0], right, lat)
    to_left = copy(z_first, from_right, sends.at[1], recvs.at[1], left, lat)

    @pl.when(is_far)
    def _():
        tail_copy(me).start()

    @pl.when(me == mid)
    def _():
        tail_mid.start()

    @pl.when(me == last)
    def _():
        tail_last.start()

    @pl.when(has_left)
    def _():
        to_left.start()

    for load in loads[3:]:
        load.wait()
    load_state(ms, m_ref, mc_ref, cells, rows_dev)
    pack_ends(m_first, m_last, ms, cells, rows_dev)
    to_south = copy(
        m_first, m_halo.at[south_slot], sends.at[2], recvs.at[2 + south_slot], south_lon, south_lat
    )
    to_north = copy(
        m_last, m_halo.at[north_slot], sends.at[3], recvs.at[2 + north_slot], north_lon, north_lat
    )

    @pl.when(south_earlier)
    def _():
        to_south.start()

    @pl.when(north_earlier)
    def _():
        to_north.start()

    tiled = jnp.concatenate([mix_ref[...]] * 4, axis=1)
    block_of = lambda axis: lax.broadcasted_iota(jnp.int32, (128, 128), axis) // 32
    matrix = jnp.where(block_of(0) == block_of(1), tiled, 0.0).T
    w_high = matrix.astype(jnp.bfloat16)
    w_low = (matrix - w_high.astype(F32)).astype(jnp.bfloat16)
    pair = jnp.concatenate([w_high, w_low], axis=1)
    weights[pl.ds(0, 128), :] = pair
    weights[pl.ds(128, 128), :] = pair
    for buf in (zh, zh1, mh, mh1):
        for ch in range(3):
            buf[ch, pl.ds(0, 8), :] = jnp.zeros((8, 128), F32)
            buf[ch, pl.ds(PAD + 32 * rows_dev, 8), :] = jnp.zeros((8, 128), F32)

    @pl.when(has_right)
    def _():
        pl.semaphore_wait(hello_next.at[0], 1)
        to_right.start()

    def serve(low, high):
        @pl.when(is_hub)
        def _():
            for j in range(max(low, wrap_from), high):
                pl.semaphore_wait(hello_far.at[j], 1)
                head_copy(j).start()
                if j == mid:
                    head_mid.start()
                if j == last:
                    head_last.start()

    ends = [jnp.clip(lengths[r] - start, 0, cells) for r in range(rows_dev)]
    for src, dst in ((zs, zs1), (zs1, zs2), (zs2, zs1), (zs1, zs2)):
        advance(src, dst, zs, products, weights, cells, rows_dev, ends)
    serve(0, mid)

    @pl.when(north_later)
    def _():
        pl.semaphore_wait(hello_merid.at[1], 1)
        to_north.start()

    @pl.when(south_later)
    def _():
        pl.semaphore_wait(hello_merid.at[0], 1)
        to_south.start()

    for src, dst in ((ms, ms1), (ms1, ms2)):
        advance(src, dst, ms, products, weights, cells, rows_dev, None)
    serve(mid, mid + n // 4)
    for src, dst in ((ms2, ms1), (ms1, ms2)):
        advance(src, dst, ms, products, weights, cells, rows_dev, None)
    serve(mid + n // 4, n)

    copy(m_first, m_halo.at[0], sends.at[2], recvs.at[2], south_lon, south_lat).wait()
    copy(m_last, m_halo.at[1], sends.at[3], recvs.at[3], north_lon, north_lat).wait()
    for r in range(rows_dev):
        take = (r % 2) * 4
        for ch in range(4):
            turned = ch if ch == 3 else 2 - ch
            sign = -1.0 if ch == 3 else 1.0
            base = PAD + r * 32
            for j in range(4):
                plain = m_halo[0, r // 2, ch, pl.ds(take + j, 1), :]
                pole = sign * m_halo[0, r // 2, turned, pl.ds(take + 3 - j, 1), :]
                mh[ch, pl.ds(base + j, 1), :] = jnp.where(at_south, pole, plain)
                plain = m_halo[1, r // 2, ch, pl.ds(take + j, 1), :]
                pole = sign * m_halo[1, r // 2, turned, pl.ds(take + 3 - j, 1), :]
                mh[ch, pl.ds(base + 24 + j, 1), :] = jnp.where(at_north, pole, plain)
            mh[ch, pl.ds(base + 4, 12), :] = ms[ch * 4 + r, pl.ds(PAD, 12), :]
            mh[ch, pl.ds(base + 16, 8), :] = ms[ch * 4 + r, pl.ds(PAD + cells - 8, 8), :]
            mh[ch, pl.ds(base + 28, 4), :] = jnp.zeros((4, 128), F32)
    advance_strips(mh, mh1, products, weights, rows_dev)
    for r in range(rows_dev):
        for w in range(3):
            at, base = w * 4 + r, PAD + r * 32
            ms2[at, pl.ds(PAD, 4), :] = mh[w, pl.ds(base + 4, 4), :]
            ms2[at, pl.ds(PAD + cells - 4, 4), :] = mh[w, pl.ds(base + 20, 4), :]
    store_state(mo, ms2, cells, rows_dev)

    @pl.when(has_right)
    def _():
        to_right.wait_send()
        to_left_of_right = copy(z_first, from_right, sends.at[1], recvs.at[1], left, lat)
        to_left_of_right.wait_recv()

    @pl.when(has_left)
    def _():
        to_left.wait_send()
        to_right.wait_recv()

    @pl.when(is_far)
    def _():
        tail_copy(me).wait_send()
        head_copy(me).wait_recv()

    @pl.when(me == mid)
    def _():
        tail_mid.wait_send()
        head_mid.wait_recv()

    @pl.when(me == last)
    def _():
        tail_last.wait_send()
        head_last.wait_recv()

    @pl.when(is_hub)
    def _():
        for j in range(wrap_from, n):
            head_copy(j).wait_send()
            tail_copy(j).wait_recv()
        head_mid.wait_send()
        tail_mid.wait_recv()
        head_last.wait_send()
        tail_last.wait_recv()

    for r in range(rows_dev):
        take = pl.ds((r % 2) * 4, 4)
        for ch in range(4):
            zs[ch * 4 + r, pl.ds(PAD - 4, 4), :] = from_left[r // 2, ch, take, :]
            zs[ch * 4 + r, pl.ds(PAD + cells, 4), :] = from_right[r // 2, ch, take, :]

    @pl.when(is_hub)
    def _():
        for ch in range(4):
            zs[ch * 4, pl.ds(PAD - 4, 4), :] = tail_zero[ch, pl.ds(0, 4), :]
            total = tails_in[wrap_from, ch]
            for j in range(wrap_from + 1, n):
                total = total + tails_in[j, ch]
            for r in range(2, rows_dev):
                zs[ch * 4 + r, pl.ds(PAD - 4, 4), :] = total[(r % 2) * 4 : (r % 2) * 4 + 4]

    index16 = lax.broadcasted_iota(jnp.int32, (16, 128), 0)
    for r in range(rows_dev):
        room = lengths[r] - start
        end = ends[r]
        over = jnp.clip(room - cells, 0, 5)
        short = jnp.clip(room, 0, 12)
        for ch in range(4):
            upper = zs[ch * 4 + r, pl.ds(PAD + end - 8, 16), :]
            lower = zs[ch * 4 + r, pl.ds(PAD - 4, 16), :]
            if r != 1:
                head_rows[r, ch, pl.ds(16, 4), :] = heads[r // 2, ch, pl.ds((r % 2) * 4, 4), :]
                upper = jnp.where(
                    index16 - 8 >= over, head_rows[r, ch, pl.ds(8 - over, 16), :], upper
                )
                lower = jnp.where(
                    index16 - 4 >= short, head_rows[r, ch, pl.ds(12 - short, 16), :], lower
                )
            zh[ch, pl.ds(PAD + r * 32, 16), :] = lower
            zh[ch, pl.ds(PAD + r * 32 + 16, 16), :] = upper
    advance_strips(zh, zh1, products, weights, rows_dev)
    index4 = lax.broadcasted_iota(jnp.int32, (4, 128), 0)
    for r in range(rows_dev):
        base = PAD + r * 32
        for w in range(3):
            at = w * 4 + r
            low = zs2[at, pl.ds(PAD, 4), :]
            zs2[at, pl.ds(PAD, 4), :] = jnp.where(
                index4 < ends[r], zh[w, pl.ds(base + 4, 4), :], low
            )
        for block in range(0, cells, 8):
            ahead = block - ends[r]
            inside = (index8 + ahead >= -4) & (index8 + ahead < 0)
            take = base + 16 + jnp.clip(ahead + 8, -8, 8)
            for w in range(3):
                at = w * 4 + r
                high = zs2[at, pl.ds(PAD + block, 8), :]
                zs2[at, pl.ds(PAD + block, 8), :] = jnp.where(
                    inside, zh[w, pl.ds(take, 8), :], high
                )

    scale = GLON_DEV / (3.0 * cells)
    near = me * GLON_DEV - 1 + lax.broadcasted_iota(jnp.int32, (8, cells), 0)
    for r in range(rows_dev):
        body = pl.ds(PAD, cells)
        before = zs[r, body, :] + zs[4 + r, body, :] + zs[8 + r, body, :]
        after = zs2[r, body, :] + zs2[4 + r, body, :] + zs2[8 + r, body, :]
        delta = (after - before) * scale
        table = (own_ref[pl.ds(r, 1), :] == near).astype(F32)
        terms = jnp.dot(
            table, delta, precision=lax.Precision.HIGHEST, preferred_element_type=F32
        )
        c_left[pl.ds(r, 1), :] = terms[0:1]
        c_right[pl.ds(r, 1), :] = terms[GLON_DEV + 1 : GLON_DEV + 2]
        for g in range(GLON_DEV):
            co_ref[g, pl.ds(r, 1), :] = terms[g + 1 : g + 2]
    part_left = copy(c_left, c_from_right, sends.at[6], recvs.at[7], left, lat)
    part_right = copy(c_right, c_from_left, sends.at[7], recvs.at[8], right, lat)

    @pl.when(has_left)
    def _():
        part_left.start()

    @pl.when(has_right)
    def _():
        part_right.start()

    @pl.when(has_left)
    def _():
        part_left.wait_send()
        part_right.wait_recv()
        for r in range(rows_dev):
            co_ref[0, pl.ds(r, 1), :] += c_from_left[pl.ds(r, 1), :]

    @pl.when(has_right)
    def _():
        part_right.wait_send()
        part_left.wait_recv()
        for r in range(rows_dev):
            co_ref[GLON_DEV - 1, pl.ds(r, 1), :] += c_from_right[pl.ds(r, 1), :]


def finish(
    cells, rows_dev,
    zs, mo, co_in,
    zo_hbm, mo_hbm, co_hbm,
    zo, sems,
):
    mo_copy = pltpu.make_async_copy(mo, mo_hbm, sems.at[1])
    mo_copy.start()
    co_copy = pltpu.make_async_copy(co_in, co_hbm, sems.at[2])
    co_copy.start()
    store_state(zo, zs, cells, rows_dev)
    zo_copy = pltpu.make_async_copy(zo, zo_hbm, sems.at[0])
    zo_copy.start()
    mo_copy.wait()
    co_copy.wait()
    zo_copy.wait()


def solution(mesh):
    n, n_lat = mesh.shape["lon"], mesh.shape["lat"]

    def shards(
        zonal_state, zonal_courant, zonal_length, zonal_owner, merid_state, merid_courant, mixing
    ):
        nv, lev, wid, rows_dev, cells = zonal_state.shape
        flat = nv * lev * wid * rows_dev
        vmem = pl.BlockSpec(memory_space=pltpu.VMEM)
        hbm = pl.BlockSpec(memory_space=pltpu.HBM)
        shape = jax.ShapeDtypeStruct
        state = (16, cells + 2 * PAD, 128)
        strips = (4, 32 * rows_dev + 2 * PAD, 128)
        packet = pltpu.VMEM((2, 4, 8, 128), F32)
        small = pltpu.VMEM((8, 128), F32)
        products = pltpu.VMEM((rows_dev * 3 * cells, 128), F32)
        dma = pltpu.SemaphoreType.DMA
        regular = pltpu.SemaphoreType.REGULAR
        held = pl.pallas_call(
            functools.partial(kernel, n, n_lat, cells, rows_dev),
            out_shape=(
                shape(state, F32), shape((flat, cells), F32),
                shape((GLON_DEV, rows_dev, nv * lev), F32),
            ),
            in_specs=[hbm] * 7,
            out_specs=(vmem,) * 3,
            scratch_shapes=[
                pltpu.SMEM((rows_dev,), jnp.int32),
                pltpu.VMEM((flat, cells), F32),
                pltpu.VMEM((lev * rows_dev, cells), F32),
                pltpu.VMEM((rows_dev, cells), jnp.int32),
                pltpu.VMEM((flat, cells), F32),
                pltpu.VMEM((lev * rows_dev, cells), F32),
                pltpu.VMEM((nv * lev, lev), F32),
                dma((7,)),
                pltpu.VMEM(state, F32), pltpu.VMEM(state, F32),
                pltpu.VMEM(state, F32), pltpu.VMEM(state, F32), pltpu.VMEM(state, F32),
                pltpu.VMEM(strips, F32), pltpu.VMEM(strips, F32),
                pltpu.VMEM(strips, F32), pltpu.VMEM(strips, F32),
                products, pltpu.VMEM((256, 256), jnp.bfloat16),
                packet, packet, packet, packet, packet,
                packet, packet, packet,
                pltpu.VMEM((n, 4, 8, 128), F32),
                pltpu.VMEM((4, 8, 128), F32),
                pltpu.VMEM((2, 2, 4, 8, 128), F32),
                pltpu.VMEM((rows_dev, 4, 40, 128), F32),
                small, small, small, small,
                dma((9,)), dma((10,)), dma((1,)), dma((n,)), dma((n,)),
                regular((1,)), regular((2,)), regular((n,)),
            ],
            compiler_params=pltpu.CompilerParams(
                collective_id=0, has_side_effects=True, vmem_limit_bytes=48 * 1024 * 1024
            ),
        )(
            *(
                pltpu.with_memory_space_constraint(value, pltpu.HBM)
                for value in (
                    zonal_length,
                    zonal_state.reshape(flat, cells),
                    zonal_courant.reshape(lev * rows_dev, cells),
                    zonal_owner,
                    merid_state.reshape(flat, cells),
                    merid_courant.reshape(lev * rows_dev, cells),
                    mixing.reshape(nv * lev, lev),
                )
            )
        )
        zo, mo, co = pl.pallas_call(
            functools.partial(finish, cells, rows_dev),
            out_shape=(
                shape((flat, cells), F32), shape((flat, cells), F32),
                shape((GLON_DEV, rows_dev, nv * lev), F32),
            ),
            in_specs=[vmem] * 3,
            out_specs=(hbm,) * 3,
            scratch_shapes=[pltpu.VMEM((flat, cells), F32), dma((3,))],
            compiler_params=pltpu.CompilerParams(vmem_limit_bytes=40 * 1024 * 1024),
        )(*held)
        return zo.reshape(zonal_state.shape), mo.reshape(merid_state.shape), co

    return jax.shard_map(
        shards,
        mesh=mesh,
        in_specs=(
            P(None, None, None, "lat", "lon"),
            P(None, "lat", "lon"),
            P("lat"),
            P("lat", "lon"),
            P(None, None, None, "lon", "lat"),
            P(None, "lon", "lat"),
            P(),
        ),
        out_specs=(
            P(None, None, None, "lat", "lon"),
            P(None, None, None, "lon", "lat"),
            P("lon", "lat", None),
        ),
        check_vma=False,
    )
```

```python
import functools

import jax
import jax.numpy as jnp
from jax import lax
from jax.experimental import pallas as pl
from jax.experimental.pallas import tpu as pltpu
from jax.sharding import PartitionSpec as P

SUB = 4
GLON_DEV = 4
PAD = 8
STEP = 32
UNSCALE = 10.0**-SUB
MESH = pl.DeviceIdType.MESH
F32 = jnp.float32


def mix_into(products, at, fields, weights):
    wide = jnp.concatenate(fields, axis=0)
    high = wide.astype(jnp.bfloat16)
    low = (wide - high.astype(F32)).astype(jnp.bfloat16)
    out = jnp.dot(jnp.concatenate([high, low], axis=1), weights[...], preferred_element_type=F32)
    half = out.shape[1] // 2
    products[pl.ds(at, wide.shape[0]), :] = out[:, :half] + out[:, half:]


def updated(now, ahead, behind, five, product):
    c_ahead = 3.0 - five
    c_behind = 3.0 + five
    x0, x1, x2 = now
    pairs = (x0 + x1, x0 + x2, x1 + x2)
    return [
        (pairs[w] + product[w]) + (c_ahead * ahead[w] + c_behind * behind[w]) for w in range(3)
    ]


def advance(src, dst, fives, products, weights, cells, rows_dev, ends, final=False):
    rows = 3 * cells
    step = STEP
    for r in range(rows_dev):
        mix_into(
            products,
            r * rows,
            [src[w * 4 + r, pl.ds(PAD, cells), :] for w in range(3)],
            weights,
        )
    for r in range(rows_dev):
        for at in range(0, cells, step):
            now = [src[w * 4 + r, pl.ds(PAD + at, step), :] for w in range(3)]
            ahead = [src[w * 4 + r, pl.ds(PAD + at + 1, step), :] for w in range(3)]
            behind = [src[w * 4 + r, pl.ds(PAD + at - 1, step), :] for w in range(3)]
            five = fives[12 + r, pl.ds(PAD + at, step), :]
            product = [
                products[pl.ds(r * rows + w * cells + at, step), :] for w in range(3)
            ]
            new = updated(now, ahead, behind, five, product)
            for w in range(3):
                value = new[w] * UNSCALE if final else new[w]
                if ends is not None:
                    index = at + lax.broadcasted_iota(jnp.int32, (step, 128), 0)
                    kept = fives[w * 4 + r, pl.ds(PAD + at, step), :]
                    value = jnp.where(index < ends[r], value, kept)
                dst[w * 4 + r, pl.ds(PAD + at, step), :] = value


def advance_strips(first, second, products, weights, rows_dev):
    rows = 32 * rows_dev
    step = STEP
    for t in range(SUB):
        src, dst = (first, second) if t % 2 == 0 else (second, first)
        mix_into(products, 0, [src[w, pl.ds(PAD, rows), :] for w in range(3)], weights)
        for at in range(0, rows, step):
            now = [src[w, pl.ds(PAD + at, step), :] for w in range(3)]
            ahead = [src[w, pl.ds(PAD + at + 1, step), :] for w in range(3)]
            behind = [src[w, pl.ds(PAD + at - 1, step), :] for w in range(3)]
            five = first[3, pl.ds(PAD + at, step), :]
            product = [products[pl.ds(w * rows + at, step), :] for w in range(3)]
            new = updated(now, ahead, behind, five, product)
            for w in range(3):
                dst[w, pl.ds(PAD + at, step), :] = new[w] * UNSCALE if t == SUB - 1 else new[w]


def load_state(state, field, courant, cells, rows_dev):
    for r in range(rows_dev):
        for w in range(3):
            at = w * rows_dev + r
            block = field[pl.ds(at, 128, stride=3 * rows_dev), :]
            state[w * 4 + r, pl.ds(PAD, cells), :] = block.T
        levels = courant[pl.ds(r, 32, stride=rows_dev), :]
        state[12 + r, pl.ds(PAD, cells), :] = jnp.concatenate([5.0 * levels] * 4, axis=0).T


def store_state(out, state, cells, rows_dev):
    for r in range(rows_dev):
        for w in range(3):
            at = w * rows_dev + r
            out[pl.ds(at, 128, stride=3 * rows_dev), :] = state[w * 4 + r, pl.ds(PAD, cells), :].T


def pack_ends(first, last, state, cells, rows_dev):
    for r in range(rows_dev):
        for ch in range(4):
            put = pl.ds((r % 2) * 4, 4)
            first[r // 2, ch, put, :] = state[ch * 4 + r, pl.ds(PAD, 4), :]
            last[r // 2, ch, put, :] = state[ch * 4 + r, pl.ds(PAD + cells - 4, 4), :]


def kernel(
    n, n_lat, cells, rows_dev,
    len_hbm, z_hbm, zc_hbm, own_hbm, m_hbm, mc_hbm, mix_hbm,
    zo, mo, co_ref,
    len_ref, z_ref, zc_ref, own_ref, m_ref, mc_ref, mix_ref, in_sems,
    zs, zs1, zs2, ms, ms1, ms2, mh, mh1, zh, zh1, products, weights,
    z_first, z_last, z_tail, m_first, m_last,
    from_left, from_right, heads, tails_in, tail_zero, m_halo, head_rows,
    c_left, c_right, c_from_left, c_from_right,
    sends, recvs, tail_recvs, head_sends,
    hello_side, hello_merid, hello_far,
):
    me = lax.axis_index("lon")
    lat = lax.axis_index("lat")
    right, left = lax.rem(me + 1, n), lax.rem(me + n - 1, n)
    partner = lax.rem(me + n // 2, n)
    wrap_from = n // 4 - 1
    mid = n // 2
    last = n - 1
    start = me * cells
    loads = [
        pltpu.make_async_copy(src, dst, in_sems.at[i])
        for i, (src, dst) in enumerate(
            (
                (z_hbm, z_ref), (zc_hbm, zc_ref), (len_hbm, len_ref), (m_hbm, m_ref),
                (mc_hbm, mc_ref), (mix_hbm, mix_ref), (own_hbm, own_ref),
            )
        )
    ]
    for load in loads:
        load.start()
    barrier = pltpu.get_barrier_semaphore()

    def greet(lon_to, lat_to):
        pl.semaphore_signal(barrier, inc=1, device_id=(lon_to, lat_to), device_id_type=MESH)

    def hello(semaphore, lon_to, lat_to):
        pl.semaphore_signal(semaphore, inc=1, device_id=(lon_to, lat_to), device_id_type=MESH)

    at_south, at_north = lat == 0, lat == n_lat - 1
    south_lon = jnp.where(at_south, partner, me)
    south_lat = jnp.where(at_south, 0, lat - 1)
    north_lon = jnp.where(at_north, partner, me)
    north_lat = jnp.where(at_north, n_lat - 1, lat + 1)
    south_slot = jnp.where(at_south, 0, 1)
    north_slot = jnp.where(at_north, 1, 0)
    is_hub, is_far, has_left, has_right = me == 0, me >= wrap_from, me > 0, me < last
    south_later = jnp.logical_and(at_south, me < mid)
    north_later = jnp.logical_or(jnp.logical_not(at_north), me < mid)
    south_earlier, north_earlier = jnp.logical_not(south_later), jnp.logical_not(north_later)

    odd = lax.rem(me, 2) == 1
    even = lax.rem(me, 2) == 0
    right_later, right_earlier = has_right & odd, has_right & even
    left_later, left_earlier = has_left & odd, has_left & even

    @pl.when(right_later)
    def _():
        greet(right, lat)

    @pl.when(left_later)
    def _():
        greet(left, lat)

    @pl.when(south_later)
    def _():
        greet(south_lon, south_lat)

    @pl.when(north_later)
    def _():
        greet(north_lon, north_lat)

    @pl.when(is_hub)
    def _():
        for j in range(wrap_from, n):
            greet(j, lat)

    one = lambda flag: jnp.where(flag, 1, 0)
    peers = (
        one(left_earlier) + one(right_earlier)
        + one(south_earlier) + one(north_earlier) + one(is_far)
    )

    @pl.when(peers > 0)
    def _():
        pl.semaphore_wait(barrier, peers)

    @pl.when(is_far)
    def _():
        hello(hello_far.at[lax.div(me, n // 4)], 0, lat)

    @pl.when(left_earlier)
    def _():
        hello(hello_side.at[1], left, lat)

    @pl.when(right_earlier)
    def _():
        hello(hello_side.at[0], right, lat)

    @pl.when(south_earlier)
    def _():
        hello(hello_merid.at[south_slot], south_lon, south_lat)

    @pl.when(north_earlier)
    def _():
        hello(hello_merid.at[north_slot], north_lon, north_lat)

    for load in loads[:3]:
        load.wait()
    load_state(zs, z_ref, zc_ref, cells, rows_dev)
    pack_ends(z_first, z_last, zs, cells, rows_dev)
    lengths = [len_ref[r] for r in range(rows_dev)]
    index8 = lax.broadcasted_iota(jnp.int32, (8, 128), 0)
    for r in range(rows_dev):
        at = jnp.clip(lengths[r] - 4 - start, -4, cells)
        cell = lengths[r] - 4 - start + index8
        own = (cell >= 0) & (cell < cells)
        for ch in range(4):
            value = zs[ch * 4 + r, pl.ds(PAD + at, 8), :]
            z_tail[r // 2, ch, pl.ds((r % 2) * 4, 4), :] = jnp.where(own, value, 0.0)[:4]

    def copy(src, dst, send, recv, lon_to, lat_to):
        return pltpu.make_async_remote_copy(
            src_ref=src, dst_ref=dst, send_sem=send, recv_sem=recv,
            device_id=(lon_to, lat_to), device_id_type=MESH,
        )

    def head_copy(j):
        return copy(z_first.at[1], heads.at[1], head_sends.at[0], recvs.at[4], j, lat)

    head_mid = copy(z_first.at[0], heads.at[0], sends.at[5], recvs.at[5], mid, lat)
    head_last = copy(z_first.at[0], from_right.at[0], sends.at[8], recvs.at[9], last, lat)
    tail_mid = copy(z_tail.at[0], tail_zero, sends.at[5], recvs.at[6], 0, lat)
    tail_last = copy(z_last.at[0], from_left.at[0], sends.at[8], recvs.at[9], 0, lat)

    def tail_copy(j):
        return copy(z_tail.at[1], tails_in.at[j], sends.at[4], tail_recvs.at[0], 0, lat)

    to_right = copy(z_last, from_left, sends.at[0], recvs.at[0], right, lat)
    to_left = copy(z_first, from_right, sends.at[1], recvs.at[1], left, lat)

    farthest = me >= last - n // 4 + 1

    @pl.when(farthest)
    def _():
        tail_copy(me).start()

    @pl.when(me == last)
    def _():
        tail_last.start()

    @pl.when(left_earlier)
    def _():
        to_left.start()

    @pl.when(right_earlier)
    def _():
        to_right.start()

    for load in loads[3:]:
        load.wait()
    load_state(ms, m_ref, mc_ref, cells, rows_dev)
    pack_ends(m_first, m_last, ms, cells, rows_dev)
    to_south = copy(
        m_first, m_halo.at[south_slot], sends.at[2], recvs.at[2 + south_slot], south_lon, south_lat
    )
    to_north = copy(
        m_last, m_halo.at[north_slot], sends.at[3], recvs.at[2 + north_slot], north_lon, north_lat
    )

    @pl.when(south_earlier)
    def _():
        to_south.start()

    @pl.when(north_earlier)
    def _():
        to_north.start()

    @pl.when(is_far & jnp.logical_not(farthest))
    def _():
        tail_copy(me).start()

    @pl.when(me == mid)
    def _():
        tail_mid.start()

    tiled = jnp.concatenate([mix_ref[...]] * 4, axis=1)
    index_of = lambda axis: lax.broadcasted_iota(jnp.int32, (128, 128), axis)
    block_of = lambda axis: index_of(axis) // 32
    matrix = jnp.where(block_of(0) == block_of(1), tiled, 0.0).T
    matrix = 10.0 * matrix + jnp.where(index_of(0) == index_of(1), 2.0, 0.0)
    w_high = matrix.astype(jnp.bfloat16)
    w_low = (matrix - w_high.astype(F32)).astype(jnp.bfloat16)
    pair = jnp.concatenate([w_high, w_low], axis=1)
    weights[pl.ds(0, 128), :] = pair
    weights[pl.ds(128, 128), :] = pair
    for slot in range(16):
        zs[slot, pl.ds(0, PAD), :] = jnp.zeros((PAD, 128), F32)
    for buf in (zh, zh1, mh, mh1):
        for ch in range(3):
            buf[ch, pl.ds(0, 8), :] = jnp.zeros((8, 128), F32)
            buf[ch, pl.ds(PAD + 32 * rows_dev, 8), :] = jnp.zeros((8, 128), F32)

    @pl.when(left_later)
    def _():
        pl.semaphore_wait(hello_side.at[0], 1)
        to_left.start()

    @pl.when(right_later)
    def _():
        pl.semaphore_wait(hello_side.at[1], 1)
        to_right.start()

    quarter = n // 4

    def serve(group, now):
        targets = [j for j in range(quarter * group, quarter * (group + 1)) if j >= wrap_from]

        @pl.when(is_hub & now)
        def _():
            pl.semaphore_wait(hello_far.at[group], len(targets))
            for j in targets[::2] + targets[1::2]:
                head_copy(j).start()
                if j == mid:
                    head_mid.start()
                if j == last:
                    head_last.start()

    ends = [jnp.clip(lengths[r] - start, 0, cells) for r in range(rows_dev)]
    for src, dst in ((zs, zs1), (zs1, zs2), (zs2, zs1)):
        advance(src, dst, zs, products, weights, cells, rows_dev, None)
    advance(zs1, zs2, zs, products, weights, cells, rows_dev, ends, final=True)
    always = me >= 0
    serve(0, always)
    serve(1, always)
    serve(2, lat > 0)

    def turn_poles():
        @pl.when(north_later)
        def _():
            pl.semaphore_wait(hello_merid.at[1], 1)
            to_north.start()

        @pl.when(south_later)
        def _():
            pl.semaphore_wait(hello_merid.at[0], 1)
            to_south.start()

    @pl.when(me > 1)
    def _():
        turn_poles()

    for src, dst in ((ms, ms1), (ms1, ms2)):
        advance(src, dst, ms, products, weights, cells, rows_dev, None)
    @pl.when(me <= 1)
    def _():
        turn_poles()

    serve(2, at_south)
    serve(3, lat > 0)
    for src, dst in ((ms2, ms1), (ms1, ms2)):
        advance(src, dst, ms, products, weights, cells, rows_dev, None, final=dst is ms2)
    serve(3, at_south)

    def fill_left():
        for r in range(rows_dev):
            take = pl.ds((r % 2) * 4, 4)
            for ch in range(4):
                zs[ch * 4 + r, pl.ds(PAD - 4, 4), :] = from_left[r // 2, ch, take, :]

    def fill_right():
        for r in range(rows_dev):
            take = pl.ds((r % 2) * 4, 4)
            for ch in range(4):
                zs[ch * 4 + r, pl.ds(PAD + cells, 4), :] = from_right[r // 2, ch, take, :]

    index16 = lax.broadcasted_iota(jnp.int32, (16, 128), 0)
    index4 = lax.broadcasted_iota(jnp.int32, (4, 128), 0)

    def seams():
        for r in range(rows_dev):
            room = lengths[r] - start
            end = ends[r]
            over = jnp.clip(room - cells, 0, 5)
            short = jnp.clip(room, 0, 12)
            for ch in range(4):
                upper = zs[ch * 4 + r, pl.ds(PAD + end - 8, 16), :]
                lower = zs[ch * 4 + r, pl.ds(PAD - 4, 16), :]
                if r != 1:
                    head_rows[r, ch, pl.ds(16, 4), :] = heads[
                        r // 2, ch, pl.ds((r % 2) * 4, 4), :
                    ]
                    upper = jnp.where(
                        index16 - 8 >= over, head_rows[r, ch, pl.ds(8 - over, 16), :], upper
                    )
                    lower = jnp.where(
                        index16 - 4 >= short, head_rows[r, ch, pl.ds(12 - short, 16), :], lower
                    )
                zh[ch, pl.ds(PAD + r * 32, 16), :] = lower
                zh[ch, pl.ds(PAD + r * 32 + 16, 16), :] = upper
        advance_strips(zh, zh1, products, weights, rows_dev)
        for r in range(rows_dev):
            base = PAD + r * 32
            for w in range(3):
                at = w * 4 + r
                low = zs2[at, pl.ds(PAD, 4), :]
                zs2[at, pl.ds(PAD, 4), :] = jnp.where(
                    index4 < ends[r], zh[w, pl.ds(base + 4, 4), :], low
                )
            for block in range(0, cells, 8):
                ahead = block - ends[r]
                inside = (index8 + ahead >= -4) & (index8 + ahead < 0)
                take = base + 16 + jnp.clip(ahead + 8, -8, 8)
                for w in range(3):
                    at = w * 4 + r
                    high = zs2[at, pl.ds(PAD + block, 8), :]
                    zs2[at, pl.ds(PAD + block, 8), :] = jnp.where(
                        inside, zh[w, pl.ds(take, 8), :], high
                    )

    scale = GLON_DEV / (3.0 * cells)
    near = me * GLON_DEV - 1 + lax.broadcasted_iota(jnp.int32, (8, cells), 0)

    def column_terms(r):
        body = pl.ds(PAD, cells)
        before = zs[r, body, :] + zs[4 + r, body, :] + zs[8 + r, body, :]
        after = zs2[r, body, :] + zs2[4 + r, body, :] + zs2[8 + r, body, :]
        delta = (after - before) * scale
        high = delta.astype(jnp.bfloat16)
        low = (delta - high.astype(F32)).astype(jnp.bfloat16)
        table = (own_ref[pl.ds(r, 1), :] == near).astype(jnp.bfloat16)
        both = jnp.dot(
            table, jnp.concatenate([high, low], axis=1), preferred_element_type=F32
        )
        half = both.shape[1] // 2
        return both[:, :half] + both[:, half:]

    part_left = copy(c_left, c_from_right, sends.at[6], recvs.at[7], left, lat)
    part_right = copy(c_right, c_from_left, sends.at[7], recvs.at[8], right, lat)

    @pl.when(has_right)
    def _():
        to_right.wait_send()
        to_left.wait_recv()

    @pl.when(has_left)
    def _():
        to_left.wait_send()
        to_right.wait_recv()

    @pl.when(is_far)
    def _():
        tail_copy(me).wait_send()
        head_copy(me).wait_recv()

    @pl.when(me == mid)
    def _():
        tail_mid.wait_send()
        head_mid.wait_recv()

    @pl.when(me == last)
    def _():
        tail_last.wait_send()
        head_last.wait_recv()

    @pl.when(has_left)
    def _():
        fill_left()

    fill_right()
    seams()
    for r in range(rows_dev):
        terms = column_terms(r)
        c_left[pl.ds(r, 1), :] = terms[0:1]
        c_right[pl.ds(r, 1), :] = terms[GLON_DEV + 1 : GLON_DEV + 2]
        for g in range(GLON_DEV):
            co_ref[g, pl.ds(r, 1), :] = terms[g + 1 : g + 2]

    @pl.when(has_left)
    def _():
        part_left.start()

    @pl.when(has_right)
    def _():
        part_right.start()

    @pl.when(has_left)
    def _():
        store_state(zo, zs2, cells, rows_dev)

    copy(m_first, m_halo.at[0], sends.at[2], recvs.at[2], south_lon, south_lat).wait()
    copy(m_last, m_halo.at[1], sends.at[3], recvs.at[3], north_lon, north_lat).wait()
    for r in range(rows_dev):
        take = (r % 2) * 4
        for ch in range(4):
            turned = ch if ch == 3 else 2 - ch
            sign = -1.0 if ch == 3 else 1.0
            base = PAD + r * 32
            for j in range(4):
                plain = m_halo[0, r // 2, ch, pl.ds(take + j, 1), :]
                pole = sign * m_halo[0, r // 2, turned, pl.ds(take + 3 - j, 1), :]
                mh[ch, pl.ds(base + j, 1), :] = jnp.where(at_south, pole, plain)
                plain = m_halo[1, r // 2, ch, pl.ds(take + j, 1), :]
                pole = sign * m_halo[1, r // 2, turned, pl.ds(take + 3 - j, 1), :]
                mh[ch, pl.ds(base + 24 + j, 1), :] = jnp.where(at_north, pole, plain)
            mh[ch, pl.ds(base + 4, 12), :] = ms[ch * 4 + r, pl.ds(PAD, 12), :]
            mh[ch, pl.ds(base + 16, 8), :] = ms[ch * 4 + r, pl.ds(PAD + cells - 8, 8), :]
            mh[ch, pl.ds(base + 28, 4), :] = jnp.zeros((4, 128), F32)
    advance_strips(mh, mh1, products, weights, rows_dev)
    for r in range(rows_dev):
        for w in range(3):
            at, base = w * 4 + r, PAD + r * 32
            ms2[at, pl.ds(PAD, 4), :] = mh[w, pl.ds(base + 4, 4), :]
            ms2[at, pl.ds(PAD + cells - 4, 4), :] = mh[w, pl.ds(base + 20, 4), :]
    store_state(mo, ms2, cells, rows_dev)

    @pl.when(is_hub)
    def _():
        every = tails_in.at[pl.ds(wrap_from, n - wrap_from)]
        all_far = copy(every, every, head_sends.at[0], tail_recvs.at[0], last, lat)
        all_far.wait_send()
        all_far.wait_recv()
        head_mid.wait_send()
        tail_mid.wait_recv()
        head_last.wait_send()
        tail_last.wait_recv()
        fill_left()
        for ch in range(4):
            zs[ch * 4, pl.ds(PAD - 4, 4), :] = tail_zero[ch, pl.ds(0, 4), :]
            total = tails_in[wrap_from, ch]
            for j in range(wrap_from + 1, n):
                total = total + tails_in[j, ch]
            for r in range(2, rows_dev):
                zs[ch * 4 + r, pl.ds(PAD - 4, 4), :] = total[(r % 2) * 4 : (r % 2) * 4 + 4]
        seams()
        for r in range(rows_dev):
            terms = column_terms(r)
            for g in range(GLON_DEV):
                co_ref[g, pl.ds(r, 1), :] = terms[g + 1 : g + 2]
        store_state(zo, zs2, cells, rows_dev)

    @pl.when(has_left)
    def _():
        part_left.wait_send()
        part_right.wait_recv()
        for r in range(rows_dev):
            co_ref[0, pl.ds(r, 1), :] += c_from_left[pl.ds(r, 1), :]

    @pl.when(has_right)
    def _():
        part_right.wait_send()
        part_left.wait_recv()
        for r in range(rows_dev):
            co_ref[GLON_DEV - 1, pl.ds(r, 1), :] += c_from_right[pl.ds(r, 1), :]


def finish(zo, mo, co, zo_hbm, mo_hbm, co_hbm, sems):
    copies = [
        pltpu.make_async_copy(src, dst, sems.at[i])
        for i, (src, dst) in enumerate(((zo, zo_hbm), (mo, mo_hbm), (co, co_hbm)))
    ]
    for out in copies:
        out.start()
    for out in copies:
        out.wait()


def solution(mesh):
    n, n_lat = mesh.shape["lon"], mesh.shape["lat"]

    def shards(
        zonal_state, zonal_courant, zonal_length, zonal_owner, merid_state, merid_courant, mixing
    ):
        nv, lev, wid, rows_dev, cells = zonal_state.shape
        flat = nv * lev * wid * rows_dev
        vmem = pl.BlockSpec(memory_space=pltpu.VMEM)
        hbm = pl.BlockSpec(memory_space=pltpu.HBM)
        shape = jax.ShapeDtypeStruct
        state = (16, cells + 2 * PAD, 128)
        strips = (4, 32 * rows_dev + 2 * PAD, 128)
        packet = pltpu.VMEM((2, 4, 8, 128), F32)
        small = pltpu.VMEM((8, 128), F32)
        products = pltpu.VMEM((rows_dev * 3 * cells, 128), F32)
        dma = pltpu.SemaphoreType.DMA
        regular = pltpu.SemaphoreType.REGULAR
        held = pl.pallas_call(
            functools.partial(kernel, n, n_lat, cells, rows_dev),
            out_shape=(
                shape((flat, cells), F32), shape((flat, cells), F32),
                shape((GLON_DEV, rows_dev, nv * lev), F32),
            ),
            in_specs=[hbm] * 7,
            out_specs=(vmem,) * 3,
            scratch_shapes=[
                pltpu.SMEM((rows_dev,), jnp.int32),
                pltpu.VMEM((flat, cells), F32),
                pltpu.VMEM((lev * rows_dev, cells), F32),
                pltpu.VMEM((rows_dev, cells), jnp.int32),
                pltpu.VMEM((flat, cells), F32),
                pltpu.VMEM((lev * rows_dev, cells), F32),
                pltpu.VMEM((nv * lev, lev), F32),
                dma((7,)),
                pltpu.VMEM(state, F32), pltpu.VMEM(state, F32), pltpu.VMEM(state, F32),
                pltpu.VMEM(state, F32), pltpu.VMEM(state, F32), pltpu.VMEM(state, F32),
                pltpu.VMEM(strips, F32), pltpu.VMEM(strips, F32),
                pltpu.VMEM(strips, F32), pltpu.VMEM(strips, F32),
                products, pltpu.VMEM((256, 256), jnp.bfloat16),
                packet, packet, packet, packet, packet,
                packet, packet, packet,
                pltpu.VMEM((n, 4, 8, 128), F32),
                pltpu.VMEM((4, 8, 128), F32),
                pltpu.VMEM((2, 2, 4, 8, 128), F32),
                pltpu.VMEM((rows_dev, 4, 40, 128), F32),
                small, small, small, small,
                dma((9,)), dma((10,)), dma((1,)), dma((1,)),
                regular((2,)), regular((2,)), regular((4,)),
            ],
            compiler_params=pltpu.CompilerParams(
                collective_id=0, has_side_effects=True, vmem_limit_bytes=48 * 1024 * 1024
            ),
        )(
            *(
                pltpu.with_memory_space_constraint(value, pltpu.HBM)
                for value in (
                    zonal_length,
                    zonal_state.reshape(flat, cells),
                    zonal_courant.reshape(lev * rows_dev, cells),
                    zonal_owner,
                    merid_state.reshape(flat, cells),
                    merid_courant.reshape(lev * rows_dev, cells),
                    mixing.reshape(nv * lev, lev),
                )
            )
        )
        zo, mo, co = pl.pallas_call(
            finish,
            out_shape=(
                shape((flat, cells), F32), shape((flat, cells), F32),
                shape((GLON_DEV, rows_dev, nv * lev), F32),
            ),
            in_specs=[vmem] * 3,
            out_specs=(hbm,) * 3,
            scratch_shapes=[dma((3,))],
            compiler_params=pltpu.CompilerParams(vmem_limit_bytes=40 * 1024 * 1024),
        )(*held)
        return zo.reshape(zonal_state.shape), mo.reshape(merid_state.shape), co

    return jax.shard_map(
        shards,
        mesh=mesh,
        in_specs=(
            P(None, None, None, "lat", "lon"),
            P(None, "lat", "lon"),
            P("lat"),
            P("lat", "lon"),
            P(None, None, None, "lon", "lat"),
            P(None, "lon", "lat"),
            P(),
        ),
        out_specs=(
            P(None, None, None, "lat", "lon"),
            P(None, None, None, "lon", "lat"),
            P("lon", "lat", None),
        ),
        check_vma=False,
    )
```

```python
import functools

import jax
import jax.numpy as jnp
from jax import lax
from jax.experimental import pallas as pl
from jax.experimental.pallas import tpu as pltpu
from jax.sharding import PartitionSpec as P

SUB = 4
GLON_DEV = 4
PAD = 8
STEP = 32
UNSCALE = 10.0**-SUB
MESH = pl.DeviceIdType.MESH
F32 = jnp.float32


def mix_into(products, at, fields, weights):
    wide = jnp.concatenate(fields, axis=0)
    high = wide.astype(jnp.bfloat16)
    low = (wide - high.astype(F32)).astype(jnp.bfloat16)
    out = jnp.dot(jnp.concatenate([high, low], axis=1), weights[...], preferred_element_type=F32)
    half = out.shape[1] // 2
    products[pl.ds(at, wide.shape[0]), :] = out[:, :half] + out[:, half:]


def updated(now, ahead, behind, five, product):
    c_ahead = 3.0 - five
    c_behind = 3.0 + five
    x0, x1, x2 = now
    pairs = (x0 + x1, x0 + x2, x1 + x2)
    return [
        (pairs[w] + product[w]) + (c_ahead * ahead[w] + c_behind * behind[w]) for w in range(3)
    ]


def advance(src, dst, fives, products, weights, cells, rows_dev, ends, final=False):
    rows = 3 * cells
    step = STEP
    for r in range(rows_dev):
        mix_into(
            products,
            r * rows,
            [src[w * 4 + r, pl.ds(PAD, cells), :] for w in range(3)],
            weights,
        )
    for r in range(rows_dev):
        for at in range(0, cells, step):
            now = [src[w * 4 + r, pl.ds(PAD + at, step), :] for w in range(3)]
            ahead = [src[w * 4 + r, pl.ds(PAD + at + 1, step), :] for w in range(3)]
            behind = [src[w * 4 + r, pl.ds(PAD + at - 1, step), :] for w in range(3)]
            five = fives[12 + r, pl.ds(PAD + at, step), :]
            product = [
                products[pl.ds(r * rows + w * cells + at, step), :] for w in range(3)
            ]
            new = updated(now, ahead, behind, five, product)
            for w in range(3):
                value = new[w] * UNSCALE if final else new[w]
                if ends is not None:
                    index = at + lax.broadcasted_iota(jnp.int32, (step, 128), 0)
                    kept = fives[w * 4 + r, pl.ds(PAD + at, step), :]
                    value = jnp.where(index < ends[r], value, kept)
                dst[w * 4 + r, pl.ds(PAD + at, step), :] = value


def advance_strips(first, second, products, weights, rows):
    step = STEP
    for t in range(SUB):
        src, dst = (first, second) if t % 2 == 0 else (second, first)
        mix_into(products, 0, [src[w, pl.ds(PAD, rows), :] for w in range(3)], weights)
        for at in range(0, rows, step):
            now = [src[w, pl.ds(PAD + at, step), :] for w in range(3)]
            ahead = [src[w, pl.ds(PAD + at + 1, step), :] for w in range(3)]
            behind = [src[w, pl.ds(PAD + at - 1, step), :] for w in range(3)]
            five = first[3, pl.ds(PAD + at, step), :]
            product = [products[pl.ds(w * rows + at, step), :] for w in range(3)]
            new = updated(now, ahead, behind, five, product)
            for w in range(3):
                dst[w, pl.ds(PAD + at, step), :] = new[w] * UNSCALE if t == SUB - 1 else new[w]


def load_state(state, field, courant, cells, rows_dev):
    for r in range(rows_dev):
        for w in range(3):
            at = w * rows_dev + r
            block = field[pl.ds(at, 128, stride=3 * rows_dev), :]
            state[w * 4 + r, pl.ds(PAD, cells), :] = block.T
        levels = courant[pl.ds(r, 32, stride=rows_dev), :]
        state[12 + r, pl.ds(PAD, cells), :] = jnp.concatenate([5.0 * levels] * 4, axis=0).T


def store_state(out, state, cells, rows_dev):
    for r in range(rows_dev):
        for w in range(3):
            at = w * rows_dev + r
            out[pl.ds(at, 128, stride=3 * rows_dev), :] = state[w * 4 + r, pl.ds(PAD, cells), :].T


def pack_ends(first, last, state, cells, rows_dev):
    for r in range(rows_dev):
        for ch in range(4):
            put = pl.ds((r % 2) * 4, 4)
            first[r // 2, ch, put, :] = state[ch * 4 + r, pl.ds(PAD, 4), :]
            last[r // 2, ch, put, :] = state[ch * 4 + r, pl.ds(PAD + cells - 4, 4), :]


def kernel(
    n, n_lat, cells, rows_dev,
    len_hbm, z_hbm, zc_hbm, own_hbm, m_hbm, mc_hbm, mix_hbm,
    zo, mo, co_ref,
    len_ref, z_ref, zc_ref, own_ref, m_ref, mc_ref, mix_ref, in_sems,
    zs, zs1, zs2, ms, ms1, ms2, fh, fh1, zh, zh1, products, weights,
    z_first, z_last, z_tail, m_first, m_last,
    from_left, from_right, heads, tails_in, tail_zero, m_halo,
    z_window, w_left, w_right, seam_owner,
    c_left, c_right, c_from_left, c_from_right,
    sends, recvs, tail_recvs, head_sends,
    hello_side, hello_merid, hello_far,
):
    me = lax.axis_index("lon")
    lat = lax.axis_index("lat")
    right, left = lax.rem(me + 1, n), lax.rem(me + n - 1, n)
    partner = lax.rem(me + n // 2, n)
    wrap_from = n // 4 - 1
    mid = n // 2
    last = n - 1
    start = me * cells
    loads = [
        pltpu.make_async_copy(src, dst, in_sems.at[i])
        for i, (src, dst) in enumerate(
            (
                (z_hbm, z_ref), (zc_hbm, zc_ref), (len_hbm, len_ref), (m_hbm, m_ref),
                (mc_hbm, mc_ref), (mix_hbm, mix_ref), (own_hbm, own_ref),
            )
        )
    ]
    for load in loads:
        load.start()
    barrier = pltpu.get_barrier_semaphore()

    def greet(lon_to, lat_to):
        pl.semaphore_signal(barrier, inc=1, device_id=(lon_to, lat_to), device_id_type=MESH)

    def hello(semaphore, lon_to, lat_to):
        pl.semaphore_signal(semaphore, inc=1, device_id=(lon_to, lat_to), device_id_type=MESH)

    at_south, at_north = lat == 0, lat == n_lat - 1
    south_lon = jnp.where(at_south, partner, me)
    south_lat = jnp.where(at_south, 0, lat - 1)
    north_lon = jnp.where(at_north, partner, me)
    north_lat = jnp.where(at_north, n_lat - 1, lat + 1)
    south_slot = jnp.where(at_south, 0, 1)
    north_slot = jnp.where(at_north, 1, 0)
    is_hub, is_far, has_left, has_right = me == 0, me >= wrap_from, me > 0, me < last
    south_later = jnp.logical_and(at_south, me < mid)
    north_later = jnp.logical_or(jnp.logical_not(at_north), me < mid)
    south_earlier, north_earlier = jnp.logical_not(south_later), jnp.logical_not(north_later)

    odd = lax.rem(me, 2) == 1
    even = lax.rem(me, 2) == 0
    right_later, right_earlier = has_right & odd, has_right & even
    left_later, left_earlier = has_left & odd, has_left & even

    @pl.when(right_later)
    def _():
        greet(right, lat)

    @pl.when(left_later)
    def _():
        greet(left, lat)

    @pl.when(south_later)
    def _():
        greet(south_lon, south_lat)

    @pl.when(north_later)
    def _():
        greet(north_lon, north_lat)

    @pl.when(is_hub)
    def _():
        for j in range(wrap_from, n):
            greet(j, lat)

    one = lambda flag: jnp.where(flag, 1, 0)
    peers = (
        one(left_earlier) + one(right_earlier)
        + one(south_earlier) + one(north_earlier) + one(is_far)
    )

    @pl.when(peers > 0)
    def _():
        pl.semaphore_wait(barrier, peers)

    @pl.when(is_far)
    def _():
        hello(hello_far.at[lax.div(me, n // 4)], 0, lat)

    @pl.when(left_earlier)
    def _():
        hello(hello_side.at[1], left, lat)

    @pl.when(right_earlier)
    def _():
        hello(hello_side.at[0], right, lat)

    @pl.when(south_earlier)
    def _():
        hello(hello_merid.at[south_slot], south_lon, south_lat)

    @pl.when(north_earlier)
    def _():
        hello(hello_merid.at[north_slot], north_lon, north_lat)

    for load in loads[:3]:
        load.wait()
    load_state(zs, z_ref, zc_ref, cells, rows_dev)
    pack_ends(z_first, z_last, zs, cells, rows_dev)
    lengths = [len_ref[r] for r in range(rows_dev)]
    index8 = lax.broadcasted_iota(jnp.int32, (8, 128), 0)
    for r in range(rows_dev):
        at = jnp.clip(lengths[r] - 4 - start, -4, cells)
        cell = lengths[r] - 4 - start + index8
        own = (cell >= 0) & (cell < cells)
        for ch in range(4):
            value = zs[ch * 4 + r, pl.ds(PAD + at, 8), :]
            z_tail[r // 2, ch, pl.ds((r % 2) * 4, 4), :] = jnp.where(own, value, 0.0)[:4]

    def copy(src, dst, send, recv, lon_to, lat_to):
        return pltpu.make_async_remote_copy(
            src_ref=src, dst_ref=dst, send_sem=send, recv_sem=recv,
            device_id=(lon_to, lat_to), device_id_type=MESH,
        )

    def head_copy(j):
        return copy(z_first.at[1], heads.at[1], head_sends.at[0], recvs.at[4], j, lat)

    head_mid = copy(z_first.at[0], heads.at[0], sends.at[5], recvs.at[5], mid, lat)
    head_last = copy(z_first.at[0], heads.at[0], sends.at[8], recvs.at[9], last, lat)
    tail_mid = copy(z_tail.at[0], tail_zero, sends.at[5], recvs.at[6], 0, lat)
    tail_last = copy(z_last.at[0], from_left.at[0], sends.at[8], recvs.at[9], 0, lat)

    def tail_copy(j):
        return copy(z_tail.at[1], tails_in.at[j], sends.at[4], tail_recvs.at[0], 0, lat)

    to_right = copy(z_last, from_left, sends.at[0], recvs.at[0], right, lat)
    to_left = copy(z_first, from_right, sends.at[1], recvs.at[1], left, lat)

    @pl.when(is_far)
    def _():
        tail_copy(me).start()

    @pl.when(me == mid)
    def _():
        tail_mid.start()

    @pl.when(me == last)
    def _():
        tail_last.start()

    @pl.when(left_earlier)
    def _():
        to_left.start()

    @pl.when(right_earlier)
    def _():
        to_right.start()

    for load in loads[3:]:
        load.wait()
    load_state(ms, m_ref, mc_ref, cells, rows_dev)
    pack_ends(m_first, m_last, ms, cells, rows_dev)
    to_south = copy(
        m_first, m_halo.at[south_slot], sends.at[2], recvs.at[2 + south_slot], south_lon, south_lat
    )
    to_north = copy(
        m_last, m_halo.at[north_slot], sends.at[3], recvs.at[2 + north_slot], north_lon, north_lat
    )

    def over_poles(some):
        @pl.when(at_south & some)
        def _():
            to_south.start()

        @pl.when(at_north & some)
        def _():
            to_north.start()

    @pl.when(jnp.logical_not(at_south))
    def _():
        to_south.start()

    over_poles((me >= mid) & (me < mid + 2))

    tiled = jnp.concatenate([mix_ref[...]] * 4, axis=1)
    index_of = lambda axis: lax.broadcasted_iota(jnp.int32, (128, 128), axis)
    block_of = lambda axis: index_of(axis) // 32
    matrix = jnp.where(block_of(0) == block_of(1), tiled, 0.0).T
    matrix = 10.0 * matrix + jnp.where(index_of(0) == index_of(1), 2.0, 0.0)
    w_high = matrix.astype(jnp.bfloat16)
    w_low = (matrix - w_high.astype(F32)).astype(jnp.bfloat16)
    pair = jnp.concatenate([w_high, w_low], axis=1)
    weights[pl.ds(0, 128), :] = pair
    weights[pl.ds(128, 128), :] = pair
    zeros = jnp.zeros((PAD, 128), F32)
    for slot in range(16):
        zs[slot, pl.ds(0, PAD), :] = zeros
        zs[slot, pl.ds(PAD + cells, PAD), :] = zeros
    for buf in (zh, zh1, fh, fh1):
        for ch in range(3):
            buf[ch, pl.ds(0, PAD), :] = zeros
            buf[ch, pl.ds(buf.shape[1] - PAD, PAD), :] = zeros

    @pl.when(left_later)
    def _():
        pl.semaphore_wait(hello_side.at[0], 1)
        to_left.start()

    @pl.when(right_later)
    def _():
        pl.semaphore_wait(hello_side.at[1], 1)
        to_right.start()

    quarter = n // 4

    def serve(group, now):
        targets = [j for j in range(quarter * group, quarter * (group + 1)) if j >= wrap_from]

        @pl.when(is_hub & now)
        def _():
            pl.semaphore_wait(hello_far.at[group], len(targets))
            for j in targets[::2] + targets[1::2]:
                head_copy(j).start()
                if j == mid:
                    head_mid.start()
                if j == last:
                    head_last.start()

    ends = [jnp.clip(lengths[r] - start, 0, cells) for r in range(rows_dev)]
    for src, dst in ((zs, zs1), (zs1, zs2), (zs2, zs1)):
        advance(src, dst, zs, products, weights, cells, rows_dev, None)
    advance(zs1, zs2, zs, products, weights, cells, rows_dev, ends, final=True)
    always = me >= 0
    serve(0, always)
    serve(1, always)
    serve(2, lat > 0)

    @pl.when(jnp.logical_not(at_north))
    def _():
        pl.semaphore_wait(hello_merid.at[1], 1)
        to_north.start()

    def ready_poles(some):
        @pl.when(at_south & some)
        def _():
            pl.semaphore_wait(hello_merid.at[0], 1)

        @pl.when(at_north & some)
        def _():
            pl.semaphore_wait(hello_merid.at[1], 1)

    ready_poles((me > 1) & (me < mid))
    over_poles((me > 1) & ((me < mid) | (me >= mid + 2)))

    for r in range(rows_dev):
        owners = (own_ref[pl.ds(r, 1), :] + 1).astype(F32)
        zs[16 + r, pl.ds(PAD, cells), :] = jnp.broadcast_to(owners, (128, cells)).T
    for r in range(rows_dev):
        at = jnp.clip(lengths[r] - 8 - start, -8, cells)
        cell = lengths[r] - 8 - start + index8
        for ch in range(5):
            value = zs[ch * 4 + r, pl.ds(PAD + at, 8), :]
            z_window[r, ch, :, :] = jnp.where((cell >= 0) & (cell < cells), value, 0.0)
    moving = z_window.at[pl.ds(2, rows_dev - 2)]
    window_left = copy(moving, w_right, sends.at[9], recvs.at[10], left, lat)
    window_right = copy(moving, w_left, sends.at[10], recvs.at[11], right, lat)

    @pl.when(has_left)
    def _():
        window_left.start()

    @pl.when(has_right)
    def _():
        window_right.start()

    for src, dst in ((ms, ms1), (ms1, ms2)):
        advance(src, dst, ms, products, weights, cells, rows_dev, None)
    serve(2, at_south)
    serve(3, lat > 0)
    for src, dst in ((ms2, ms1), (ms1, ms2)):
        advance(src, dst, ms, products, weights, cells, rows_dev, None, final=dst is ms2)
    serve(3, at_south)
    ready_poles(me <= 1)
    over_poles(me <= 1)

    def fill_left():
        for r in range(rows_dev):
            take = pl.ds((r % 2) * 4, 4)
            for ch in range(4):
                zs[ch * 4 + r, pl.ds(PAD - 4, 4), :] = from_left[r // 2, ch, take, :]

    def fill_right():
        for r in range(rows_dev):
            take = pl.ds((r % 2) * 4, 4)
            for ch in range(4):
                zs[ch * 4 + r, pl.ds(PAD + cells, 4), :] = from_right[r // 2, ch, take, :]

    index4 = lax.broadcasted_iota(jnp.int32, (4, 128), 0)

    scale = GLON_DEV / (3.0 * cells)
    near = me * GLON_DEV - 1 + lax.broadcasted_iota(jnp.int32, (8, cells), 0)
    lane = lax.broadcasted_iota(jnp.int32, (8, cells), 1)

    first_late = jnp.where(is_hub, 4, 0)

    def column_terms(r):
        body = pl.ds(PAD, cells)
        before = zs[r, body, :] + zs[4 + r, body, :] + zs[8 + r, body, :]
        after = zs2[r, body, :] + zs2[4 + r, body, :] + zs2[8 + r, body, :]
        delta = (after - before) * scale
        high = delta.astype(jnp.bfloat16)
        low = (delta - high.astype(F32)).astype(jnp.bfloat16)
        to_end = lane - (lengths[r] - start)
        early = ((to_end < -4) | (to_end >= 0)) & (lane >= first_late)
        table = ((own_ref[pl.ds(r, 1), :] == near) & early).astype(jnp.bfloat16)
        both = jnp.dot(
            table, jnp.concatenate([high, low], axis=1), preferred_element_type=F32
        )
        half = both.shape[1] // 2
        return both[:, :half] + both[:, half:]

    part_left = copy(c_left, c_from_right, sends.at[6], recvs.at[7], left, lat)
    part_right = copy(c_right, c_from_left, sends.at[7], recvs.at[8], right, lat)

    @pl.when(has_right)
    def _():
        to_right.wait_send()
        to_left.wait_recv()

    @pl.when(has_left)
    def _():
        to_left.wait_send()
        to_right.wait_recv()

    @pl.when(has_left)
    def _():
        fill_left()

    @pl.when(has_right)
    def _():
        fill_right()

    for r in range(rows_dev):
        for ch in range(4):
            base = PAD + r * 32
            zh[ch, pl.ds(base, 16), :] = zs[ch * 4 + r, pl.ds(PAD - 4, 16), :]
            zh[ch, pl.ds(base + 16, 16), :] = zs[ch * 4 + r, pl.ds(PAD + cells - 8, 16), :]
    advance_strips(zh, zh1, products, weights, 32 * rows_dev)
    for r in range(rows_dev):
        base = PAD + r * 32
        for w in range(3):
            for cell, take in ((0, base + 4), (cells - 4, base + 20)):
                old = zs2[w * 4 + r, pl.ds(PAD + cell, 4), :]
                zs2[w * 4 + r, pl.ds(PAD + cell, 4), :] = jnp.where(
                    index4 + cell < ends[r], zh[w, pl.ds(take, 4), :], old
                )
    for r in range(rows_dev):
        terms = column_terms(r)
        c_left[pl.ds(r, 1), :] = terms[0:1]
        c_right[pl.ds(r, 1), :] = terms[GLON_DEV + 1 : GLON_DEV + 2]
        for g in range(GLON_DEV):
            co_ref[g, pl.ds(r, 1), :] = terms[g + 1 : g + 2]

    @pl.when(has_left)
    def _():
        part_left.start()

    @pl.when(has_right)
    def _():
        part_right.start()

    copy(m_first, m_halo.at[0], sends.at[2], recvs.at[2], south_lon, south_lat).wait()
    copy(m_last, m_halo.at[1], sends.at[3], recvs.at[3], north_lon, north_lat).wait()

    @pl.when(is_far)
    def _():
        tail_copy(me).wait_send()
        head_copy(me).wait_recv()

    @pl.when(me == mid)
    def _():
        tail_mid.wait_send()
        head_mid.wait_recv()

    @pl.when(me == last)
    def _():
        tail_last.wait_send()
        head_last.wait_recv()

    @pl.when(has_left)
    def _():
        window_left.wait_send()
        window_right.wait_recv()

    @pl.when(has_right)
    def _():
        window_right.wait_send()
        window_left.wait_recv()

    @pl.when(is_hub)
    def _():
        every = tails_in.at[pl.ds(wrap_from, n - wrap_from)]
        all_far = copy(every, every, head_sends.at[0], tail_recvs.at[0], last, lat)
        all_far.wait_send()
        all_far.wait_recv()
        head_mid.wait_send()
        tail_mid.wait_recv()
        head_last.wait_send()
        tail_last.wait_recv()

    @pl.when(is_hub)
    def _():
        for ch in range(4):
            total = tails_in[wrap_from, ch]
            for j in range(wrap_from + 1, n):
                total = total + tails_in[j, ch]
            fh[ch, pl.ds(PAD, 4), :] = tail_zero[ch, pl.ds(0, 4), :]
            fh[ch, pl.ds(PAD + 16, 4), :] = from_left[0, ch, pl.ds(4, 4), :]
            for r in range(2, rows_dev):
                half = (r % 2) * 4
                fh[ch, pl.ds(PAD + 16 * r, 4), :] = total[half : half + 4]
            for r in range(rows_dev):
                fh[ch, pl.ds(PAD + 16 * r + 4, 12), :] = zs[ch * 4 + r, pl.ds(PAD, 12), :]
        for r in range(rows_dev):
            seam_owner[r, :, :] = zs[16 + r, pl.ds(PAD, 8), :]

    @pl.when(has_left)
    def _():
        for r in range(rows_dev):
            for ch in range(5):
                window = z_window[r, ch]
                if r >= 2:
                    window = window + w_left[r - 2, ch]
                    window = window + jnp.where(has_right, w_right[r - 2, ch], 0.0)
                if ch == 4:
                    seam_owner[r, pl.ds(0, 4), :] = window[4:8]
                    continue
                base = PAD + 16 * r
                fh[ch, pl.ds(base, 8), :] = window
                fh[ch, pl.ds(base + 8, 4), :] = heads[r // 2, ch, pl.ds((r % 2) * 4, 4), :]
                fh[ch, pl.ds(base + 12, 4), :] = jnp.zeros((4, 128), F32)

    merid = PAD + 16 * rows_dev
    for r in range(rows_dev):
        take = (r % 2) * 4
        for ch in range(4):
            turned = ch if ch == 3 else 2 - ch
            sign = -1.0 if ch == 3 else 1.0
            base = merid + r * 32
            for j in range(4):
                plain = m_halo[0, r // 2, ch, pl.ds(take + j, 1), :]
                pole = sign * m_halo[0, r // 2, turned, pl.ds(take + 3 - j, 1), :]
                fh[ch, pl.ds(base + j, 1), :] = jnp.where(at_south, pole, plain)
                plain = m_halo[1, r // 2, ch, pl.ds(take + j, 1), :]
                pole = sign * m_halo[1, r // 2, turned, pl.ds(take + 3 - j, 1), :]
                fh[ch, pl.ds(base + 24 + j, 1), :] = jnp.where(at_north, pole, plain)
            fh[ch, pl.ds(base + 4, 12), :] = ms[ch * 4 + r, pl.ds(PAD, 12), :]
            fh[ch, pl.ds(base + 16, 8), :] = ms[ch * 4 + r, pl.ds(PAD + cells - 8, 8), :]
            fh[ch, pl.ds(base + 28, 4), :] = jnp.zeros((4, 128), F32)

    def wanted(r):
        at = pl.ds(PAD + 16 * r + 4, 4)
        return fh[0, at, :] + fh[1, at, :] + fh[2, at, :]

    seam_before = [wanted(r) for r in range(rows_dev)]
    advance_strips(fh, fh1, products, weights, 48 * rows_dev)
    for r in range(rows_dev):
        for w in range(3):
            at, base = w * 4 + r, merid + r * 32
            ms2[at, pl.ds(PAD, 4), :] = fh[w, pl.ds(base + 4, 4), :]
            ms2[at, pl.ds(PAD + cells - 4, 4), :] = fh[w, pl.ds(base + 20, 4), :]
    store_state(mo, ms2, cells, rows_dev)

    @pl.when(is_hub)
    def _():
        for r in range(rows_dev):
            for w in range(3):
                zs2[w * 4 + r, pl.ds(PAD, 4), :] = fh[w, pl.ds(PAD + 16 * r + 4, 4), :]

    @pl.when(has_left)
    def _():
        for r in range(rows_dev):
            for block in range(0, cells, 8):
                ahead = block - (lengths[r] - start)
                inside = (index8 + ahead >= -4) & (index8 + ahead < 0)
                take = PAD + 16 * r + 8 + jnp.clip(ahead, -12, 0)
                for w in range(3):
                    at = w * 4 + r
                    old = zs2[at, pl.ds(PAD + block, 8), :]
                    zs2[at, pl.ds(PAD + block, 8), :] = jnp.where(
                        inside, fh[w, pl.ds(take, 8), :], old
                    )

    store_state(zo, zs2, cells, rows_dev)
    for r in range(rows_dev):
        delta = (wanted(r) - seam_before[r]) * scale
        owner = seam_owner[r, pl.ds(0, 4), :]
        for g in range(GLON_DEV):
            mine = owner == (me * GLON_DEV + g + 1).astype(F32)
            co_ref[g, pl.ds(r, 1), :] += jnp.sum(
                jnp.where(mine, delta, 0.0), axis=0, keepdims=True
            )

    @pl.when(has_left)
    def _():
        part_left.wait_send()
        part_right.wait_recv()
        for r in range(rows_dev):
            co_ref[0, pl.ds(r, 1), :] += c_from_left[pl.ds(r, 1), :]

    @pl.when(has_right)
    def _():
        part_right.wait_send()
        part_left.wait_recv()
        for r in range(rows_dev):
            co_ref[GLON_DEV - 1, pl.ds(r, 1), :] += c_from_right[pl.ds(r, 1), :]


def finish(zo, mo, co, zo_hbm, mo_hbm, co_hbm, sems):
    copies = [
        pltpu.make_async_copy(src, dst, sems.at[i])
        for i, (src, dst) in enumerate(((zo, zo_hbm), (mo, mo_hbm), (co, co_hbm)))
    ]
    for out in copies:
        out.start()
    for out in copies:
        out.wait()


def solution(mesh):
    n, n_lat = mesh.shape["lon"], mesh.shape["lat"]

    def shards(
        zonal_state, zonal_courant, zonal_length, zonal_owner, merid_state, merid_courant, mixing
    ):
        nv, lev, wid, rows_dev, cells = zonal_state.shape
        flat = nv * lev * wid * rows_dev
        vmem = pl.BlockSpec(memory_space=pltpu.VMEM)
        hbm = pl.BlockSpec(memory_space=pltpu.HBM)
        shape = jax.ShapeDtypeStruct
        state = (16, cells + 2 * PAD, 128)
        strips = (4, 32 * rows_dev + 2 * PAD, 128)
        packet = pltpu.VMEM((2, 4, 8, 128), F32)
        small = pltpu.VMEM((8, 128), F32)
        products = pltpu.VMEM((rows_dev * 3 * cells, 128), F32)
        dma = pltpu.SemaphoreType.DMA
        regular = pltpu.SemaphoreType.REGULAR
        held = pl.pallas_call(
            functools.partial(kernel, n, n_lat, cells, rows_dev),
            out_shape=(
                shape((flat, cells), F32), shape((flat, cells), F32),
                shape((GLON_DEV, rows_dev, nv * lev), F32),
            ),
            in_specs=[hbm] * 7,
            out_specs=(vmem,) * 3,
            scratch_shapes=[
                pltpu.SMEM((rows_dev,), jnp.int32),
                pltpu.VMEM((flat, cells), F32),
                pltpu.VMEM((lev * rows_dev, cells), F32),
                pltpu.VMEM((rows_dev, cells), jnp.int32),
                pltpu.VMEM((flat, cells), F32),
                pltpu.VMEM((lev * rows_dev, cells), F32),
                pltpu.VMEM((nv * lev, lev), F32),
                dma((7,)),
                pltpu.VMEM((20, *state[1:]), F32), pltpu.VMEM(state, F32),
                pltpu.VMEM(state, F32), pltpu.VMEM(state, F32), pltpu.VMEM(state, F32),
                pltpu.VMEM(state, F32),
                pltpu.VMEM((4, 48 * rows_dev + 2 * PAD, 128), F32),
                pltpu.VMEM((4, 48 * rows_dev + 2 * PAD, 128), F32),
                pltpu.VMEM(strips, F32), pltpu.VMEM(strips, F32),
                products, pltpu.VMEM((256, 256), jnp.bfloat16),
                packet, packet, packet, packet, packet,
                packet, packet, packet,
                pltpu.VMEM((n, 4, 8, 128), F32),
                pltpu.VMEM((4, 8, 128), F32),
                pltpu.VMEM((2, 2, 4, 8, 128), F32),
                pltpu.VMEM((rows_dev, 5, 8, 128), F32),
                pltpu.VMEM((rows_dev - 2, 5, 8, 128), F32),
                pltpu.VMEM((rows_dev - 2, 5, 8, 128), F32),
                pltpu.VMEM((rows_dev, 8, 128), F32),
                small, small, small, small,
                dma((11,)), dma((12,)), dma((1,)), dma((1,)),
                regular((2,)), regular((2,)), regular((4,)),
            ],
            compiler_params=pltpu.CompilerParams(
                collective_id=0, has_side_effects=True, vmem_limit_bytes=48 * 1024 * 1024
            ),
        )(
            *(
                pltpu.with_memory_space_constraint(value, pltpu.HBM)
                for value in (
                    zonal_length,
                    zonal_state.reshape(flat, cells),
                    zonal_courant.reshape(lev * rows_dev, cells),
                    zonal_owner,
                    merid_state.reshape(flat, cells),
                    merid_courant.reshape(lev * rows_dev, cells),
                    mixing.reshape(nv * lev, lev),
                )
            )
        )
        zo, mo, co = pl.pallas_call(
            finish,
            out_shape=(
                shape((flat, cells), F32), shape((flat, cells), F32),
                shape((GLON_DEV, rows_dev, nv * lev), F32),
            ),
            in_specs=[vmem] * 3,
            out_specs=(hbm,) * 3,
            scratch_shapes=[dma((3,))],
            compiler_params=pltpu.CompilerParams(vmem_limit_bytes=40 * 1024 * 1024),
        )(*held)
        return zo.reshape(zonal_state.shape), mo.reshape(merid_state.shape), co

    return jax.shard_map(
        shards,
        mesh=mesh,
        in_specs=(
            P(None, None, None, "lat", "lon"),
            P(None, "lat", "lon"),
            P("lat"),
            P("lat", "lon"),
            P(None, None, None, "lon", "lat"),
            P(None, "lon", "lat"),
            P(),
        ),
        out_specs=(
            P(None, None, None, "lat", "lon"),
            P(None, None, None, "lon", "lat"),
            P("lon", "lat", None),
        ),
        check_vma=False,
    )
```

```python
import functools

import jax
import jax.numpy as jnp
from jax import lax
from jax.experimental import pallas as pl
from jax.experimental.pallas import tpu as pltpu
from jax.sharding import PartitionSpec as P

SUB = 4
GLON_DEV = 4
PAD = 8
STEP = 32
UNSCALE = 10.0**-SUB
MESH = pl.DeviceIdType.MESH
LEFT, RIGHT, MERID, TAIL, HEAD = range(5)
NEAR, PART, WINDOW = 0, 1, 5
F32 = jnp.float32


def mix_into(products, at, fields, weights):
    wide = jnp.concatenate(fields, axis=0)
    high = wide.astype(jnp.bfloat16)
    low = (wide - high.astype(F32)).astype(jnp.bfloat16)
    out = jnp.dot(jnp.concatenate([high, low], axis=1), weights[...], preferred_element_type=F32)
    half = out.shape[1] // 2
    products[pl.ds(at, wide.shape[0]), :] = out[:, :half] + out[:, half:]


def updated(now, ahead, behind, five, product):
    c_ahead = 3.0 - five
    c_behind = 3.0 + five
    x0, x1, x2 = now
    pairs = (x0 + x1, x0 + x2, x1 + x2)
    return [
        (pairs[w] + product[w]) + (c_ahead * ahead[w] + c_behind * behind[w]) for w in range(3)
    ]


def advance(src, dst, fives, products, weights, cells, rows_dev, ends, final=False):
    rows = 3 * cells
    step = STEP
    for r in range(rows_dev):
        mix_into(
            products,
            r * rows,
            [src[w * 4 + r, pl.ds(PAD, cells), :] for w in range(3)],
            weights,
        )
    for r in range(rows_dev):
        for at in range(0, cells, step):
            now = [src[w * 4 + r, pl.ds(PAD + at, step), :] for w in range(3)]
            ahead = [src[w * 4 + r, pl.ds(PAD + at + 1, step), :] for w in range(3)]
            behind = [src[w * 4 + r, pl.ds(PAD + at - 1, step), :] for w in range(3)]
            five = fives[12 + r, pl.ds(PAD + at, step), :]
            product = [
                products[pl.ds(r * rows + w * cells + at, step), :] for w in range(3)
            ]
            new = updated(now, ahead, behind, five, product)
            for w in range(3):
                value = new[w] * UNSCALE if final else new[w]
                if ends is not None:
                    index = at + lax.broadcasted_iota(jnp.int32, (step, 128), 0)
                    kept = fives[w * 4 + r, pl.ds(PAD + at, step), :]
                    value = jnp.where(index < ends[r], value, kept)
                dst[w * 4 + r, pl.ds(PAD + at, step), :] = value


def advance_strips(first, second, products, weights, rows):
    step = STEP
    for t in range(SUB):
        src, dst = (first, second) if t % 2 == 0 else (second, first)
        mix_into(products, 0, [src[w, pl.ds(PAD, rows), :] for w in range(3)], weights)
        for at in range(0, rows, step):
            now = [src[w, pl.ds(PAD + at, step), :] for w in range(3)]
            ahead = [src[w, pl.ds(PAD + at + 1, step), :] for w in range(3)]
            behind = [src[w, pl.ds(PAD + at - 1, step), :] for w in range(3)]
            five = first[3, pl.ds(PAD + at, step), :]
            product = [products[pl.ds(w * rows + at, step), :] for w in range(3)]
            new = updated(now, ahead, behind, five, product)
            for w in range(3):
                dst[w, pl.ds(PAD + at, step), :] = new[w] * UNSCALE if t == SUB - 1 else new[w]


def load_state(state, field, courant, cells, rows_dev, rows):
    for r in rows:
        for w in range(3):
            at = w * rows_dev + r
            block = field[pl.ds(at, 128, stride=3 * rows_dev), :]
            state[w * 4 + r, pl.ds(PAD, cells), :] = block.T
        levels = courant[pl.ds(r, 32, stride=rows_dev), :]
        state[12 + r, pl.ds(PAD, cells), :] = jnp.concatenate([5.0 * levels] * 4, axis=0).T


def pack_ends(first, last, state, cells, rows_dev):
    for r in range(rows_dev):
        for ch in range(4):
            put = pl.ds((r % 2) * 4, 4)
            first[r // 2, ch, put, :] = state[ch * 4 + r, pl.ds(PAD, 4), :]
            last[r // 2, ch, put, :] = state[ch * 4 + r, pl.ds(PAD + cells - 4, 4), :]


def kernel(
    n, n_lat, cells, rows_dev,
    len_hbm, z_hbm, zc_hbm, own_hbm, m_hbm, mc_hbm, mix_hbm,
    zs2, ms2, co_ref,
    len_ref, z_ref, zc_ref, own_ref, m_ref, mc_ref, mix_ref,
    zs, zs1, ms, ms1, fh, fh1, zh, zh1, products, weights,
    z_first, z_last, z_tail, m_first, m_last,
    from_left, from_right, heads, tails_in, tail_zero, m_halo,
    z_window, w_left, w_right, seam_owner,
    c_left, c_right, c_from_left, c_from_right,
    sends, recvs,
    hello_side, hello_merid, hello_far,
):
    me = lax.axis_index("lon")
    lat = lax.axis_index("lat")
    right, left = lax.rem(me + 1, n), lax.rem(me + n - 1, n)
    partner = lax.rem(me + n // 2, n)
    wrap_from = n // 4 - 1
    mid = n // 2
    last = n - 1
    start = me * cells
    halves = ((z_hbm.at[:, 1], z_ref.at[:, 1]), (z_hbm.at[:, 0], z_ref.at[:, 0]))
    loads = [
        pltpu.make_async_copy(src, dst, sends.at[sem])
        for src, dst, sem in (
            (*halves[0], LEFT), (zc_hbm, zc_ref, RIGHT), (len_hbm, len_ref, TAIL),
            (*halves[1], 5), (m_hbm, m_ref, MERID), (mc_hbm, mc_ref, HEAD),
            (mix_hbm, mix_ref, 6), (own_hbm, own_ref, 7),
        )
    ]
    for load in loads:
        load.start()
    barrier = pltpu.get_barrier_semaphore()

    def greet(lon_to, lat_to):
        pl.semaphore_signal(barrier, inc=1, device_id=(lon_to, lat_to), device_id_type=MESH)

    def hello(semaphore, lon_to, lat_to):
        pl.semaphore_signal(semaphore, inc=1, device_id=(lon_to, lat_to), device_id_type=MESH)

    at_south, at_north = lat == 0, lat == n_lat - 1
    south_lon = jnp.where(at_south, partner, me)
    south_lat = jnp.where(at_south, 0, lat - 1)
    north_lon = jnp.where(at_north, partner, me)
    north_lat = jnp.where(at_north, n_lat - 1, lat + 1)
    south_slot = jnp.where(at_south, 0, 1)
    north_slot = jnp.where(at_north, 1, 0)
    is_hub, is_far, has_left, has_right = me == 0, me >= wrap_from, me > 0, me < last
    south_later = jnp.logical_and(at_south, me < mid)
    north_later = jnp.logical_or(jnp.logical_not(at_north), me < mid)
    south_earlier, north_earlier = jnp.logical_not(south_later), jnp.logical_not(north_later)

    odd = lax.rem(me, 2) == 1
    even = lax.rem(me, 2) == 0
    right_later, right_earlier = has_right & odd, has_right & even
    left_later, left_earlier = has_left & odd, has_left & even

    @pl.when(right_later)
    def _():
        greet(right, lat)

    @pl.when(left_later)
    def _():
        greet(left, lat)

    @pl.when(south_later)
    def _():
        greet(south_lon, south_lat)

    @pl.when(north_later)
    def _():
        greet(north_lon, north_lat)

    @pl.when(is_hub)
    def _():
        for j in range(wrap_from, n):
            greet(j, lat)

    one = lambda flag: jnp.where(flag, 1, 0)
    peers = (
        one(left_earlier) + one(right_earlier)
        + one(south_earlier) + one(north_earlier) + one(is_far)
    )

    @pl.when(peers > 0)
    def _():
        pl.semaphore_wait(barrier, peers)

    @pl.when(is_far)
    def _():
        hello(hello_far.at[lax.div(me, n // 4)], 0, lat)

    @pl.when(left_earlier)
    def _():
        hello(hello_side.at[1], left, lat)

    @pl.when(right_earlier)
    def _():
        hello(hello_side.at[0], right, lat)

    @pl.when(south_earlier)
    def _():
        hello(hello_merid.at[south_slot], south_lon, south_lat)

    @pl.when(north_earlier)
    def _():
        hello(hello_merid.at[north_slot], north_lon, north_lat)

    for load in loads[:3]:
        load.wait()
    def copy(src, dst, send, recv, lon_to, lat_to):
        return pltpu.make_async_remote_copy(
            src_ref=src, dst_ref=dst, send_sem=send, recv_sem=recv,
            device_id=(lon_to, lat_to), device_id_type=MESH,
        )

    def head_copy(j):
        return copy(z_first.at[1], heads.at[1], sends.at[HEAD], recvs.at[HEAD], j, lat)

    head_mid = copy(z_first.at[0], heads.at[0], sends.at[HEAD], recvs.at[HEAD], mid, lat)
    head_last = copy(z_first.at[0], heads.at[0], sends.at[HEAD], recvs.at[HEAD], last, lat)
    tail_mid = copy(z_tail.at[0], tail_zero, sends.at[TAIL], recvs.at[TAIL], 0, lat)
    tail_last = copy(z_last.at[0], from_left.at[0], sends.at[TAIL], recvs.at[TAIL], 0, lat)

    def tail_copy(j):
        return copy(z_tail.at[1], tails_in.at[j], sends.at[TAIL], recvs.at[TAIL], 0, lat)

    to_right = copy(z_last, from_left, sends.at[RIGHT], recvs.at[NEAR], right, lat)
    to_left = copy(z_first, from_right, sends.at[LEFT], recvs.at[NEAR], left, lat)

    lengths = [len_ref[r] for r in range(rows_dev)]
    index8 = lax.broadcasted_iota(jnp.int32, (8, 128), 0)

    def load_rows(rows):
        load_state(zs, z_ref.reshape(m_ref.shape), zc_ref, cells, rows_dev, rows)
        for r in rows:
            at = jnp.clip(lengths[r] - 4 - start, -4, cells)
            cell = lengths[r] - 4 - start + index8
            own = (cell >= 0) & (cell < cells)
            for ch in range(4):
                value = zs[ch * 4 + r, pl.ds(PAD + at, 8), :]
                z_tail[r // 2, ch, pl.ds((r % 2) * 4, 4), :] = jnp.where(own, value, 0.0)[:4]

    load_rows(range(2, rows_dev))

    @pl.when(is_far)
    def _():
        tail_copy(me).start()

    loads[3].wait()
    load_rows(range(2))
    pack_ends(z_first, z_last, zs, cells, rows_dev)

    @pl.when(me == mid)
    def _():
        tail_mid.start()

    @pl.when(me == last)
    def _():
        tail_last.start()

    @pl.when(left_earlier)
    def _():
        to_left.start()

    @pl.when(right_earlier)
    def _():
        to_right.start()

    for load in loads[4:6]:
        load.wait()
    load_state(ms, m_ref, mc_ref, cells, rows_dev, range(rows_dev))
    pack_ends(m_first, m_last, ms, cells, rows_dev)
    to_south = copy(
        m_first, m_halo.at[south_slot], sends.at[MERID], recvs.at[MERID], south_lon, south_lat
    )
    to_north = copy(
        m_last, m_halo.at[north_slot], sends.at[MERID], recvs.at[MERID], north_lon, north_lat
    )

    def over_poles(some):
        @pl.when(at_south & some)
        def _():
            to_south.start()

        @pl.when(at_north & some)
        def _():
            to_north.start()

    @pl.when(jnp.logical_not(at_south))
    def _():
        to_south.start()

    over_poles((me >= mid) & (me < mid + 2))

    for load in loads[6:]:
        load.wait()
    tiled = jnp.concatenate([mix_ref[...]] * 4, axis=1)
    index_of = lambda axis: lax.broadcasted_iota(jnp.int32, (128, 128), axis)
    block_of = lambda axis: index_of(axis) // 32
    matrix = jnp.where(block_of(0) == block_of(1), tiled, 0.0).T
    matrix = 10.0 * matrix + jnp.where(index_of(0) == index_of(1), 2.0, 0.0)
    w_high = matrix.astype(jnp.bfloat16)
    w_low = (matrix - w_high.astype(F32)).astype(jnp.bfloat16)
    pair = jnp.concatenate([w_high, w_low], axis=1)
    weights[pl.ds(0, 128), :] = pair
    weights[pl.ds(128, 128), :] = pair
    zeros = jnp.zeros((PAD, 128), F32)
    for slot in range(16):
        zs[slot, pl.ds(0, PAD), :] = zeros
        zs[slot, pl.ds(PAD + cells, PAD), :] = zeros
    for buf in (zh, zh1, fh, fh1):
        for ch in range(3):
            buf[ch, pl.ds(0, PAD), :] = zeros
            buf[ch, pl.ds(buf.shape[1] - PAD, PAD), :] = zeros

    @pl.when(left_later)
    def _():
        pl.semaphore_wait(hello_side.at[0], 1)
        to_left.start()

    @pl.when(right_later)
    def _():
        pl.semaphore_wait(hello_side.at[1], 1)
        to_right.start()

    quarter = n // 4

    def serve(group, now):
        targets = [j for j in range(quarter * group, quarter * (group + 1)) if j >= wrap_from]

        @pl.when(is_hub & now)
        def _():
            pl.semaphore_wait(hello_far.at[group], len(targets))
            for j in targets[::2] + targets[1::2]:
                head_copy(j).start()
                if j == mid:
                    head_mid.start()
                if j == last:
                    head_last.start()

    ends = [jnp.clip(lengths[r] - start, 0, cells) for r in range(rows_dev)]
    for src, dst in ((zs, zs1), (zs1, zs2)):
        advance(src, dst, zs, products, weights, cells, rows_dev, None)
    @pl.when(jnp.logical_not(at_north))
    def _():
        pl.semaphore_wait(hello_merid.at[1], 1)
        to_north.start()

    def ready_poles(some):
        @pl.when(at_south & some)
        def _():
            pl.semaphore_wait(hello_merid.at[0], 1)

        @pl.when(at_north & some)
        def _():
            pl.semaphore_wait(hello_merid.at[1], 1)

    ready_poles((me > 1) & (me < mid))
    over_poles((me > 1) & ((me < mid) | (me >= mid + 2)))

    advance(zs2, zs1, zs, products, weights, cells, rows_dev, None)
    advance(zs1, zs2, zs, products, weights, cells, rows_dev, ends, final=True)
    always = me >= 0
    serve(0, always)
    serve(1, always)
    serve(2, lat > 0)

    ready_poles((me <= 1) & (lat > 0))
    over_poles((me <= 1) & (lat > 0))

    for r in range(rows_dev):
        owners = (own_ref[pl.ds(r, 1), :] + 1).astype(F32)
        zs[16 + r, pl.ds(PAD, cells), :] = jnp.broadcast_to(owners, (128, cells)).T
    for r in range(rows_dev):
        at = jnp.clip(lengths[r] - 8 - start, -8, cells)
        cell = lengths[r] - 8 - start + index8
        for ch in range(5):
            value = zs[ch * 4 + r, pl.ds(PAD + at, 8), :]
            z_window[r, ch, :, :] = jnp.where((cell >= 0) & (cell < cells), value, 0.0)
    moving = z_window.at[pl.ds(2, rows_dev - 2)]
    window_left = copy(moving, w_right, sends.at[LEFT], recvs.at[WINDOW], left, lat)
    window_right = copy(moving, w_left, sends.at[RIGHT], recvs.at[WINDOW], right, lat)

    @pl.when(has_left)
    def _():
        window_left.start()

    @pl.when(has_right)
    def _():
        window_right.start()

    for src, dst in ((ms, ms1), (ms1, ms2)):
        advance(src, dst, ms, products, weights, cells, rows_dev, None)
    serve(2, at_south)
    serve(3, lat > 0)
    def fill_left():
        for r in range(rows_dev):
            take = pl.ds((r % 2) * 4, 4)
            for ch in range(4):
                zs[ch * 4 + r, pl.ds(PAD - 4, 4), :] = from_left[r // 2, ch, take, :]

    def fill_right():
        for r in range(rows_dev):
            take = pl.ds((r % 2) * 4, 4)
            for ch in range(4):
                zs[ch * 4 + r, pl.ds(PAD + cells, 4), :] = from_right[r // 2, ch, take, :]

    index4 = lax.broadcasted_iota(jnp.int32, (4, 128), 0)

    scale = GLON_DEV / (3.0 * cells)
    near = me * GLON_DEV - 1 + lax.broadcasted_iota(jnp.int32, (8, cells), 0)
    lane = lax.broadcasted_iota(jnp.int32, (8, cells), 1)

    first_late = jnp.where(is_hub, 4, 0)

    def column_terms(r):
        body = pl.ds(PAD, cells)
        before = zs[r, body, :] + zs[4 + r, body, :] + zs[8 + r, body, :]
        after = zs2[r, body, :] + zs2[4 + r, body, :] + zs2[8 + r, body, :]
        delta = (after - before) * scale
        high = delta.astype(jnp.bfloat16)
        low = (delta - high.astype(F32)).astype(jnp.bfloat16)
        to_end = lane - (lengths[r] - start)
        early = ((to_end < -4) | (to_end >= 0)) & (lane >= first_late)
        table = ((own_ref[pl.ds(r, 1), :] == near) & early).astype(jnp.bfloat16)
        both = jnp.dot(
            table, jnp.concatenate([high, low], axis=1), preferred_element_type=F32
        )
        half = both.shape[1] // 2
        return both[:, :half] + both[:, half:]

    part_left = copy(c_left, c_from_right, sends.at[LEFT], recvs.at[PART], left, lat)
    part_right = copy(c_right, c_from_left, sends.at[RIGHT], recvs.at[PART], right, lat)

    def transfers(count, sem):
        lines = products.at[pl.ds(0, count)]
        return copy(lines, lines, sends.at[sem], recvs.at[sem], partner, lat)

    both = has_left & has_right
    one_side = jnp.logical_not(both)
    ends_here = (me == mid) | (me == last)
    plain_far = is_far & jnp.logical_not(ends_here)
    all_tails = (n - wrap_from + 2) * 32

    def beside(count, sem):
        @pl.when(both)
        def _():
            transfers(2 * count, sem).wait_recv()

        @pl.when(one_side)
        def _():
            transfers(count, sem).wait_recv()

    beside(64, NEAR)

    @pl.when(has_left)
    def _():
        fill_left()

    @pl.when(has_right)
    def _():
        fill_right()

    for r in range(rows_dev):
        for ch in range(4):
            base = PAD + r * 32
            zh[ch, pl.ds(base, 16), :] = zs[ch * 4 + r, pl.ds(PAD - 4, 16), :]
            zh[ch, pl.ds(base + 16, 16), :] = zs[ch * 4 + r, pl.ds(PAD + cells - 8, 16), :]
    advance_strips(zh, zh1, products, weights, 32 * rows_dev)
    for r in range(rows_dev):
        base = PAD + r * 32
        for w in range(3):
            for cell, take in ((0, base + 4), (cells - 4, base + 20)):
                old = zs2[w * 4 + r, pl.ds(PAD + cell, 4), :]
                zs2[w * 4 + r, pl.ds(PAD + cell, 4), :] = jnp.where(
                    index4 + cell < ends[r], zh[w, pl.ds(take, 4), :], old
                )
    for r in range(rows_dev):
        terms = column_terms(r)
        c_left[pl.ds(r, 1), :] = terms[0:1]
        c_right[pl.ds(r, 1), :] = terms[GLON_DEV + 1 : GLON_DEV + 2]
        for g in range(GLON_DEV):
            co_ref[g, pl.ds(r, 1), :] = terms[g + 1 : g + 2]

    @pl.when(has_left)
    def _():
        part_left.start()

    @pl.when(has_right)
    def _():
        part_right.start()

    ready_poles((me <= 1) & at_south)
    over_poles((me <= 1) & at_south)

    serve(3, at_south)

    for src, dst in ((ms2, ms1), (ms1, ms2)):
        advance(src, dst, ms, products, weights, cells, rows_dev, None, final=dst is ms2)
    transfers(128, MERID).wait_recv()

    @pl.when(plain_far)
    def _():
        transfers(32, HEAD).wait_recv()

    @pl.when(ends_here)
    def _():
        transfers(64, HEAD).wait_recv()

    beside((rows_dev - 2) * 40, WINDOW)

    @pl.when(is_hub)
    def _():
        transfers(all_tails, TAIL).wait_recv()

    @pl.when(is_hub)
    def _():
        for ch in range(4):
            total = tails_in[wrap_from, ch]
            for j in range(wrap_from + 1, n):
                total = total + tails_in[j, ch]
            fh[ch, pl.ds(PAD, 4), :] = tail_zero[ch, pl.ds(0, 4), :]
            fh[ch, pl.ds(PAD + 16, 4), :] = from_left[0, ch, pl.ds(4, 4), :]
            for r in range(2, rows_dev):
                half = (r % 2) * 4
                fh[ch, pl.ds(PAD + 16 * r, 4), :] = total[half : half + 4]
            for r in range(rows_dev):
                fh[ch, pl.ds(PAD + 16 * r + 4, 12), :] = zs[ch * 4 + r, pl.ds(PAD, 12), :]
        for r in range(rows_dev):
            seam_owner[r, :, :] = zs[16 + r, pl.ds(PAD, 8), :]

    @pl.when(has_left)
    def _():
        for r in range(rows_dev):
            for ch in range(5):
                window = z_window[r, ch]
                if r >= 2:
                    window = window + w_left[r - 2, ch]
                    window = window + jnp.where(has_right, w_right[r - 2, ch], 0.0)
                if ch == 4:
                    seam_owner[r, pl.ds(0, 4), :] = window[4:8]
                    continue
                base = PAD + 16 * r
                fh[ch, pl.ds(base, 8), :] = window
                fh[ch, pl.ds(base + 8, 4), :] = heads[r // 2, ch, pl.ds((r % 2) * 4, 4), :]
                fh[ch, pl.ds(base + 12, 4), :] = jnp.zeros((4, 128), F32)

    merid = PAD + 16 * rows_dev
    for r in range(rows_dev):
        take = (r % 2) * 4
        for ch in range(4):
            turned = ch if ch == 3 else 2 - ch
            sign = -1.0 if ch == 3 else 1.0
            base = merid + r * 32
            for j in range(4):
                plain = m_halo[0, r // 2, ch, pl.ds(take + j, 1), :]
                pole = sign * m_halo[0, r // 2, turned, pl.ds(take + 3 - j, 1), :]
                fh[ch, pl.ds(base + j, 1), :] = jnp.where(at_south, pole, plain)
                plain = m_halo[1, r // 2, ch, pl.ds(take + j, 1), :]
                pole = sign * m_halo[1, r // 2, turned, pl.ds(take + 3 - j, 1), :]
                fh[ch, pl.ds(base + 24 + j, 1), :] = jnp.where(at_north, pole, plain)
            fh[ch, pl.ds(base + 4, 12), :] = ms[ch * 4 + r, pl.ds(PAD, 12), :]
            fh[ch, pl.ds(base + 16, 8), :] = ms[ch * 4 + r, pl.ds(PAD + cells - 8, 8), :]
            fh[ch, pl.ds(base + 28, 4), :] = jnp.zeros((4, 128), F32)

    def wanted(r):
        at = pl.ds(PAD + 16 * r + 4, 4)
        return fh[0, at, :] + fh[1, at, :] + fh[2, at, :]

    seam_before = [wanted(r) for r in range(rows_dev)]
    advance_strips(fh, fh1, products, weights, 48 * rows_dev)
    for r in range(rows_dev):
        for w in range(3):
            at, base = w * 4 + r, merid + r * 32
            ms2[at, pl.ds(PAD, 4), :] = fh[w, pl.ds(base + 4, 4), :]
            ms2[at, pl.ds(PAD + cells - 4, 4), :] = fh[w, pl.ds(base + 20, 4), :]

    @pl.when(is_hub)
    def _():
        for r in range(rows_dev):
            for w in range(3):
                zs2[w * 4 + r, pl.ds(PAD, 4), :] = fh[w, pl.ds(PAD + 16 * r + 4, 4), :]

    @pl.when(has_left)
    def _():
        for r in range(rows_dev):
            for block in range(0, cells, 8):
                ahead = block - (lengths[r] - start)
                inside = (index8 + ahead >= -4) & (index8 + ahead < 0)
                take = PAD + 16 * r + 8 + jnp.clip(ahead, -12, 0)
                for w in range(3):
                    at = w * 4 + r
                    old = zs2[at, pl.ds(PAD + block, 8), :]
                    zs2[at, pl.ds(PAD + block, 8), :] = jnp.where(
                        inside, fh[w, pl.ds(take, 8), :], old
                    )

    for r in range(rows_dev):
        delta = (wanted(r) - seam_before[r]) * scale
        owner = seam_owner[r, pl.ds(0, 4), :]
        for g in range(GLON_DEV):
            mine = owner == (me * GLON_DEV + g + 1).astype(F32)
            co_ref[g, pl.ds(r, 1), :] += jnp.sum(
                jnp.where(mine, delta, 0.0), axis=0, keepdims=True
            )

    beside(8, PART)

    @pl.when(has_left)
    def _():
        for r in range(rows_dev):
            co_ref[0, pl.ds(r, 1), :] += c_from_left[pl.ds(r, 1), :]

    @pl.when(has_right)
    def _():
        for r in range(rows_dev):
            co_ref[GLON_DEV - 1, pl.ds(r, 1), :] += c_from_right[pl.ds(r, 1), :]

    sideways = 64 + (rows_dev - 2) * 40 + 8
    transfers(128, MERID).wait_send()
    for flag, count, sem in (
        (has_left, sideways, LEFT),
        (has_right, sideways, RIGHT),
        (plain_far, 32, TAIL),
        (ends_here, 64, TAIL),
        (is_hub, all_tails, HEAD),
    ):

        @pl.when(flag)
        def _():
            transfers(count, sem).wait_send()


def finish(cells, rows_dev, zs, ms, co, zo_hbm, mo_hbm, co_hbm, zo, mo, sems):
    copies = [pltpu.make_async_copy(co, co_hbm, sems.at[6])]
    copies[0].start()
    for i, (state, staged, out) in enumerate(((ms, mo, mo_hbm), (zs, zo, zo_hbm))):
        for w in range(3):
            rows = staged.at[w].reshape(128 * rows_dev, cells)
            for r in range(rows_dev):
                block = state[w * 4 + r, pl.ds(PAD, cells), :]
                rows[pl.ds(r, 128, stride=rows_dev), :] = block.T
            copies.append(
                pltpu.make_async_copy(staged.at[w], out.at[:, w], sems.at[3 * i + w])
            )
            copies[-1].start()
    for done in copies:
        done.wait()


def solution(mesh):
    n, n_lat = mesh.shape["lon"], mesh.shape["lat"]

    def shards(
        zonal_state, zonal_courant, zonal_length, zonal_owner, merid_state, merid_courant, mixing
    ):
        nv, lev, wid, rows_dev, cells = zonal_state.shape
        flat = nv * lev * wid * rows_dev
        vmem = pl.BlockSpec(memory_space=pltpu.VMEM)
        hbm = pl.BlockSpec(memory_space=pltpu.HBM)
        shape = jax.ShapeDtypeStruct
        state = (16, cells + 2 * PAD, 128)
        strips = (4, 32 * rows_dev + 2 * PAD, 128)
        packet = pltpu.VMEM((2, 4, 8, 128), F32)
        small = pltpu.VMEM((8, 128), F32)
        products = pltpu.VMEM((rows_dev * 3 * cells, 128), F32)
        dma = pltpu.SemaphoreType.DMA
        regular = pltpu.SemaphoreType.REGULAR
        held = pl.pallas_call(
            functools.partial(kernel, n, n_lat, cells, rows_dev),
            out_shape=(
                shape(state, F32), shape(state, F32),
                shape((GLON_DEV, rows_dev, nv * lev), F32),
            ),
            in_specs=[hbm] * 7,
            out_specs=(vmem,) * 3,
            scratch_shapes=[
                pltpu.SMEM((rows_dev,), jnp.int32),
                pltpu.VMEM((nv * lev * wid, 2, rows_dev // 2, cells), F32),
                pltpu.VMEM((lev * rows_dev, cells), F32),
                pltpu.VMEM((rows_dev, cells), jnp.int32),
                pltpu.VMEM((flat, cells), F32),
                pltpu.VMEM((lev * rows_dev, cells), F32),
                pltpu.VMEM((nv * lev, lev), F32),
                pltpu.VMEM((20, *state[1:]), F32), pltpu.VMEM(state, F32),
                pltpu.VMEM(state, F32), pltpu.VMEM(state, F32),
                pltpu.VMEM((4, 48 * rows_dev + 2 * PAD, 128), F32),
                pltpu.VMEM((4, 48 * rows_dev + 2 * PAD, 128), F32),
                pltpu.VMEM(strips, F32), pltpu.VMEM(strips, F32),
                products, pltpu.VMEM((256, 256), jnp.bfloat16),
                packet, packet, packet, packet, packet,
                packet, packet, packet,
                pltpu.VMEM((n, 4, 8, 128), F32),
                pltpu.VMEM((4, 8, 128), F32),
                pltpu.VMEM((2, 2, 4, 8, 128), F32),
                pltpu.VMEM((rows_dev, 5, 8, 128), F32),
                pltpu.VMEM((rows_dev - 2, 5, 8, 128), F32),
                pltpu.VMEM((rows_dev - 2, 5, 8, 128), F32),
                pltpu.VMEM((rows_dev, 8, 128), F32),
                small, small, small, small,
                dma((8,)), dma((6,)),
                regular((2,)), regular((2,)), regular((4,)),
            ],
            compiler_params=pltpu.CompilerParams(
                collective_id=0, has_side_effects=True, vmem_limit_bytes=48 * 1024 * 1024
            ),
        )(
            *(
                pltpu.with_memory_space_constraint(value, pltpu.HBM)
                for value in (
                    zonal_length,
                    zonal_state.reshape(nv * lev * wid, 2, rows_dev // 2, cells),
                    zonal_courant.reshape(lev * rows_dev, cells),
                    zonal_owner,
                    merid_state.reshape(flat, cells),
                    merid_courant.reshape(lev * rows_dev, cells),
                    mixing.reshape(nv * lev, lev),
                )
            )
        )
        zo, mo, co = pl.pallas_call(
            functools.partial(finish, cells, rows_dev),
            out_shape=(
                shape((nv * lev, wid, rows_dev, cells), F32),
                shape((nv * lev, wid, rows_dev, cells), F32),
                shape((GLON_DEV, rows_dev, nv * lev), F32),
            ),
            in_specs=[vmem] * 3,
            out_specs=(hbm,) * 3,
            scratch_shapes=[
                pltpu.VMEM((wid, nv * lev, rows_dev, cells), F32),
                pltpu.VMEM((wid, nv * lev, rows_dev, cells), F32),
                dma((7,)),
            ],
            compiler_params=pltpu.CompilerParams(vmem_limit_bytes=40 * 1024 * 1024),
        )(*held)
        return zo.reshape(zonal_state.shape), mo.reshape(merid_state.shape), co

    return jax.shard_map(
        shards,
        mesh=mesh,
        in_specs=(
            P(None, None, None, "lat", "lon"),
            P(None, "lat", "lon"),
            P("lat"),
            P("lat", "lon"),
            P(None, None, None, "lon", "lat"),
            P(None, "lon", "lat"),
            P(),
        ),
        out_specs=(
            P(None, None, None, "lat", "lon"),
            P(None, None, None, "lon", "lat"),
            P("lon", "lat", None),
        ),
        check_vma=False,
    )
```

```python
import functools

import jax
import jax.numpy as jnp
from jax import lax
from jax.experimental import pallas as pl
from jax.experimental.pallas import tpu as pltpu
from jax.sharding import PartitionSpec as P

SUB = 4
GLON_DEV = 4
PAD = 8
STEP = 32
UNSCALE = 10.0**-SUB
MESH = pl.DeviceIdType.MESH
LEFT, RIGHT, MERID, TAIL, HEAD = range(5)
NEAR, PART, WINDOW = 0, 1, 5
F32 = jnp.float32


def mix_into(products, at, fields, weights):
    wide = jnp.concatenate(fields, axis=0)
    high = wide.astype(jnp.bfloat16)
    low = (wide - high.astype(F32)).astype(jnp.bfloat16)
    out = jnp.dot(jnp.concatenate([high, low], axis=1), weights[...], preferred_element_type=F32)
    half = out.shape[1] // 2
    products[pl.ds(at, wide.shape[0]), :] = out[:, :half] + out[:, half:]


def updated(now, ahead, behind, five, product):
    c_ahead = 3.0 - five
    c_behind = 3.0 + five
    x0, x1, x2 = now
    pairs = (x0 + x1, x0 + x2, x1 + x2)
    return [
        (pairs[w] + product[w]) + (c_ahead * ahead[w] + c_behind * behind[w]) for w in range(3)
    ]


def advance(src, dst, fives, products, weights, cells, rows_dev, ends, final=False):
    rows = 3 * cells
    step = STEP
    for r in range(rows_dev):
        mix_into(
            products,
            r * rows,
            [src[w * 4 + r, pl.ds(PAD, cells), :] for w in range(3)],
            weights,
        )
    for r in range(rows_dev):
        for at in range(0, cells, step):
            now = [src[w * 4 + r, pl.ds(PAD + at, step), :] for w in range(3)]
            ahead = [src[w * 4 + r, pl.ds(PAD + at + 1, step), :] for w in range(3)]
            behind = [src[w * 4 + r, pl.ds(PAD + at - 1, step), :] for w in range(3)]
            five = fives[12 + r, pl.ds(PAD + at, step), :]
            product = [
                products[pl.ds(r * rows + w * cells + at, step), :] for w in range(3)
            ]
            new = updated(now, ahead, behind, five, product)
            for w in range(3):
                value = new[w] * UNSCALE if final else new[w]
                if ends is not None:
                    index = at + lax.broadcasted_iota(jnp.int32, (step, 128), 0)
                    kept = fives[w * 4 + r, pl.ds(PAD + at, step), :]
                    value = jnp.where(index < ends[r], value, kept)
                dst[w * 4 + r, pl.ds(PAD + at, step), :] = value


def advance_strips(first, second, products, weights, rows, step):
    for t in range(SUB):
        src, dst = (first, second) if t % 2 == 0 else (second, first)
        mix_into(products, 0, [src[w, pl.ds(PAD, rows), :] for w in range(3)], weights)
        for at in range(0, rows, step):
            now = [src[w, pl.ds(PAD + at, step), :] for w in range(3)]
            ahead = [src[w, pl.ds(PAD + at + 1, step), :] for w in range(3)]
            behind = [src[w, pl.ds(PAD + at - 1, step), :] for w in range(3)]
            five = first[3, pl.ds(PAD + at, step), :]
            product = [products[pl.ds(w * rows + at, step), :] for w in range(3)]
            new = updated(now, ahead, behind, five, product)
            for w in range(3):
                dst[w, pl.ds(PAD + at, step), :] = new[w] * UNSCALE if t == SUB - 1 else new[w]


def load_state(state, field, courant, cells, rows_dev, rows):
    for r in rows:
        for w in range(3):
            at = w * rows_dev + r
            block = field[pl.ds(at, 128, stride=3 * rows_dev), :]
            state[w * 4 + r, pl.ds(PAD, cells), :] = block.T
        levels = courant[pl.ds(r, 32, stride=rows_dev), :]
        state[12 + r, pl.ds(PAD, cells), :] = jnp.concatenate([5.0 * levels] * 4, axis=0).T


def pack_ends(first, last, state, cells, rows_dev):
    for r in range(rows_dev):
        for ch in range(4):
            put = pl.ds((r % 2) * 4, 4)
            first[r // 2, ch, put, :] = state[ch * 4 + r, pl.ds(PAD, 4), :]
            last[r // 2, ch, put, :] = state[ch * 4 + r, pl.ds(PAD + cells - 4, 4), :]


def kernel(
    n, n_lat, cells, rows_dev,
    len_hbm, z_hbm, zc_hbm, own_hbm, m_hbm, mc_hbm, mix_hbm,
    zs2, ms2, co_ref,
    len_ref, z_ref, zc_ref, own_ref, m_ref, mc_ref, mix_ref,
    zs, zs1, ms, ms1, fh, fh1, zh, zh1, products, weights,
    z_first, z_last, z_tail, m_first, m_last,
    from_left, from_right, heads, tails_in, tail_zero, m_halo,
    z_window, w_left, w_right, seam_owner,
    c_left, c_right, c_from_left, c_from_right,
    sends, recvs,
    hello_side, hello_merid, hello_far,
):
    me = lax.axis_index("lon")
    lat = lax.axis_index("lat")
    right, left = lax.rem(me + 1, n), lax.rem(me + n - 1, n)
    partner = lax.rem(me + n // 2, n)
    wrap_from = n // 4 - 1
    mid = n // 2
    last = n - 1
    start = me * cells
    halves = ((z_hbm.at[:, 1], z_ref.at[:, 1]), (z_hbm.at[:, 0], z_ref.at[:, 0]))
    loads = [
        pltpu.make_async_copy(src, dst, sends.at[sem])
        for src, dst, sem in (
            (*halves[0], LEFT), (zc_hbm, zc_ref, RIGHT), (len_hbm, len_ref, TAIL),
            (*halves[1], 5), (m_hbm, m_ref, MERID), (mc_hbm, mc_ref, HEAD),
            (mix_hbm, mix_ref, 6), (own_hbm, own_ref, 7),
        )
    ]
    for load in loads:
        load.start()
    barrier = pltpu.get_barrier_semaphore()

    def greet(lon_to, lat_to):
        pl.semaphore_signal(barrier, inc=1, device_id=(lon_to, lat_to), device_id_type=MESH)

    def hello(semaphore, lon_to, lat_to):
        pl.semaphore_signal(semaphore, inc=1, device_id=(lon_to, lat_to), device_id_type=MESH)

    at_south, at_north = lat == 0, lat == n_lat - 1
    south_lon = jnp.where(at_south, partner, me)
    south_lat = jnp.where(at_south, 0, lat - 1)
    north_lon = jnp.where(at_north, partner, me)
    north_lat = jnp.where(at_north, n_lat - 1, lat + 1)
    south_slot = jnp.where(at_south, 0, 1)
    north_slot = jnp.where(at_north, 1, 0)
    is_hub, is_far, has_left, has_right = me == 0, me >= wrap_from, me > 0, me < last
    south_later = jnp.logical_and(at_south, me < mid)
    north_later = jnp.logical_or(jnp.logical_not(at_north), me < mid)
    south_earlier, north_earlier = jnp.logical_not(south_later), jnp.logical_not(north_later)

    odd = lax.rem(me, 2) == 1
    even = lax.rem(me, 2) == 0
    right_later, right_earlier = has_right & odd, has_right & even
    left_later, left_earlier = has_left & odd, has_left & even

    @pl.when(right_later)
    def _():
        greet(right, lat)

    @pl.when(left_later)
    def _():
        greet(left, lat)

    @pl.when(south_later)
    def _():
        greet(south_lon, south_lat)

    @pl.when(north_later)
    def _():
        greet(north_lon, north_lat)

    @pl.when(is_hub)
    def _():
        for j in range(wrap_from, n):
            greet(j, lat)

    one = lambda flag: jnp.where(flag, 1, 0)
    peers = (
        one(left_earlier) + one(right_earlier)
        + one(south_earlier) + one(north_earlier) + one(is_far)
    )

    @pl.when(peers > 0)
    def _():
        pl.semaphore_wait(barrier, peers)

    @pl.when(is_far)
    def _():
        hello(hello_far.at[lax.div(me, n // 4)], 0, lat)

    @pl.when(left_earlier)
    def _():
        hello(hello_side.at[1], left, lat)

    @pl.when(right_earlier)
    def _():
        hello(hello_side.at[0], right, lat)

    @pl.when(south_earlier)
    def _():
        hello(hello_merid.at[south_slot], south_lon, south_lat)

    @pl.when(north_earlier)
    def _():
        hello(hello_merid.at[north_slot], north_lon, north_lat)

    for load in loads[:2]:
        load.wait()
    def copy(src, dst, send, recv, lon_to, lat_to):
        return pltpu.make_async_remote_copy(
            src_ref=src, dst_ref=dst, send_sem=send, recv_sem=recv,
            device_id=(lon_to, lat_to), device_id_type=MESH,
        )

    def head_copy(j):
        return copy(z_first.at[1], heads.at[1], sends.at[HEAD], recvs.at[HEAD], j, lat)

    head_mid = copy(z_first.at[0], heads.at[0], sends.at[HEAD], recvs.at[HEAD], mid, lat)
    head_last = copy(z_first.at[0], heads.at[0], sends.at[HEAD], recvs.at[HEAD], last, lat)
    tail_mid = copy(z_tail.at[1], tail_zero, sends.at[TAIL], recvs.at[TAIL], 0, lat)
    tail_last = copy(z_tail.at[2], from_left.at[0], sends.at[TAIL], recvs.at[TAIL], 0, lat)

    def tail_copy(j):
        return copy(z_tail.at[0], tails_in.at[j], sends.at[TAIL], recvs.at[TAIL], 0, lat)

    to_right = copy(z_last, from_left, sends.at[RIGHT], recvs.at[NEAR], right, lat)
    to_left = copy(z_first, from_right, sends.at[LEFT], recvs.at[NEAR], left, lat)

    index8 = lax.broadcasted_iota(jnp.int32, (8, 128), 0)

    def load_rows(rows):
        load_state(zs, z_ref.reshape(m_ref.shape), zc_ref, cells, rows_dev, rows)

    def pack_tails(rows, packet):
        for r in rows:
            at = jnp.clip(lengths[r] - 4 - start, -4, cells)
            cell = lengths[r] - 4 - start + index8
            own = (cell >= 0) & (cell < cells)
            for ch in range(4):
                value = zs[ch * 4 + r, pl.ds(PAD + at, 8), :]
                z_tail[packet, ch, pl.ds((r % 2) * 4, 4), :] = jnp.where(own, value, 0.0)[:4]

    load_rows(range(2, rows_dev))
    loads[2].wait()
    lengths = [len_ref[r] for r in range(rows_dev)]
    pack_tails(range(2, rows_dev), 0)

    @pl.when(is_far)
    def _():
        tail_copy(me).start()

    loads[3].wait()
    load_rows(range(1, 2))
    pack_tails(range(1, 2), 2)

    @pl.when(me == last)
    def _():
        tail_last.start()

    load_rows(range(1))
    pack_tails(range(1), 1)
    pack_ends(z_first, z_last, zs, cells, rows_dev)

    @pl.when(me == mid)
    def _():
        tail_mid.start()

    @pl.when(left_earlier)
    def _():
        to_left.start()

    @pl.when(right_earlier)
    def _():
        to_right.start()

    for load in loads[4:6]:
        load.wait()
    load_state(ms, m_ref, mc_ref, cells, rows_dev, range(rows_dev))
    pack_ends(m_first, m_last, ms, cells, rows_dev)
    to_south = copy(
        m_first, m_halo.at[south_slot], sends.at[MERID], recvs.at[MERID], south_lon, south_lat
    )
    to_north = copy(
        m_last, m_halo.at[north_slot], sends.at[MERID], recvs.at[MERID], north_lon, north_lat
    )

    def over_poles(some):
        @pl.when(at_south & some)
        def _():
            to_south.start()

        @pl.when(at_north & some)
        def _():
            to_north.start()

    @pl.when(jnp.logical_not(at_south))
    def _():
        to_south.start()

    over_poles((me >= mid) & (me < mid + 2))

    for load in loads[6:]:
        load.wait()
    tiled = jnp.concatenate([mix_ref[...]] * 4, axis=1)
    index_of = lambda axis: lax.broadcasted_iota(jnp.int32, (128, 128), axis)
    block_of = lambda axis: index_of(axis) // 32
    matrix = jnp.where(block_of(0) == block_of(1), tiled, 0.0).T
    matrix = 10.0 * matrix + jnp.where(index_of(0) == index_of(1), 2.0, 0.0)
    w_high = matrix.astype(jnp.bfloat16)
    w_low = (matrix - w_high.astype(F32)).astype(jnp.bfloat16)
    pair = jnp.concatenate([w_high, w_low], axis=1)
    weights[pl.ds(0, 128), :] = pair
    weights[pl.ds(128, 128), :] = pair
    zeros = jnp.zeros((PAD, 128), F32)
    for slot in range(16):
        zs[slot, pl.ds(0, PAD), :] = zeros
        zs[slot, pl.ds(PAD + cells, PAD), :] = zeros
    for buf in (zh, zh1, fh, fh1):
        for ch in range(3):
            buf[ch, pl.ds(0, PAD), :] = zeros
            buf[ch, pl.ds(buf.shape[1] - PAD, PAD), :] = zeros

    @pl.when(left_later)
    def _():
        pl.semaphore_wait(hello_side.at[0], 1)
        to_left.start()

    @pl.when(right_later)
    def _():
        pl.semaphore_wait(hello_side.at[1], 1)
        to_right.start()

    quarter = n // 4

    def serve(group, now):
        targets = [j for j in range(quarter * group, quarter * (group + 1)) if j >= wrap_from]

        @pl.when(is_hub & now)
        def _():
            pl.semaphore_wait(hello_far.at[group], len(targets))
            for j in targets[::2] + targets[1::2]:
                head_copy(j).start()
                if j == mid:
                    head_mid.start()
                if j == last:
                    head_last.start()

    ends = [jnp.clip(lengths[r] - start, 0, cells) for r in range(rows_dev)]
    for src, dst in ((zs, zs1), (zs1, zs2)):
        advance(src, dst, zs, products, weights, cells, rows_dev, None)
    @pl.when(jnp.logical_not(at_north))
    def _():
        pl.semaphore_wait(hello_merid.at[1], 1)
        to_north.start()

    def ready_poles(some):
        @pl.when(at_south & some)
        def _():
            pl.semaphore_wait(hello_merid.at[0], 1)

        @pl.when(at_north & some)
        def _():
            pl.semaphore_wait(hello_merid.at[1], 1)

    ready_poles((me > 1) & (me < mid))
    over_poles((me > 1) & ((me < mid) | (me >= mid + 2)))

    advance(zs2, zs1, zs, products, weights, cells, rows_dev, None)
    advance(zs1, zs2, zs, products, weights, cells, rows_dev, ends, final=True)
    always = me >= 0
    serve(0, always)
    serve(1, always)
    serve(2, lat > 0)

    first_chip = ((me == 0) & (lat > 0)) | (me == 1)
    ready_poles(first_chip)
    over_poles(first_chip)

    for r in range(rows_dev):
        owners = (own_ref[pl.ds(r, 1), :] + 1).astype(F32)
        zs[16 + r, pl.ds(PAD, cells), :] = jnp.broadcast_to(owners, (128, cells)).T
    for r in range(rows_dev):
        at = jnp.clip(lengths[r] - 8 - start, -8, cells)
        cell = lengths[r] - 8 - start + index8
        for ch in range(5):
            value = zs[ch * 4 + r, pl.ds(PAD + at, 8), :]
            z_window[r, ch, :, :] = jnp.where((cell >= 0) & (cell < cells), value, 0.0)
    moving = z_window.at[pl.ds(2, rows_dev - 2)]
    window_left = copy(moving, w_right, sends.at[LEFT], recvs.at[WINDOW], left, lat)
    window_right = copy(moving, w_left, sends.at[RIGHT], recvs.at[WINDOW], right, lat)

    far_left, far_right = me > wrap_from, is_far & has_right

    @pl.when(far_left)
    def _():
        window_left.start()

    @pl.when(far_right)
    def _():
        window_right.start()

    def fill_left():
        for r in range(rows_dev):
            take = pl.ds((r % 2) * 4, 4)
            for ch in range(4):
                zs[ch * 4 + r, pl.ds(PAD - 4, 4), :] = from_left[r // 2, ch, take, :]

    def fill_right():
        for r in range(rows_dev):
            take = pl.ds((r % 2) * 4, 4)
            for ch in range(4):
                zs[ch * 4 + r, pl.ds(PAD + cells, 4), :] = from_right[r // 2, ch, take, :]

    index4 = lax.broadcasted_iota(jnp.int32, (4, 128), 0)

    scale = GLON_DEV / (3.0 * cells)
    near = me * GLON_DEV - 1 + lax.broadcasted_iota(jnp.int32, (8, cells), 0)
    lane = lax.broadcasted_iota(jnp.int32, (8, cells), 1)

    first_late = jnp.where(is_hub, 4, 0)

    def column_terms(r):
        body = pl.ds(PAD, cells)
        before = zs[r, body, :] + zs[4 + r, body, :] + zs[8 + r, body, :]
        after = zs2[r, body, :] + zs2[4 + r, body, :] + zs2[8 + r, body, :]
        delta = (after - before) * scale
        high = delta.astype(jnp.bfloat16)
        low = (delta - high.astype(F32)).astype(jnp.bfloat16)
        to_end = lane - (lengths[r] - start)
        early = ((to_end < -4) | (to_end >= 0)) & (lane >= first_late)
        table = ((own_ref[pl.ds(r, 1), :] == near) & early).astype(jnp.bfloat16)
        both = jnp.dot(
            table, jnp.concatenate([high, low], axis=1), preferred_element_type=F32
        )
        half = both.shape[1] // 2
        return both[:, :half] + both[:, half:]

    part_left = copy(c_left, c_from_right, sends.at[LEFT], recvs.at[PART], left, lat)
    part_right = copy(c_right, c_from_left, sends.at[RIGHT], recvs.at[PART], right, lat)

    def transfers(count, sem):
        lines = products.at[pl.ds(0, count)]
        return copy(lines, lines, sends.at[sem], recvs.at[sem], partner, lat)

    ends_here = (me == mid) | (me == last)
    plain_far = is_far & jnp.logical_not(ends_here)
    all_tails = (n - wrap_from + 2) * 32

    def beside(count, sem, from_left, from_right):
        @pl.when(from_left & from_right)
        def _():
            transfers(2 * count, sem).wait_recv()

        @pl.when(jnp.logical_xor(from_left, from_right))
        def _():
            transfers(count, sem).wait_recv()

    beside(64, NEAR, has_left, has_right)

    @pl.when(has_left)
    def _():
        fill_left()

    @pl.when(has_right)
    def _():
        fill_right()

    for r in range(rows_dev):
        for ch in range(4):
            base = PAD + r * 32
            zh[ch, pl.ds(base, 16), :] = zs[ch * 4 + r, pl.ds(PAD - 4, 16), :]
            zh[ch, pl.ds(base + 16, 16), :] = zs[ch * 4 + r, pl.ds(PAD + cells - 8, 16), :]
    advance_strips(zh, zh1, products, weights, 32 * rows_dev, STEP)
    for r in range(rows_dev):
        base = PAD + r * 32
        for w in range(3):
            for cell, take in ((0, base + 4), (cells - 4, base + 20)):
                old = zs2[w * 4 + r, pl.ds(PAD + cell, 4), :]
                zs2[w * 4 + r, pl.ds(PAD + cell, 4), :] = jnp.where(
                    index4 + cell < ends[r], zh[w, pl.ds(take, 4), :], old
                )
    for r in range(rows_dev):
        terms = column_terms(r)
        c_left[pl.ds(r, 1), :] = terms[0:1]
        c_right[pl.ds(r, 1), :] = terms[GLON_DEV + 1 : GLON_DEV + 2]
        for g in range(GLON_DEV):
            co_ref[g, pl.ds(r, 1), :] = terms[g + 1 : g + 2]

    @pl.when(has_left)
    def _():
        part_left.start()

    @pl.when(has_right)
    def _():
        part_right.start()

    for src, dst in ((ms, ms1), (ms1, ms2)):
        advance(src, dst, ms, products, weights, cells, rows_dev, None)
    serve(2, at_south)
    serve(3, lat > 0)
    ready_poles(is_hub & at_south)
    over_poles(is_hub & at_south)

    serve(3, at_south)

    for src, dst in ((ms2, ms1), (ms1, ms2)):
        advance(src, dst, ms, products, weights, cells, rows_dev, None, final=dst is ms2)
    transfers(128, MERID).wait_recv()

    @pl.when(plain_far)
    def _():
        transfers(32, HEAD).wait_recv()

    @pl.when(ends_here)
    def _():
        transfers(64, HEAD).wait_recv()

    beside((rows_dev - 2) * 40, WINDOW, far_left, far_right)

    @pl.when(is_hub)
    def _():
        transfers(all_tails, TAIL).wait_recv()

    @pl.when(is_hub)
    def _():
        for ch in range(4):
            total = tails_in[wrap_from, ch]
            for j in range(wrap_from + 1, n):
                total = total + tails_in[j, ch]
            fh[ch, pl.ds(PAD, 4), :] = tail_zero[ch, pl.ds(0, 4), :]
            fh[ch, pl.ds(PAD + 12, 4), :] = from_left[0, ch, pl.ds(4, 4), :]
            for r in range(2, rows_dev):
                half = (r % 2) * 4
                fh[ch, pl.ds(PAD + 12 * r, 4), :] = total[half : half + 4]
            for r in range(rows_dev):
                fh[ch, pl.ds(PAD + 12 * r + 4, 8), :] = zs[ch * 4 + r, pl.ds(PAD, 8), :]
        for r in range(rows_dev):
            seam_owner[r, :, :] = zs[16 + r, pl.ds(PAD, 8), :]

    @pl.when(has_left)
    def _():
        for r in range(rows_dev):
            for ch in range(5):
                window = z_window[r, ch]
                if r >= 2:
                    window = window + jnp.where(far_left, w_left[r - 2, ch], 0.0)
                    window = window + jnp.where(far_right, w_right[r - 2, ch], 0.0)
                if ch == 4:
                    seam_owner[r, pl.ds(0, 4), :] = window[4:8]
                    continue
                base = PAD + 12 * r
                fh[ch, pl.ds(base, 8), :] = window
                fh[ch, pl.ds(base + 8, 4), :] = heads[r // 2, ch, pl.ds((r % 2) * 4, 4), :]

    merid = PAD + 12 * rows_dev
    for r in range(rows_dev):
        take = (r % 2) * 4
        for ch in range(4):
            turned = ch if ch == 3 else 2 - ch
            sign = -1.0 if ch == 3 else 1.0
            base = merid + r * 24
            for j in range(4):
                plain = m_halo[0, r // 2, ch, pl.ds(take + j, 1), :]
                pole = sign * m_halo[0, r // 2, turned, pl.ds(take + 3 - j, 1), :]
                fh[ch, pl.ds(base + j, 1), :] = jnp.where(at_south, pole, plain)
                plain = m_halo[1, r // 2, ch, pl.ds(take + j, 1), :]
                pole = sign * m_halo[1, r // 2, turned, pl.ds(take + 3 - j, 1), :]
                fh[ch, pl.ds(base + 20 + j, 1), :] = jnp.where(at_north, pole, plain)
            fh[ch, pl.ds(base + 4, 8), :] = ms[ch * 4 + r, pl.ds(PAD, 8), :]
            fh[ch, pl.ds(base + 12, 8), :] = ms[ch * 4 + r, pl.ds(PAD + cells - 8, 8), :]

    def wanted(r):
        at = pl.ds(PAD + 12 * r + 4, 4)
        return fh[0, at, :] + fh[1, at, :] + fh[2, at, :]

    seam_before = [wanted(r) for r in range(rows_dev)]
    advance_strips(fh, fh1, products, weights, 36 * rows_dev, 48)
    for r in range(rows_dev):
        for w in range(3):
            at, base = w * 4 + r, merid + r * 24
            ms2[at, pl.ds(PAD, 4), :] = fh[w, pl.ds(base + 4, 4), :]
            ms2[at, pl.ds(PAD + cells - 4, 4), :] = fh[w, pl.ds(base + 16, 4), :]

    @pl.when(is_hub)
    def _():
        for r in range(rows_dev):
            for w in range(3):
                zs2[w * 4 + r, pl.ds(PAD, 4), :] = fh[w, pl.ds(PAD + 12 * r + 4, 4), :]

    @pl.when(has_left)
    def _():
        for r in range(rows_dev):
            for block in range(0, cells, 8):
                ahead = block - (lengths[r] - start)
                inside = (index8 + ahead >= -4) & (index8 + ahead < 0)
                take = PAD + 12 * r + 8 + jnp.clip(ahead, -12, 0)
                for w in range(3):
                    at = w * 4 + r
                    old = zs2[at, pl.ds(PAD + block, 8), :]
                    zs2[at, pl.ds(PAD + block, 8), :] = jnp.where(
                        inside, fh[w, pl.ds(take, 8), :], old
                    )

    for r in range(rows_dev):
        delta = (wanted(r) - seam_before[r]) * scale
        owner = seam_owner[r, pl.ds(0, 4), :]
        for g in range(GLON_DEV):
            mine = owner == (me * GLON_DEV + g + 1).astype(F32)
            co_ref[g, pl.ds(r, 1), :] += jnp.sum(
                jnp.where(mine, delta, 0.0), axis=0, keepdims=True
            )

    beside(8, PART, has_left, has_right)

    @pl.when(has_left)
    def _():
        for r in range(rows_dev):
            co_ref[0, pl.ds(r, 1), :] += c_from_left[pl.ds(r, 1), :]

    @pl.when(has_right)
    def _():
        for r in range(rows_dev):
            co_ref[GLON_DEV - 1, pl.ds(r, 1), :] += c_from_right[pl.ds(r, 1), :]

    moved = (rows_dev - 2) * 40
    transfers(128, MERID).wait_send()
    for flag, count, sem in (
        (far_left, 72 + moved, LEFT),
        (has_left & jnp.logical_not(far_left), 72, LEFT),
        (far_right, 72 + moved, RIGHT),
        (has_right & jnp.logical_not(far_right), 72, RIGHT),
        (plain_far, 32, TAIL),
        (ends_here, 64, TAIL),
        (is_hub, all_tails, HEAD),
    ):

        @pl.when(flag)
        def _():
            transfers(count, sem).wait_send()


def finish(cells, rows_dev, zs, ms, co, zo_hbm, mo_hbm, co_hbm, zo, mo, sems):
    copies = [pltpu.make_async_copy(co, co_hbm, sems.at[6])]
    copies[0].start()
    for i, (state, staged, out) in enumerate(((ms, mo, mo_hbm), (zs, zo, zo_hbm))):
        for w in range(3):
            rows = staged.at[w].reshape(128 * rows_dev, cells)
            for r in range(rows_dev):
                block = state[w * 4 + r, pl.ds(PAD, cells), :]
                rows[pl.ds(r, 128, stride=rows_dev), :] = block.T
            copies.append(
                pltpu.make_async_copy(staged.at[w], out.at[:, w], sems.at[3 * i + w])
            )
            copies[-1].start()
    for done in copies:
        done.wait()


def solution(mesh):
    n, n_lat = mesh.shape["lon"], mesh.shape["lat"]

    def shards(
        zonal_state, zonal_courant, zonal_length, zonal_owner, merid_state, merid_courant, mixing
    ):
        nv, lev, wid, rows_dev, cells = zonal_state.shape
        flat = nv * lev * wid * rows_dev
        vmem = pl.BlockSpec(memory_space=pltpu.VMEM)
        hbm = pl.BlockSpec(memory_space=pltpu.HBM)
        shape = jax.ShapeDtypeStruct
        state = (16, cells + 2 * PAD, 128)
        strips = (4, 32 * rows_dev + 2 * PAD, 128)
        packet = pltpu.VMEM((2, 4, 8, 128), F32)
        small = pltpu.VMEM((8, 128), F32)
        products = pltpu.VMEM((rows_dev * 3 * cells, 128), F32)
        dma = pltpu.SemaphoreType.DMA
        regular = pltpu.SemaphoreType.REGULAR
        held = pl.pallas_call(
            functools.partial(kernel, n, n_lat, cells, rows_dev),
            out_shape=(
                shape(state, F32), shape(state, F32),
                shape((GLON_DEV, rows_dev, nv * lev), F32),
            ),
            in_specs=[hbm] * 7,
            out_specs=(vmem,) * 3,
            scratch_shapes=[
                pltpu.SMEM((rows_dev,), jnp.int32),
                pltpu.VMEM((nv * lev * wid, 2, rows_dev // 2, cells), F32),
                pltpu.VMEM((lev * rows_dev, cells), F32),
                pltpu.VMEM((rows_dev, cells), jnp.int32),
                pltpu.VMEM((flat, cells), F32),
                pltpu.VMEM((lev * rows_dev, cells), F32),
                pltpu.VMEM((nv * lev, lev), F32),
                pltpu.VMEM((20, *state[1:]), F32), pltpu.VMEM(state, F32),
                pltpu.VMEM(state, F32), pltpu.VMEM(state, F32),
                pltpu.VMEM((4, 36 * rows_dev + 2 * PAD, 128), F32),
                pltpu.VMEM((4, 36 * rows_dev + 2 * PAD, 128), F32),
                pltpu.VMEM(strips, F32), pltpu.VMEM(strips, F32),
                products, pltpu.VMEM((256, 256), jnp.bfloat16),
                packet, packet, pltpu.VMEM((3, 4, 8, 128), F32), packet, packet,
                packet, packet, packet,
                pltpu.VMEM((n, 4, 8, 128), F32),
                pltpu.VMEM((4, 8, 128), F32),
                pltpu.VMEM((2, 2, 4, 8, 128), F32),
                pltpu.VMEM((rows_dev, 5, 8, 128), F32),
                pltpu.VMEM((rows_dev - 2, 5, 8, 128), F32),
                pltpu.VMEM((rows_dev - 2, 5, 8, 128), F32),
                pltpu.VMEM((rows_dev, 8, 128), F32),
                small, small, small, small,
                dma((8,)), dma((6,)),
                regular((2,)), regular((2,)), regular((4,)),
            ],
            compiler_params=pltpu.CompilerParams(
                collective_id=0, has_side_effects=True, vmem_limit_bytes=48 * 1024 * 1024
            ),
        )(
            *(
                pltpu.with_memory_space_constraint(value, pltpu.HBM)
                for value in (
                    zonal_length,
                    zonal_state.reshape(nv * lev * wid, 2, rows_dev // 2, cells),
                    zonal_courant.reshape(lev * rows_dev, cells),
                    zonal_owner,
                    merid_state.reshape(flat, cells),
                    merid_courant.reshape(lev * rows_dev, cells),
                    mixing.reshape(nv * lev, lev),
                )
            )
        )
        zo, mo, co = pl.pallas_call(
            functools.partial(finish, cells, rows_dev),
            out_shape=(
                shape((nv * lev, wid, rows_dev, cells), F32),
                shape((nv * lev, wid, rows_dev, cells), F32),
                shape((GLON_DEV, rows_dev, nv * lev), F32),
            ),
            in_specs=[vmem] * 3,
            out_specs=(hbm,) * 3,
            scratch_shapes=[
                pltpu.VMEM((wid, nv * lev, rows_dev, cells), F32),
                pltpu.VMEM((wid, nv * lev, rows_dev, cells), F32),
                dma((7,)),
            ],
            compiler_params=pltpu.CompilerParams(vmem_limit_bytes=40 * 1024 * 1024),
        )(*held)
        return zo.reshape(zonal_state.shape), mo.reshape(merid_state.shape), co

    return jax.shard_map(
        shards,
        mesh=mesh,
        in_specs=(
            P(None, None, None, "lat", "lon"),
            P(None, "lat", "lon"),
            P("lat"),
            P("lat", "lon"),
            P(None, None, None, "lon", "lat"),
            P(None, "lon", "lat"),
            P(),
        ),
        out_specs=(
            P(None, None, None, "lat", "lon"),
            P(None, None, None, "lon", "lat"),
            P("lon", "lat", None),
        ),
        check_vma=False,
    )
```

```python
import functools

import jax
import jax.numpy as jnp
from jax import lax
from jax.experimental import pallas as pl
from jax.experimental.pallas import tpu as pltpu
from jax.sharding import PartitionSpec as P

SUB = 4
GLON_DEV = 4
PAD = 8
STEP = 32
UNSCALE = 10.0**-SUB
MESH = pl.DeviceIdType.MESH
LEFT, RIGHT, MERID, TAIL, HEAD = range(5)
NEAR, PART, WINDOW = 0, 1, 5
F32 = jnp.float32


def mix_into(products, at, fields, weights):
    wide = jnp.concatenate(fields, axis=0)
    high = wide.astype(jnp.bfloat16)
    low = (wide - high.astype(F32)).astype(jnp.bfloat16)
    out = jnp.dot(jnp.concatenate([high, low], axis=1), weights[...], preferred_element_type=F32)
    half = out.shape[1] // 2
    products[pl.ds(at, wide.shape[0]), :] = out[:, :half] + out[:, half:]


def updated(now, ahead, behind, five, product):
    c_ahead = 3.0 - five
    c_behind = 3.0 + five
    x0, x1, x2 = now
    pairs = (x0 + x1, x0 + x2, x1 + x2)
    return [
        (pairs[w] + product[w]) + (c_ahead * ahead[w] + c_behind * behind[w]) for w in range(3)
    ]


def advance(src, dst, fives, products, weights, cells, rows_dev, ends, final=False):
    rows = 3 * cells
    step = STEP
    for r in range(rows_dev):
        mix_into(
            products,
            r * rows,
            [src[w * 4 + r, pl.ds(PAD, cells), :] for w in range(3)],
            weights,
        )
    for r in range(rows_dev):
        for at in range(0, cells, step):
            now = [src[w * 4 + r, pl.ds(PAD + at, step), :] for w in range(3)]
            ahead = [src[w * 4 + r, pl.ds(PAD + at + 1, step), :] for w in range(3)]
            behind = [src[w * 4 + r, pl.ds(PAD + at - 1, step), :] for w in range(3)]
            five = fives[12 + r, pl.ds(PAD + at, step), :]
            product = [
                products[pl.ds(r * rows + w * cells + at, step), :] for w in range(3)
            ]
            new = updated(now, ahead, behind, five, product)
            for w in range(3):
                value = new[w] * UNSCALE if final else new[w]
                if ends is not None:
                    index = at + lax.broadcasted_iota(jnp.int32, (step, 128), 0)
                    kept = fives[w * 4 + r, pl.ds(PAD + at, step), :]
                    value = jnp.where(index < ends[r], value, kept)
                dst[w * 4 + r, pl.ds(PAD + at, step), :] = value


def strips_substep(src, dst, fives, products, weights, rows, step, final):
    mix_into(products, 0, [src[w, pl.ds(PAD, rows), :] for w in range(3)], weights)
    for at in range(0, rows, step):
        now = [src[w, pl.ds(PAD + at, step), :] for w in range(3)]
        ahead = [src[w, pl.ds(PAD + at + 1, step), :] for w in range(3)]
        behind = [src[w, pl.ds(PAD + at - 1, step), :] for w in range(3)]
        five = fives[3, pl.ds(PAD + at, step), :]
        product = [products[pl.ds(w * rows + at, step), :] for w in range(3)]
        new = updated(now, ahead, behind, five, product)
        for w in range(3):
            dst[w, pl.ds(PAD + at, step), :] = new[w] * UNSCALE if final else new[w]


def advance_strips(first, second, products, weights, rows, step):
    for t in range(SUB):
        src, dst = (first, second) if t % 2 == 0 else (second, first)
        strips_substep(src, dst, first, products, weights, rows, step, t == SUB - 1)


def load_state(state, field, courant, cells, rows_dev, rows):
    for r in rows:
        for w in range(3):
            at = w * rows_dev + r
            block = field[pl.ds(at, 128, stride=3 * rows_dev), :]
            state[w * 4 + r, pl.ds(PAD, cells), :] = block.T
        levels = courant[pl.ds(r, 32, stride=rows_dev), :]
        state[12 + r, pl.ds(PAD, cells), :] = jnp.concatenate([5.0 * levels] * 4, axis=0).T


def pack_ends(first, last, state, cells, rows_dev):
    for r in range(rows_dev):
        for ch in range(4):
            put = pl.ds((r % 2) * 4, 4)
            first[r // 2, ch, put, :] = state[ch * 4 + r, pl.ds(PAD, 4), :]
            last[r // 2, ch, put, :] = state[ch * 4 + r, pl.ds(PAD + cells - 4, 4), :]


def kernel(
    n, n_lat, cells, rows_dev,
    len_hbm, z_hbm, zc_hbm, own_hbm, m_hbm, mc_hbm, mix_hbm,
    zs2, ms2, co_ref, fz, seam_owner, seam_room, weights,
    len_ref, z_ref, zc_ref, own_ref, m_ref, mc_ref, mix_ref,
    zs, zs1, ms, ms1, fh, fh1, zh, zh1, products,
    z_first, z_last, z_tail, m_first, m_last,
    from_left, from_right, heads, tails_in, tail_zero, m_halo,
    z_window, w_left, w_right,
    c_left, c_right, c_from_left, c_from_right,
    sends, recvs,
    hello_side, hello_merid, hello_far,
):
    me = lax.axis_index("lon")
    lat = lax.axis_index("lat")
    right, left = lax.rem(me + 1, n), lax.rem(me + n - 1, n)
    partner = lax.rem(me + n // 2, n)
    wrap_from = n // 4 - 1
    mid = n // 2
    last = n - 1
    start = me * cells
    halves = ((z_hbm.at[:, 1], z_ref.at[:, 1]), (z_hbm.at[:, 0], z_ref.at[:, 0]))
    loads = [
        pltpu.make_async_copy(src, dst, sends.at[sem])
        for src, dst, sem in (
            (*halves[0], LEFT), (zc_hbm, zc_ref, RIGHT), (len_hbm, len_ref, TAIL),
            (*halves[1], 5), (m_hbm, m_ref, MERID), (mc_hbm, mc_ref, HEAD),
            (mix_hbm, mix_ref, 6), (own_hbm, own_ref, 7),
        )
    ]
    for load in loads:
        load.start()
    barrier = pltpu.get_barrier_semaphore()

    def greet(lon_to, lat_to):
        pl.semaphore_signal(barrier, inc=1, device_id=(lon_to, lat_to), device_id_type=MESH)

    def hello(semaphore, lon_to, lat_to):
        pl.semaphore_signal(semaphore, inc=1, device_id=(lon_to, lat_to), device_id_type=MESH)

    at_south, at_north = lat == 0, lat == n_lat - 1
    south_lon = jnp.where(at_south, partner, me)
    south_lat = jnp.where(at_south, 0, lat - 1)
    north_lon = jnp.where(at_north, partner, me)
    north_lat = jnp.where(at_north, n_lat - 1, lat + 1)
    south_slot = jnp.where(at_south, 0, 1)
    north_slot = jnp.where(at_north, 1, 0)
    is_hub, is_far, has_left, has_right = me == 0, me >= wrap_from, me > 0, me < last
    south_later = jnp.logical_and(at_south, me < mid)
    north_later = jnp.logical_or(jnp.logical_not(at_north), me < mid)
    south_earlier, north_earlier = jnp.logical_not(south_later), jnp.logical_not(north_later)

    odd = lax.rem(me, 2) == 1
    even = lax.rem(me, 2) == 0
    right_later, right_earlier = has_right & odd, has_right & even
    left_later, left_earlier = has_left & odd, has_left & even

    @pl.when(right_later)
    def _():
        greet(right, lat)

    @pl.when(left_later)
    def _():
        greet(left, lat)

    @pl.when(south_later)
    def _():
        greet(south_lon, south_lat)

    @pl.when(north_later)
    def _():
        greet(north_lon, north_lat)

    @pl.when(is_hub)
    def _():
        for j in range(wrap_from, n):
            greet(j, lat)

    one = lambda flag: jnp.where(flag, 1, 0)
    peers = (
        one(left_earlier) + one(right_earlier)
        + one(south_earlier) + one(north_earlier) + one(is_far)
    )

    @pl.when(peers > 0)
    def _():
        pl.semaphore_wait(barrier, peers)

    @pl.when(is_far)
    def _():
        hello(hello_far.at[lax.div(me, n // 4)], 0, lat)

    @pl.when(left_earlier)
    def _():
        hello(hello_side.at[1], left, lat)

    @pl.when(right_earlier)
    def _():
        hello(hello_side.at[0], right, lat)

    @pl.when(south_earlier)
    def _():
        hello(hello_merid.at[south_slot], south_lon, south_lat)

    @pl.when(north_earlier)
    def _():
        hello(hello_merid.at[north_slot], north_lon, north_lat)

    for load in loads[:2]:
        load.wait()
    def copy(src, dst, send, recv, lon_to, lat_to):
        return pltpu.make_async_remote_copy(
            src_ref=src, dst_ref=dst, send_sem=send, recv_sem=recv,
            device_id=(lon_to, lat_to), device_id_type=MESH,
        )

    def head_copy(j):
        return copy(z_first.at[1], heads.at[1], sends.at[HEAD], recvs.at[HEAD], j, lat)

    head_mid = copy(z_first.at[0], heads.at[0], sends.at[HEAD], recvs.at[HEAD], mid, lat)
    head_last = copy(z_first.at[0], heads.at[0], sends.at[HEAD], recvs.at[HEAD], last, lat)
    tail_mid = copy(z_tail.at[1], tail_zero, sends.at[TAIL], recvs.at[TAIL], 0, lat)
    tail_last = copy(z_tail.at[2], from_left.at[0], sends.at[TAIL], recvs.at[TAIL], 0, lat)

    def tail_copy(j):
        return copy(z_tail.at[0], tails_in.at[j], sends.at[TAIL], recvs.at[TAIL], 0, lat)

    to_right = copy(z_last, from_left, sends.at[RIGHT], recvs.at[NEAR], right, lat)
    to_left = copy(z_first, from_right, sends.at[LEFT], recvs.at[NEAR], left, lat)

    index8 = lax.broadcasted_iota(jnp.int32, (8, 128), 0)

    def load_rows(rows):
        load_state(zs, z_ref.reshape(m_ref.shape), zc_ref, cells, rows_dev, rows)

    def pack_tails(rows, packet):
        for r in rows:
            at = jnp.clip(lengths[r] - 4 - start, -4, cells)
            cell = lengths[r] - 4 - start + index8
            own = (cell >= 0) & (cell < cells)
            for ch in range(4):
                value = zs[ch * 4 + r, pl.ds(PAD + at, 8), :]
                z_tail[packet, ch, pl.ds((r % 2) * 4, 4), :] = jnp.where(own, value, 0.0)[:4]

    load_rows(range(2, rows_dev))
    loads[2].wait()
    lengths = [len_ref[r] for r in range(rows_dev)]
    pack_tails(range(2, rows_dev), 0)

    @pl.when(is_far)
    def _():
        tail_copy(me).start()

    loads[3].wait()
    load_rows(range(1, 2))
    pack_tails(range(1, 2), 2)

    @pl.when(me == last)
    def _():
        tail_last.start()

    load_rows(range(1))
    pack_tails(range(1), 1)
    pack_ends(z_first, z_last, zs, cells, rows_dev)

    @pl.when(me == mid)
    def _():
        tail_mid.start()

    @pl.when(left_earlier)
    def _():
        to_left.start()

    @pl.when(right_earlier)
    def _():
        to_right.start()

    for load in loads[4:6]:
        load.wait()
    load_state(ms, m_ref, mc_ref, cells, rows_dev, range(rows_dev))
    pack_ends(m_first, m_last, ms, cells, rows_dev)
    to_south = copy(
        m_first, m_halo.at[south_slot], sends.at[MERID], recvs.at[MERID], south_lon, south_lat
    )
    to_north = copy(
        m_last, m_halo.at[north_slot], sends.at[MERID], recvs.at[MERID], north_lon, north_lat
    )

    def over_poles(some):
        @pl.when(at_south & some)
        def _():
            to_south.start()

        @pl.when(at_north & some)
        def _():
            to_north.start()

    @pl.when(jnp.logical_not(at_south))
    def _():
        to_south.start()

    over_poles((me >= mid) & (me < mid + 2))

    for load in loads[6:]:
        load.wait()
    tiled = jnp.concatenate([mix_ref[...]] * 4, axis=1)
    index_of = lambda axis: lax.broadcasted_iota(jnp.int32, (128, 128), axis)
    block_of = lambda axis: index_of(axis) // 32
    matrix = jnp.where(block_of(0) == block_of(1), tiled, 0.0).T
    matrix = 10.0 * matrix + jnp.where(index_of(0) == index_of(1), 2.0, 0.0)
    w_high = matrix.astype(jnp.bfloat16)
    w_low = (matrix - w_high.astype(F32)).astype(jnp.bfloat16)
    pair = jnp.concatenate([w_high, w_low], axis=1)
    weights[pl.ds(0, 128), :] = pair
    weights[pl.ds(128, 128), :] = pair
    zeros = jnp.zeros((PAD, 128), F32)
    for slot in range(16):
        zs[slot, pl.ds(0, PAD), :] = zeros
        zs[slot, pl.ds(PAD + cells, PAD), :] = zeros
    for buf in (zh, zh1, fh, fh1, fz):
        for ch in range(3):
            buf[ch, pl.ds(0, PAD), :] = zeros
            buf[ch, pl.ds(buf.shape[1] - PAD, PAD), :] = zeros

    @pl.when(left_later)
    def _():
        pl.semaphore_wait(hello_side.at[0], 1)
        to_left.start()

    @pl.when(right_later)
    def _():
        pl.semaphore_wait(hello_side.at[1], 1)
        to_right.start()

    quarter = n // 4

    def serve(group, now):
        targets = [j for j in range(quarter * group, quarter * (group + 1)) if j >= wrap_from]

        @pl.when(is_hub & now)
        def _():
            pl.semaphore_wait(hello_far.at[group], len(targets))
            for j in targets[::2] + targets[1::2]:
                head_copy(j).start()
                if j == mid:
                    head_mid.start()
                if j == last:
                    head_last.start()

    ends = [jnp.clip(lengths[r] - start, 0, cells) for r in range(rows_dev)]
    for src, dst in ((zs, zs1), (zs1, zs2)):
        advance(src, dst, zs, products, weights, cells, rows_dev, None)
    @pl.when(jnp.logical_not(at_north))
    def _():
        pl.semaphore_wait(hello_merid.at[1], 1)
        to_north.start()

    def ready_poles(some):
        @pl.when(at_south & some)
        def _():
            pl.semaphore_wait(hello_merid.at[0], 1)

        @pl.when(at_north & some)
        def _():
            pl.semaphore_wait(hello_merid.at[1], 1)

    ready_poles((me > 1) & (me < mid))
    over_poles((me > 1) & ((me < mid) | (me >= mid + 2)))

    advance(zs2, zs1, zs, products, weights, cells, rows_dev, None)
    advance(zs1, zs2, zs, products, weights, cells, rows_dev, ends, final=True)
    always = me >= 0
    serve(0, always)
    serve(1, always)
    serve(2, lat > 0)

    first_chip = ((me == 0) & (lat > 0)) | (me == 1)
    ready_poles(first_chip)
    over_poles(first_chip)

    for r in range(rows_dev):
        owners = (own_ref[pl.ds(r, 1), :] + 1).astype(F32)
        zs[16 + r, pl.ds(PAD, cells), :] = jnp.broadcast_to(owners, (128, cells)).T
    for r in range(rows_dev):
        at = jnp.clip(lengths[r] - 8 - start, -8, cells)
        cell = lengths[r] - 8 - start + index8
        for ch in range(5):
            value = zs[ch * 4 + r, pl.ds(PAD + at, 8), :]
            z_window[r, ch, :, :] = jnp.where((cell >= 0) & (cell < cells), value, 0.0)
    moving = z_window.at[pl.ds(2, rows_dev - 2)]
    window_left = copy(moving, w_right, sends.at[LEFT], recvs.at[WINDOW], left, lat)
    window_right = copy(moving, w_left, sends.at[RIGHT], recvs.at[WINDOW], right, lat)

    far_left, far_right = me > wrap_from, is_far & has_right

    @pl.when(far_left)
    def _():
        window_left.start()

    @pl.when(far_right)
    def _():
        window_right.start()

    first_partials = lax.rem(me, 4) == 2

    def merid_begin(some):
        @pl.when(some)
        def _():
            for src, dst in ((ms, ms1), (ms1, ms2)):
                advance(src, dst, ms, products, weights, cells, rows_dev, None)

    merid_begin(jnp.logical_not(first_partials))

    def fill_left():
        for r in range(rows_dev):
            take = pl.ds((r % 2) * 4, 4)
            for ch in range(4):
                zs[ch * 4 + r, pl.ds(PAD - 4, 4), :] = from_left[r // 2, ch, take, :]

    def fill_right():
        for r in range(rows_dev):
            take = pl.ds((r % 2) * 4, 4)
            for ch in range(4):
                zs[ch * 4 + r, pl.ds(PAD + cells, 4), :] = from_right[r // 2, ch, take, :]

    index4 = lax.broadcasted_iota(jnp.int32, (4, 128), 0)

    scale = GLON_DEV / (3.0 * cells)
    near = me * GLON_DEV - 1 + lax.broadcasted_iota(jnp.int32, (8, cells), 0)
    lane = lax.broadcasted_iota(jnp.int32, (8, cells), 1)

    first_late = jnp.where(is_hub, 4, 0)

    def column_terms(r):
        body = pl.ds(PAD, cells)
        before = zs[r, body, :] + zs[4 + r, body, :] + zs[8 + r, body, :]
        after = zs2[r, body, :] + zs2[4 + r, body, :] + zs2[8 + r, body, :]
        delta = (after - before) * scale
        high = delta.astype(jnp.bfloat16)
        low = (delta - high.astype(F32)).astype(jnp.bfloat16)
        to_end = lane - (lengths[r] - start)
        early = ((to_end < -4) | (to_end >= 0)) & (lane >= first_late)
        table = ((own_ref[pl.ds(r, 1), :] == near) & early).astype(jnp.bfloat16)
        both = jnp.dot(
            table, jnp.concatenate([high, low], axis=1), preferred_element_type=F32
        )
        half = both.shape[1] // 2
        return both[:, :half] + both[:, half:]

    part_left = copy(c_left, c_from_right, sends.at[LEFT], recvs.at[PART], left, lat)
    part_right = copy(c_right, c_from_left, sends.at[RIGHT], recvs.at[PART], right, lat)

    def transfers(count, sem):
        lines = products.at[pl.ds(0, count)]
        return copy(lines, lines, sends.at[sem], recvs.at[sem], partner, lat)

    ends_here = (me == mid) | (me == last)
    plain_far = is_far & jnp.logical_not(ends_here)
    all_tails = (n - wrap_from + 2) * 32

    def beside(count, sem, from_left, from_right):
        @pl.when(from_left & from_right)
        def _():
            transfers(2 * count, sem).wait_recv()

        @pl.when(jnp.logical_xor(from_left, from_right))
        def _():
            transfers(count, sem).wait_recv()

    beside(64, NEAR, has_left, has_right)

    @pl.when(has_left)
    def _():
        fill_left()

    @pl.when(has_right)
    def _():
        fill_right()

    for r in range(rows_dev):
        for ch in range(4):
            base = PAD + r * 24
            zh[ch, pl.ds(base, 12), :] = zs[ch * 4 + r, pl.ds(PAD - 4, 12), :]
            zh[ch, pl.ds(base + 12, 12), :] = zs[ch * 4 + r, pl.ds(PAD + cells - 8, 12), :]
    advance_strips(zh, zh1, products, weights, 24 * rows_dev, 48)
    for r in range(rows_dev):
        base = PAD + r * 24
        for w in range(3):
            for cell, take in ((0, base + 4), (cells - 4, base + 16)):
                old = zs2[w * 4 + r, pl.ds(PAD + cell, 4), :]
                zs2[w * 4 + r, pl.ds(PAD + cell, 4), :] = jnp.where(
                    index4 + cell < ends[r], zh[w, pl.ds(take, 4), :], old
                )
    for r in range(rows_dev):
        terms = column_terms(r)
        c_left[pl.ds(r, 1), :] = terms[0:1]
        c_right[pl.ds(r, 1), :] = terms[GLON_DEV + 1 : GLON_DEV + 2]
        for g in range(GLON_DEV):
            co_ref[g, pl.ds(r, 1), :] = terms[g + 1 : g + 2]

    @pl.when(has_left)
    def _():
        part_left.start()

    @pl.when(has_right)
    def _():
        part_right.start()

    merid_begin(first_partials)
    serve(2, at_south)
    serve(3, lat > 0)
    ready_poles(is_hub & at_south)
    over_poles(is_hub & at_south)

    serve(3, at_south)

    for src, dst in ((ms2, ms1), (ms1, ms2)):
        advance(src, dst, ms, products, weights, cells, rows_dev, None, final=dst is ms2)
    transfers(128, MERID).wait_recv()

    for r in range(rows_dev):
        take = (r % 2) * 4
        for ch in range(4):
            turned = ch if ch == 3 else 2 - ch
            sign = -1.0 if ch == 3 else 1.0
            base = PAD + r * 24
            for j in range(4):
                plain = m_halo[0, r // 2, ch, pl.ds(take + j, 1), :]
                pole = sign * m_halo[0, r // 2, turned, pl.ds(take + 3 - j, 1), :]
                fh[ch, pl.ds(base + j, 1), :] = jnp.where(at_south, pole, plain)
                plain = m_halo[1, r // 2, ch, pl.ds(take + j, 1), :]
                pole = sign * m_halo[1, r // 2, turned, pl.ds(take + 3 - j, 1), :]
                fh[ch, pl.ds(base + 20 + j, 1), :] = jnp.where(at_north, pole, plain)
            fh[ch, pl.ds(base + 4, 8), :] = ms[ch * 4 + r, pl.ds(PAD, 8), :]
            fh[ch, pl.ds(base + 12, 8), :] = ms[ch * 4 + r, pl.ds(PAD + cells - 8, 8), :]

    advance_strips(fh, fh1, products, weights, 24 * rows_dev, 48)
    for r in range(rows_dev):
        for w in range(3):
            at, base = w * 4 + r, PAD + r * 24
            ms2[at, pl.ds(PAD, 4), :] = fh[w, pl.ds(base + 4, 4), :]
            ms2[at, pl.ds(PAD + cells - 4, 4), :] = fh[w, pl.ds(base + 16, 4), :]

    @pl.when(plain_far)
    def _():
        transfers(32, HEAD).wait_recv()

    @pl.when(ends_here)
    def _():
        transfers(64, HEAD).wait_recv()

    beside((rows_dev - 2) * 40, WINDOW, far_left, far_right)

    @pl.when(is_hub)
    def _():
        transfers(all_tails, TAIL).wait_recv()

    own_base = (me * GLON_DEV + 1).astype(F32)
    for r in range(rows_dev):
        end = jnp.where(is_hub, 4, lengths[r] - start)
        seam_room[r, :, :] = jnp.full((8, 128), end, jnp.int32).astype(F32)

    @pl.when(is_hub)
    def _():
        for ch in range(4):
            total = tails_in[wrap_from, ch]
            for j in range(wrap_from + 1, n):
                total = total + tails_in[j, ch]
            fz[ch, pl.ds(PAD, 4), :] = tail_zero[ch, pl.ds(0, 4), :]
            fz[ch, pl.ds(PAD + 12, 4), :] = from_left[0, ch, pl.ds(4, 4), :]
            for r in range(2, rows_dev):
                half = (r % 2) * 4
                fz[ch, pl.ds(PAD + 12 * r, 4), :] = total[half : half + 4]
            for r in range(rows_dev):
                fz[ch, pl.ds(PAD + 12 * r + 4, 8), :] = zs[ch * 4 + r, pl.ds(PAD, 8), :]
        for r in range(rows_dev):
            seam_owner[r, :, :] = zs[16 + r, pl.ds(PAD, 8), :] - own_base

    @pl.when(has_left)
    def _():
        for r in range(rows_dev):
            for ch in range(5):
                window = z_window[r, ch]
                if r >= 2:
                    window = window + jnp.where(far_left, w_left[r - 2, ch], 0.0)
                    window = window + jnp.where(far_right, w_right[r - 2, ch], 0.0)
                if ch == 4:
                    seam_owner[r, pl.ds(0, 4), :] = window[4:8] - own_base
                    continue
                base = PAD + 12 * r
                fz[ch, pl.ds(base, 8), :] = window
                fz[ch, pl.ds(base + 8, 4), :] = heads[r // 2, ch, pl.ds((r % 2) * 4, 4), :]

    beside(8, PART, has_left, has_right)

    @pl.when(has_left)
    def _():
        for r in range(rows_dev):
            co_ref[0, pl.ds(r, 1), :] += c_from_left[pl.ds(r, 1), :]

    @pl.when(has_right)
    def _():
        for r in range(rows_dev):
            co_ref[GLON_DEV - 1, pl.ds(r, 1), :] += c_from_right[pl.ds(r, 1), :]

    moved = (rows_dev - 2) * 40
    transfers(128, MERID).wait_send()
    for flag, count, sem in (
        (far_left, 72 + moved, LEFT),
        (has_left & jnp.logical_not(far_left), 72, LEFT),
        (far_right, 72 + moved, RIGHT),
        (has_right & jnp.logical_not(far_right), 72, RIGHT),
        (plain_far, 32, TAIL),
        (ends_here, 64, TAIL),
        (is_hub, all_tails, HEAD),
    ):

        @pl.when(flag)
        def _():
            transfers(count, sem).wait_send()


def finish(
    cells, rows_dev,
    zs, ms, co_in, fz, seam_owner, seam_room, weights,
    zo_hbm, mo_hbm, co_hbm,
    zo, mo, co, f1, f2, products, sems,
):
    rows = 12 * rows_dev
    index8 = lax.broadcasted_iota(jnp.int32, (8, 128), 0)
    copies = []

    def write(blocks, staged, out, w, sem):
        lines = staged.at[w].reshape(128 * rows_dev, cells)
        for r in range(rows_dev):
            lines[pl.ds(r, 128, stride=rows_dev), :] = blocks(w, r).T
        copies.append(pltpu.make_async_copy(staged.at[w], out.at[:, w], sems.at[sem]))
        copies[-1].start()

    def wanted(strips, r):
        at = pl.ds(PAD + 12 * r + 4, 4)
        return strips[0, at, :] + strips[1, at, :] + strips[2, at, :]

    for buf in (f1, f2):
        for ch in range(3):
            buf[ch, pl.ds(0, PAD), :] = jnp.zeros((PAD, 128), F32)
            buf[ch, pl.ds(PAD + rows, PAD), :] = jnp.zeros((PAD, 128), F32)
    rooms = [jnp.max(seam_room[r]).astype(jnp.int32) for r in range(rows_dev)]
    merid = lambda w, r: ms[w * 4 + r, pl.ds(PAD, cells), :]
    for t, (src, dst) in enumerate(((fz, f1), (f1, f2), (f2, f1), (f1, f2))):
        strips_substep(src, dst, fz, products, weights, rows, 48, t == SUB - 1)
        if t < 3:
            write(merid, mo, mo_hbm, t, t)

    def zonal(w, r):
        parts = []
        for block in range(0, cells, 8):
            ahead = block - rooms[r]
            inside = (index8 + ahead >= -4) & (index8 + ahead < 0)
            take = PAD + 12 * r + 8 + jnp.clip(ahead, -12, 0)
            old = zs[w * 4 + r, pl.ds(PAD + block, 8), :]
            parts.append(jnp.where(inside, f2[w, pl.ds(take, 8), :], old))
        return jnp.concatenate(parts, axis=0)

    for w in range(3):
        write(zonal, zo, zo_hbm, w, 3 + w)
    scale = GLON_DEV / (3.0 * cells)
    for r in range(rows_dev):
        delta = (wanted(f2, r) - wanted(fz, r)) * scale
        owner = seam_owner[r, pl.ds(0, 4), :]
        for g in range(GLON_DEV):
            mine = jnp.where(owner == float(g), delta, 0.0)
            co[g, pl.ds(r, 1), :] = co_in[g, pl.ds(r, 1), :] + jnp.sum(
                mine, axis=0, keepdims=True
            )
    copies.append(pltpu.make_async_copy(co, co_hbm, sems.at[6]))
    copies[-1].start()
    for done in copies:
        done.wait()


def solution(mesh):
    n, n_lat = mesh.shape["lon"], mesh.shape["lat"]

    def shards(
        zonal_state, zonal_courant, zonal_length, zonal_owner, merid_state, merid_courant, mixing
    ):
        nv, lev, wid, rows_dev, cells = zonal_state.shape
        flat = nv * lev * wid * rows_dev
        vmem = pl.BlockSpec(memory_space=pltpu.VMEM)
        hbm = pl.BlockSpec(memory_space=pltpu.HBM)
        shape = jax.ShapeDtypeStruct
        state = (16, cells + 2 * PAD, 128)
        strips = (4, 24 * rows_dev + 2 * PAD, 128)
        seam = (4, 12 * rows_dev + 2 * PAD, 128)
        packet = pltpu.VMEM((2, 4, 8, 128), F32)
        small = pltpu.VMEM((8, 128), F32)
        products = pltpu.VMEM((rows_dev * 3 * cells, 128), F32)
        dma = pltpu.SemaphoreType.DMA
        regular = pltpu.SemaphoreType.REGULAR
        held = pl.pallas_call(
            functools.partial(kernel, n, n_lat, cells, rows_dev),
            out_shape=(
                shape(state, F32), shape(state, F32),
                shape((GLON_DEV, rows_dev, nv * lev), F32),
                shape(seam, F32),
                shape((rows_dev, 8, 128), F32), shape((rows_dev, 8, 128), F32),
                shape((256, 256), jnp.bfloat16),
            ),
            in_specs=[hbm] * 7,
            out_specs=(vmem,) * 7,
            scratch_shapes=[
                pltpu.SMEM((rows_dev,), jnp.int32),
                pltpu.VMEM((nv * lev * wid, 2, rows_dev // 2, cells), F32),
                pltpu.VMEM((lev * rows_dev, cells), F32),
                pltpu.VMEM((rows_dev, cells), jnp.int32),
                pltpu.VMEM((flat, cells), F32),
                pltpu.VMEM((lev * rows_dev, cells), F32),
                pltpu.VMEM((nv * lev, lev), F32),
                pltpu.VMEM((20, *state[1:]), F32), pltpu.VMEM(state, F32),
                pltpu.VMEM(state, F32), pltpu.VMEM(state, F32),
                pltpu.VMEM(strips, F32),
                pltpu.VMEM(strips, F32),
                pltpu.VMEM(strips, F32), pltpu.VMEM(strips, F32),
                products,
                packet, packet, pltpu.VMEM((3, 4, 8, 128), F32), packet, packet,
                packet, packet, packet,
                pltpu.VMEM((n, 4, 8, 128), F32),
                pltpu.VMEM((4, 8, 128), F32),
                pltpu.VMEM((2, 2, 4, 8, 128), F32),
                pltpu.VMEM((rows_dev, 5, 8, 128), F32),
                pltpu.VMEM((rows_dev - 2, 5, 8, 128), F32),
                pltpu.VMEM((rows_dev - 2, 5, 8, 128), F32),
                small, small, small, small,
                dma((8,)), dma((6,)),
                regular((2,)), regular((2,)), regular((4,)),
            ],
            compiler_params=pltpu.CompilerParams(
                collective_id=0, has_side_effects=True, vmem_limit_bytes=48 * 1024 * 1024
            ),
        )(
            *(
                pltpu.with_memory_space_constraint(value, pltpu.HBM)
                for value in (
                    zonal_length,
                    zonal_state.reshape(nv * lev * wid, 2, rows_dev // 2, cells),
                    zonal_courant.reshape(lev * rows_dev, cells),
                    zonal_owner,
                    merid_state.reshape(flat, cells),
                    merid_courant.reshape(lev * rows_dev, cells),
                    mixing.reshape(nv * lev, lev),
                )
            )
        )
        zo, mo, co = pl.pallas_call(
            functools.partial(finish, cells, rows_dev),
            out_shape=(
                shape((nv * lev, wid, rows_dev, cells), F32),
                shape((nv * lev, wid, rows_dev, cells), F32),
                shape((GLON_DEV, rows_dev, nv * lev), F32),
            ),
            in_specs=[vmem] * 7,
            out_specs=(hbm,) * 3,
            scratch_shapes=[
                pltpu.VMEM((wid, nv * lev, rows_dev, cells), F32),
                pltpu.VMEM((wid, nv * lev, rows_dev, cells), F32),
                pltpu.VMEM((GLON_DEV, rows_dev, nv * lev), F32),
                pltpu.VMEM(seam, F32), pltpu.VMEM(seam, F32), products, dma((7,)),
            ],
            compiler_params=pltpu.CompilerParams(vmem_limit_bytes=40 * 1024 * 1024),
        )(*held)
        return zo.reshape(zonal_state.shape), mo.reshape(merid_state.shape), co

    return jax.shard_map(
        shards,
        mesh=mesh,
        in_specs=(
            P(None, None, None, "lat", "lon"),
            P(None, "lat", "lon"),
            P("lat"),
            P("lat", "lon"),
            P(None, None, None, "lon", "lat"),
            P(None, "lon", "lat"),
            P(),
        ),
        out_specs=(
            P(None, None, None, "lat", "lon"),
            P(None, None, None, "lon", "lat"),
            P("lon", "lat", None),
        ),
        check_vma=False,
    )
```

```python
import functools

import jax
import jax.numpy as jnp
from jax import lax
from jax.experimental import pallas as pl
from jax.experimental.pallas import tpu as pltpu
from jax.sharding import PartitionSpec as P

SUB = 4
GLON_DEV = 4
PAD = 8
STEP = 32
UNSCALE = 10.0**-SUB
MESH = pl.DeviceIdType.MESH
LEFT, RIGHT, MERID, TAIL, HEAD = range(5)
NEAR, PART, WINDOW = 0, 1, 5
F32 = jnp.float32


def mix_into(products, at, fields, weights):
    wide = jnp.concatenate(fields, axis=0)
    high = wide.astype(jnp.bfloat16)
    low = (wide - high.astype(F32)).astype(jnp.bfloat16)
    out = jnp.dot(jnp.concatenate([high, low], axis=1), weights[...], preferred_element_type=F32)
    half = out.shape[1] // 2
    products[pl.ds(at, wide.shape[0]), :] = out[:, :half] + out[:, half:]


def updated(now, ahead, behind, five, product):
    c_ahead = 3.0 - five
    c_behind = 3.0 + five
    x0, x1, x2 = now
    pairs = (x0 + x1, x0 + x2, x1 + x2)
    return [
        (pairs[w] + product[w]) + (c_ahead * ahead[w] + c_behind * behind[w]) for w in range(3)
    ]


def advance(src, dst, fives, products, weights, cells, rows_dev, ends, final=False):
    rows = 3 * cells
    step = STEP
    for r in range(rows_dev):
        mix_into(
            products,
            r * rows,
            [src[w * 4 + r, pl.ds(PAD, cells), :] for w in range(3)],
            weights,
        )
    for r in range(rows_dev):
        for at in range(0, cells, step):
            now = [src[w * 4 + r, pl.ds(PAD + at, step), :] for w in range(3)]
            ahead = [src[w * 4 + r, pl.ds(PAD + at + 1, step), :] for w in range(3)]
            behind = [src[w * 4 + r, pl.ds(PAD + at - 1, step), :] for w in range(3)]
            five = fives[12 + r, pl.ds(PAD + at, step), :]
            product = [
                products[pl.ds(r * rows + w * cells + at, step), :] for w in range(3)
            ]
            new = updated(now, ahead, behind, five, product)
            for w in range(3):
                value = new[w] * UNSCALE if final else new[w]
                if ends is not None:
                    index = at + lax.broadcasted_iota(jnp.int32, (step, 128), 0)
                    kept = fives[w * 4 + r, pl.ds(PAD + at, step), :]
                    value = jnp.where(index < ends[r], value, kept)
                dst[w * 4 + r, pl.ds(PAD + at, step), :] = value


def strips_substep(src, dst, fives, products, weights, rows, step, final):
    mix_into(products, 0, [src[w, pl.ds(PAD, rows), :] for w in range(3)], weights)
    for at in range(0, rows, step):
        now = [src[w, pl.ds(PAD + at, step), :] for w in range(3)]
        ahead = [src[w, pl.ds(PAD + at + 1, step), :] for w in range(3)]
        behind = [src[w, pl.ds(PAD + at - 1, step), :] for w in range(3)]
        five = fives[3, pl.ds(PAD + at, step), :]
        product = [products[pl.ds(w * rows + at, step), :] for w in range(3)]
        new = updated(now, ahead, behind, five, product)
        for w in range(3):
            dst[w, pl.ds(PAD + at, step), :] = new[w] * UNSCALE if final else new[w]


def advance_strips(first, second, products, weights, rows, step):
    for t in range(SUB):
        src, dst = (first, second) if t % 2 == 0 else (second, first)
        strips_substep(src, dst, first, products, weights, rows, step, t == SUB - 1)


def load_state(state, field, courant, cells, rows_dev, rows):
    for r in rows:
        for w in range(3):
            at = w * rows_dev + r
            block = field[pl.ds(at, 128, stride=3 * rows_dev), :]
            state[w * 4 + r, pl.ds(PAD, cells), :] = block.T
        levels = courant[pl.ds(r, 32, stride=rows_dev), :]
        state[12 + r, pl.ds(PAD, cells), :] = jnp.concatenate([5.0 * levels] * 4, axis=0).T


def pack_ends(first, last, state, cells, rows_dev):
    for r in range(rows_dev):
        for ch in range(4):
            put = pl.ds((r % 2) * 4, 4)
            first[r // 2, ch, put, :] = state[ch * 4 + r, pl.ds(PAD, 4), :]
            last[r // 2, ch, put, :] = state[ch * 4 + r, pl.ds(PAD + cells - 4, 4), :]


def kernel(
    n, n_lat, cells, rows_dev,
    len_hbm, z_hbm, zc_hbm, own_hbm, m_hbm, mc_hbm, mix_hbm,
    zs2, ms2, co_ref, fz, seam_owner, seam_room, weights,
    len_ref, z_ref, zc_ref, own_ref, m_ref, mc_ref, mix_ref,
    zs, zs1, ms, ms1, fh, fh1, zh, zh1, products,
    z_first, z_last, z_tail, m_first, m_last,
    from_left, from_right, heads, tails_in, tail_zero, m_halo,
    z_window, w_left, w_right,
    c_left, c_right, c_from_left, c_from_right,
    sends, recvs,
    hello_side, hello_merid, hello_far,
):
    me = lax.axis_index("lon")
    lat = lax.axis_index("lat")
    right, left = lax.rem(me + 1, n), lax.rem(me + n - 1, n)
    partner = lax.rem(me + n // 2, n)
    wrap_from = n // 4 - 1
    mid = n // 2
    last = n - 1
    start = me * cells
    halves = ((z_hbm.at[:, 1], z_ref.at[:, 1]), (z_hbm.at[:, 0], z_ref.at[:, 0]))
    loads = [
        pltpu.make_async_copy(src, dst, sends.at[sem])
        for src, dst, sem in (
            (*halves[0], LEFT), (zc_hbm, zc_ref, RIGHT), (len_hbm, len_ref, TAIL),
            (*halves[1], 5), (m_hbm, m_ref, MERID), (mc_hbm, mc_ref, HEAD),
            (mix_hbm, mix_ref, 6), (own_hbm, own_ref, 7),
        )
    ]
    for load in loads:
        load.start()
    barrier = pltpu.get_barrier_semaphore()

    def greet(lon_to, lat_to):
        pl.semaphore_signal(barrier, inc=1, device_id=(lon_to, lat_to), device_id_type=MESH)

    def hello(semaphore, lon_to, lat_to):
        pl.semaphore_signal(semaphore, inc=1, device_id=(lon_to, lat_to), device_id_type=MESH)

    at_south, at_north = lat == 0, lat == n_lat - 1
    south_lon = jnp.where(at_south, partner, me)
    south_lat = jnp.where(at_south, 0, lat - 1)
    north_lon = jnp.where(at_north, partner, me)
    north_lat = jnp.where(at_north, n_lat - 1, lat + 1)
    south_slot = jnp.where(at_south, 0, 1)
    north_slot = jnp.where(at_north, 1, 0)
    is_hub, is_far, has_left, has_right = me == 0, me >= wrap_from, me > 0, me < last
    south_later = jnp.logical_and(at_south, me < mid)
    north_later = jnp.logical_or(jnp.logical_not(at_north), me < mid)
    south_earlier, north_earlier = jnp.logical_not(south_later), jnp.logical_not(north_later)

    odd = lax.rem(me, 2) == 1
    even = lax.rem(me, 2) == 0
    right_later, right_earlier = has_right & odd, has_right & even
    left_later, left_earlier = has_left & odd, has_left & even

    @pl.when(right_later)
    def _():
        greet(right, lat)

    @pl.when(left_later)
    def _():
        greet(left, lat)

    @pl.when(south_later)
    def _():
        greet(south_lon, south_lat)

    @pl.when(north_later)
    def _():
        greet(north_lon, north_lat)

    @pl.when(is_hub)
    def _():
        for j in range(wrap_from, n):
            greet(j, lat)

    one = lambda flag: jnp.where(flag, 1, 0)
    peers = (
        one(left_earlier) + one(right_earlier)
        + one(south_earlier) + one(north_earlier) + one(is_far)
    )

    @pl.when(peers > 0)
    def _():
        pl.semaphore_wait(barrier, peers)

    @pl.when(is_far)
    def _():
        hello(hello_far.at[lax.div(me, n // 4)], 0, lat)

    @pl.when(left_earlier)
    def _():
        hello(hello_side.at[1], left, lat)

    @pl.when(right_earlier)
    def _():
        hello(hello_side.at[0], right, lat)

    @pl.when(south_earlier)
    def _():
        hello(hello_merid.at[south_slot], south_lon, south_lat)

    @pl.when(north_earlier)
    def _():
        hello(hello_merid.at[north_slot], north_lon, north_lat)

    for load in loads[:2]:
        load.wait()
    def copy(src, dst, send, recv, lon_to, lat_to):
        return pltpu.make_async_remote_copy(
            src_ref=src, dst_ref=dst, send_sem=send, recv_sem=recv,
            device_id=(lon_to, lat_to), device_id_type=MESH,
        )

    def head_copy(j):
        return copy(z_first.at[1], heads.at[1], sends.at[HEAD], recvs.at[HEAD], j, lat)

    head_mid = copy(z_first.at[0], heads.at[0], sends.at[HEAD], recvs.at[HEAD], mid, lat)
    head_last = copy(z_first.at[0], heads.at[0], sends.at[HEAD], recvs.at[HEAD], last, lat)
    tail_mid = copy(z_tail.at[1], tail_zero, sends.at[TAIL], recvs.at[TAIL], 0, lat)
    tail_last = copy(z_tail.at[2], from_left.at[0], sends.at[TAIL], recvs.at[TAIL], 0, lat)

    def tail_copy(j):
        return copy(z_tail.at[0], tails_in.at[j], sends.at[TAIL], recvs.at[TAIL], 0, lat)

    to_right = copy(z_last, from_left, sends.at[RIGHT], recvs.at[NEAR], right, lat)
    to_left = copy(z_first, from_right, sends.at[LEFT], recvs.at[NEAR], left, lat)

    index8 = lax.broadcasted_iota(jnp.int32, (8, 128), 0)

    def load_rows(rows):
        load_state(zs, z_ref.reshape(m_ref.shape), zc_ref, cells, rows_dev, rows)

    def pack_tails(rows, packet):
        for r in rows:
            at = jnp.clip(lengths[r] - 4 - start, -4, cells)
            cell = lengths[r] - 4 - start + index8
            own = (cell >= 0) & (cell < cells)
            for ch in range(4):
                value = zs[ch * 4 + r, pl.ds(PAD + at, 8), :]
                z_tail[packet, ch, pl.ds((r % 2) * 4, 4), :] = jnp.where(own, value, 0.0)[:4]

    load_rows(range(2, rows_dev))
    loads[2].wait()
    lengths = [len_ref[r] for r in range(rows_dev)]
    pack_tails(range(2, rows_dev), 0)

    @pl.when(is_far)
    def _():
        tail_copy(me).start()

    loads[3].wait()
    load_rows(range(1, 2))
    pack_tails(range(1, 2), 2)

    @pl.when(me == last)
    def _():
        tail_last.start()

    load_rows(range(1))
    pack_tails(range(1), 1)
    pack_ends(z_first, z_last, zs, cells, rows_dev)

    @pl.when(me == mid)
    def _():
        tail_mid.start()

    @pl.when(left_earlier)
    def _():
        to_left.start()

    @pl.when(right_earlier)
    def _():
        to_right.start()

    for load in loads[4:6]:
        load.wait()
    load_state(ms, m_ref, mc_ref, cells, rows_dev, range(rows_dev))
    pack_ends(m_first, m_last, ms, cells, rows_dev)
    to_south = copy(
        m_first, m_halo.at[south_slot], sends.at[MERID], recvs.at[MERID], south_lon, south_lat
    )
    to_north = copy(
        m_last, m_halo.at[north_slot], sends.at[MERID], recvs.at[MERID], north_lon, north_lat
    )

    def over_poles(some):
        @pl.when(at_south & some)
        def _():
            to_south.start()

        @pl.when(at_north & some)
        def _():
            to_north.start()

    @pl.when(jnp.logical_not(at_south))
    def _():
        to_south.start()

    over_poles((me >= mid) & (me < mid + 2))

    for load in loads[6:]:
        load.wait()
    tiled = jnp.concatenate([mix_ref[...]] * 4, axis=1)
    index_of = lambda axis: lax.broadcasted_iota(jnp.int32, (128, 128), axis)
    block_of = lambda axis: index_of(axis) // 32
    matrix = jnp.where(block_of(0) == block_of(1), tiled, 0.0).T
    matrix = 10.0 * matrix + jnp.where(index_of(0) == index_of(1), 2.0, 0.0)
    w_high = matrix.astype(jnp.bfloat16)
    w_low = (matrix - w_high.astype(F32)).astype(jnp.bfloat16)
    pair = jnp.concatenate([w_high, w_low], axis=1)
    weights[pl.ds(0, 128), :] = pair
    weights[pl.ds(128, 128), :] = pair
    zeros = jnp.zeros((PAD, 128), F32)
    for slot in range(16):
        zs[slot, pl.ds(0, PAD), :] = zeros
        zs[slot, pl.ds(PAD + cells, PAD), :] = zeros
    for buf in (zh, zh1, fh, fh1, fz):
        for ch in range(3):
            buf[ch, pl.ds(0, PAD), :] = zeros
            buf[ch, pl.ds(buf.shape[1] - PAD, PAD), :] = zeros

    @pl.when(left_later)
    def _():
        pl.semaphore_wait(hello_side.at[0], 1)
        to_left.start()

    @pl.when(right_later)
    def _():
        pl.semaphore_wait(hello_side.at[1], 1)
        to_right.start()

    quarter = n // 4

    def serve(group, now):
        targets = [j for j in range(quarter * group, quarter * (group + 1)) if j >= wrap_from]

        @pl.when(is_hub & now)
        def _():
            pl.semaphore_wait(hello_far.at[group], len(targets))
            for j in targets[::2] + targets[1::2]:
                head_copy(j).start()
                if j == mid:
                    head_mid.start()
                if j == last:
                    head_last.start()

    ends = [jnp.clip(lengths[r] - start, 0, cells) for r in range(rows_dev)]
    for src, dst in ((zs, zs1), (zs1, zs2)):
        advance(src, dst, zs, products, weights, cells, rows_dev, None)
    @pl.when(jnp.logical_not(at_north))
    def _():
        pl.semaphore_wait(hello_merid.at[1], 1)
        to_north.start()

    def ready_poles(some):
        @pl.when(at_south & some)
        def _():
            pl.semaphore_wait(hello_merid.at[0], 1)

        @pl.when(at_north & some)
        def _():
            pl.semaphore_wait(hello_merid.at[1], 1)

    ready_poles((me > 1) & (me < mid))
    over_poles((me > 1) & ((me < mid) | (me >= mid + 2)))

    advance(zs2, zs1, zs, products, weights, cells, rows_dev, None)
    advance(zs1, zs2, zs, products, weights, cells, rows_dev, ends, final=True)
    always = me >= 0
    serve(0, always)
    serve(1, always)
    serve(2, lat > 0)

    first_chip = ((me == 0) & (lat > 0)) | (me == 1)
    ready_poles(first_chip)
    over_poles(first_chip)

    for r in range(rows_dev):
        owners = (own_ref[pl.ds(r, 1), :] + 1).astype(F32)
        zs[16 + r, pl.ds(PAD, cells), :] = jnp.broadcast_to(owners, (128, cells)).T
    for r in range(rows_dev):
        at = jnp.clip(lengths[r] - 8 - start, -8, cells)
        cell = lengths[r] - 8 - start + index8
        for ch in range(5):
            value = zs[ch * 4 + r, pl.ds(PAD + at, 8), :]
            z_window[r, ch, :, :] = jnp.where((cell >= 0) & (cell < cells), value, 0.0)
    moving = z_window.at[pl.ds(2, rows_dev - 2)]
    window_left = copy(moving, w_right, sends.at[LEFT], recvs.at[WINDOW], left, lat)
    window_right = copy(moving, w_left, sends.at[RIGHT], recvs.at[WINDOW], right, lat)

    far_left, far_right = me > wrap_from, is_far & has_right

    @pl.when(far_left)
    def _():
        window_left.start()

    @pl.when(far_right)
    def _():
        window_right.start()

    first_partials = lax.rem(me, 4) == 2

    def merid_begin(some):
        @pl.when(some)
        def _():
            for src, dst in ((ms, ms1), (ms1, ms2)):
                advance(src, dst, ms, products, weights, cells, rows_dev, None)

    merid_begin(jnp.logical_not(first_partials))

    def fill_left():
        for r in range(rows_dev):
            take = pl.ds((r % 2) * 4, 4)
            for ch in range(4):
                zs[ch * 4 + r, pl.ds(PAD - 4, 4), :] = from_left[r // 2, ch, take, :]

    def fill_right():
        for r in range(rows_dev):
            take = pl.ds((r % 2) * 4, 4)
            for ch in range(4):
                zs[ch * 4 + r, pl.ds(PAD + cells, 4), :] = from_right[r // 2, ch, take, :]

    index4 = lax.broadcasted_iota(jnp.int32, (4, 128), 0)

    scale = GLON_DEV / (3.0 * cells)
    near = me * GLON_DEV - 1 + lax.broadcasted_iota(jnp.int32, (8, cells), 0)
    lane = lax.broadcasted_iota(jnp.int32, (8, cells), 1)

    first_late = jnp.where(is_hub, 4, 0)

    def column_terms(r):
        body = pl.ds(PAD, cells)
        before = zs[r, body, :] + zs[4 + r, body, :] + zs[8 + r, body, :]
        after = zs2[r, body, :] + zs2[4 + r, body, :] + zs2[8 + r, body, :]
        delta = (after - before) * scale
        high = delta.astype(jnp.bfloat16)
        low = (delta - high.astype(F32)).astype(jnp.bfloat16)
        to_end = lane - (lengths[r] - start)
        early = ((to_end < -4) | (to_end >= 0)) & (lane >= first_late)
        table = ((own_ref[pl.ds(r, 1), :] == near) & early).astype(jnp.bfloat16)
        both = jnp.dot(
            table, jnp.concatenate([high, low], axis=1), preferred_element_type=F32
        )
        half = both.shape[1] // 2
        return both[:, :half] + both[:, half:]

    part_left = copy(c_left, c_from_right, sends.at[LEFT], recvs.at[PART], left, lat)
    part_right = copy(c_right, c_from_left, sends.at[RIGHT], recvs.at[PART], right, lat)

    def transfers(count, sem):
        lines = products.at[pl.ds(0, count)]
        return copy(lines, lines, sends.at[sem], recvs.at[sem], partner, lat)

    ends_here = (me == mid) | (me == last)
    plain_far = is_far & jnp.logical_not(ends_here)
    all_tails = (n - wrap_from + 2) * 32

    def beside(count, sem, from_left, from_right):
        @pl.when(from_left & from_right)
        def _():
            transfers(2 * count, sem).wait_recv()

        @pl.when(jnp.logical_xor(from_left, from_right))
        def _():
            transfers(count, sem).wait_recv()

    beside(64, NEAR, has_left, has_right)

    @pl.when(has_left)
    def _():
        fill_left()

    @pl.when(has_right)
    def _():
        fill_right()

    for r in range(rows_dev):
        for ch in range(4):
            base = PAD + r * 24
            zh[ch, pl.ds(base, 12), :] = zs[ch * 4 + r, pl.ds(PAD - 4, 12), :]
            zh[ch, pl.ds(base + 12, 12), :] = zs[ch * 4 + r, pl.ds(PAD + cells - 8, 12), :]
    advance_strips(zh, zh1, products, weights, 24 * rows_dev, 48)
    for r in range(rows_dev):
        base = PAD + r * 24
        for w in range(3):
            for cell, take in ((0, base + 4), (cells - 4, base + 16)):
                old = zs2[w * 4 + r, pl.ds(PAD + cell, 4), :]
                zs2[w * 4 + r, pl.ds(PAD + cell, 4), :] = jnp.where(
                    index4 + cell < ends[r], zh[w, pl.ds(take, 4), :], old
                )
    for r in range(rows_dev):
        terms = column_terms(r)
        c_left[pl.ds(r, 1), :] = terms[0:1]
        c_right[pl.ds(r, 1), :] = terms[GLON_DEV + 1 : GLON_DEV + 2]
        for g in range(GLON_DEV):
            co_ref[g, pl.ds(r, 1), :] = terms[g + 1 : g + 2]

    @pl.when(has_left)
    def _():
        part_left.start()

    @pl.when(has_right)
    def _():
        part_right.start()

    merid_begin(first_partials)
    serve(2, at_south)
    serve(3, lat > 0)
    ready_poles(is_hub & at_south)
    over_poles(is_hub & at_south)

    serve(3, at_south)

    for src, dst in ((ms2, ms1), (ms1, ms2)):
        advance(src, dst, ms, products, weights, cells, rows_dev, None, final=dst is ms2)
    transfers(128, MERID).wait_recv()

    for r in range(rows_dev):
        take = (r % 2) * 4
        for ch in range(4):
            turned = ch if ch == 3 else 2 - ch
            sign = -1.0 if ch == 3 else 1.0
            base = PAD + r * 24
            for j in range(4):
                plain = m_halo[0, r // 2, ch, pl.ds(take + j, 1), :]
                pole = sign * m_halo[0, r // 2, turned, pl.ds(take + 3 - j, 1), :]
                fh[ch, pl.ds(base + j, 1), :] = jnp.where(at_south, pole, plain)
                plain = m_halo[1, r // 2, ch, pl.ds(take + j, 1), :]
                pole = sign * m_halo[1, r // 2, turned, pl.ds(take + 3 - j, 1), :]
                fh[ch, pl.ds(base + 20 + j, 1), :] = jnp.where(at_north, pole, plain)
            fh[ch, pl.ds(base + 4, 8), :] = ms[ch * 4 + r, pl.ds(PAD, 8), :]
            fh[ch, pl.ds(base + 12, 8), :] = ms[ch * 4 + r, pl.ds(PAD + cells - 8, 8), :]

    advance_strips(fh, fh1, products, weights, 24 * rows_dev, 48)
    for r in range(rows_dev):
        for w in range(3):
            at, base = w * 4 + r, PAD + r * 24
            ms2[at, pl.ds(PAD, 4), :] = fh[w, pl.ds(base + 4, 4), :]
            ms2[at, pl.ds(PAD + cells - 4, 4), :] = fh[w, pl.ds(base + 16, 4), :]

    @pl.when(plain_far)
    def _():
        transfers(32, HEAD).wait_recv()

    @pl.when(ends_here)
    def _():
        transfers(64, HEAD).wait_recv()

    beside((rows_dev - 2) * 40, WINDOW, far_left, far_right)

    @pl.when(is_hub)
    def _():
        transfers(all_tails, TAIL).wait_recv()

    own_base = (me * GLON_DEV + 1).astype(F32)
    for r in range(rows_dev):
        end = jnp.where(is_hub, 4, lengths[r] - start)
        seam_room[r, :, :] = jnp.full((8, 128), end, jnp.int32).astype(F32)

    @pl.when(is_hub)
    def _():
        for ch in range(4):
            total = tails_in[wrap_from, ch]
            for j in range(wrap_from + 1, n):
                total = total + tails_in[j, ch]
            fz[ch, pl.ds(PAD, 4), :] = tail_zero[ch, pl.ds(0, 4), :]
            fz[ch, pl.ds(PAD + 12, 4), :] = from_left[0, ch, pl.ds(4, 4), :]
            for r in range(2, rows_dev):
                half = (r % 2) * 4
                fz[ch, pl.ds(PAD + 12 * r, 4), :] = total[half : half + 4]
            for r in range(rows_dev):
                fz[ch, pl.ds(PAD + 12 * r + 4, 8), :] = zs[ch * 4 + r, pl.ds(PAD, 8), :]
        for r in range(rows_dev):
            seam_owner[r, :, :] = zs[16 + r, pl.ds(PAD, 8), :] - own_base

    @pl.when(has_left)
    def _():
        for r in range(rows_dev):
            for ch in range(5):
                window = z_window[r, ch]
                if r >= 2:
                    window = window + jnp.where(far_left, w_left[r - 2, ch], 0.0)
                    window = window + jnp.where(far_right, w_right[r - 2, ch], 0.0)
                if ch == 4:
                    seam_owner[r, pl.ds(0, 4), :] = window[4:8] - own_base
                    continue
                base = PAD + 12 * r
                fz[ch, pl.ds(base, 8), :] = window
                fz[ch, pl.ds(base + 8, 4), :] = heads[r // 2, ch, pl.ds((r % 2) * 4, 4), :]

    beside(8, PART, has_left, has_right)

    @pl.when(has_left)
    def _():
        for r in range(rows_dev):
            co_ref[0, pl.ds(r, 1), :] += c_from_left[pl.ds(r, 1), :]

    @pl.when(has_right)
    def _():
        for r in range(rows_dev):
            co_ref[GLON_DEV - 1, pl.ds(r, 1), :] += c_from_right[pl.ds(r, 1), :]

    moved = (rows_dev - 2) * 40
    transfers(128, MERID).wait_send()
    for flag, count, sem in (
        (far_left, 72 + moved, LEFT),
        (has_left & jnp.logical_not(far_left), 72, LEFT),
        (far_right, 72 + moved, RIGHT),
        (has_right & jnp.logical_not(far_right), 72, RIGHT),
        (plain_far, 32, TAIL),
        (ends_here, 64, TAIL),
        (is_hub, all_tails, HEAD),
    ):

        @pl.when(flag)
        def _():
            transfers(count, sem).wait_send()


def finish(
    cells, rows_dev,
    zs, ms, co_in, fz, seam_owner, seam_room, weights,
    zo_hbm, mo_hbm, co_hbm,
    zo, mo, co, f1, f2, products, sems,
):
    rows = 12 * rows_dev
    index8 = lax.broadcasted_iota(jnp.int32, (8, 128), 0)
    copies = []

    def write(blocks, staged, out, w, sem):
        lines = staged.at[w].reshape(128 * rows_dev, cells)
        for r in range(rows_dev):
            lines[pl.ds(r, 128, stride=rows_dev), :] = blocks(w, r).T
        copies.append(pltpu.make_async_copy(staged.at[w], out.at[:, w], sems.at[sem]))
        copies[-1].start()

    def wanted(strips, r):
        at = pl.ds(PAD + 12 * r + 4, 4)
        return strips[0, at, :] + strips[1, at, :] + strips[2, at, :]

    for buf in (f1, f2):
        for ch in range(3):
            buf[ch, pl.ds(0, PAD), :] = jnp.zeros((PAD, 128), F32)
            buf[ch, pl.ds(PAD + rows, PAD), :] = jnp.zeros((PAD, 128), F32)
    rooms = [jnp.max(seam_room[r]).astype(jnp.int32) for r in range(rows_dev)]
    merid = lambda w, r: ms[w * 4 + r, pl.ds(PAD, cells), :]
    for t, (src, dst) in enumerate(((fz, f1), (f1, f2), (f2, f1), (f1, f2))):
        strips_substep(src, dst, fz, products, weights, rows, 48, t == SUB - 1)
        if t == 0:
            for w in range(3):
                write(merid, mo, mo_hbm, w, w)

    def zonal(w, r):
        parts = []
        for block in range(0, cells, 8):
            ahead = block - rooms[r]
            inside = (index8 + ahead >= -4) & (index8 + ahead < 0)
            take = PAD + 12 * r + 8 + jnp.clip(ahead, -12, 0)
            old = zs[w * 4 + r, pl.ds(PAD + block, 8), :]
            parts.append(jnp.where(inside, f2[w, pl.ds(take, 8), :], old))
        return jnp.concatenate(parts, axis=0)

    for w in range(3):
        write(zonal, zo, zo_hbm, w, 3 + w)
    scale = GLON_DEV / (3.0 * cells)
    for r in range(rows_dev):
        delta = (wanted(f2, r) - wanted(fz, r)) * scale
        owner = seam_owner[r, pl.ds(0, 4), :]
        for g in range(GLON_DEV):
            mine = jnp.where(owner == float(g), delta, 0.0)
            co[g, pl.ds(r, 1), :] = co_in[g, pl.ds(r, 1), :] + jnp.sum(
                mine, axis=0, keepdims=True
            )
    copies.append(pltpu.make_async_copy(co, co_hbm, sems.at[6]))
    copies[-1].start()
    for done in copies:
        done.wait()


def solution(mesh):
    n, n_lat = mesh.shape["lon"], mesh.shape["lat"]

    def shards(
        zonal_state, zonal_courant, zonal_length, zonal_owner, merid_state, merid_courant, mixing
    ):
        nv, lev, wid, rows_dev, cells = zonal_state.shape
        flat = nv * lev * wid * rows_dev
        vmem = pl.BlockSpec(memory_space=pltpu.VMEM)
        hbm = pl.BlockSpec(memory_space=pltpu.HBM)
        shape = jax.ShapeDtypeStruct
        state = (16, cells + 2 * PAD, 128)
        strips = (4, 24 * rows_dev + 2 * PAD, 128)
        seam = (4, 12 * rows_dev + 2 * PAD, 128)
        packet = pltpu.VMEM((2, 4, 8, 128), F32)
        small = pltpu.VMEM((8, 128), F32)
        products = pltpu.VMEM((rows_dev * 3 * cells, 128), F32)
        dma = pltpu.SemaphoreType.DMA
        regular = pltpu.SemaphoreType.REGULAR
        held = pl.pallas_call(
            functools.partial(kernel, n, n_lat, cells, rows_dev),
            out_shape=(
                shape(state, F32), shape(state, F32),
                shape((GLON_DEV, rows_dev, nv * lev), F32),
                shape(seam, F32),
                shape((rows_dev, 8, 128), F32), shape((rows_dev, 8, 128), F32),
                shape((256, 256), jnp.bfloat16),
            ),
            in_specs=[hbm] * 7,
            out_specs=(vmem,) * 7,
            scratch_shapes=[
                pltpu.SMEM((rows_dev,), jnp.int32),
                pltpu.VMEM((nv * lev * wid, 2, rows_dev // 2, cells), F32),
                pltpu.VMEM((lev * rows_dev, cells), F32),
                pltpu.VMEM((rows_dev, cells), jnp.int32),
                pltpu.VMEM((flat, cells), F32),
                pltpu.VMEM((lev * rows_dev, cells), F32),
                pltpu.VMEM((nv * lev, lev), F32),
                pltpu.VMEM((20, *state[1:]), F32), pltpu.VMEM(state, F32),
                pltpu.VMEM(state, F32), pltpu.VMEM(state, F32),
                pltpu.VMEM(strips, F32),
                pltpu.VMEM(strips, F32),
                pltpu.VMEM(strips, F32), pltpu.VMEM(strips, F32),
                products,
                packet, packet, pltpu.VMEM((3, 4, 8, 128), F32), packet, packet,
                packet, packet, packet,
                pltpu.VMEM((n, 4, 8, 128), F32),
                pltpu.VMEM((4, 8, 128), F32),
                pltpu.VMEM((2, 2, 4, 8, 128), F32),
                pltpu.VMEM((rows_dev, 5, 8, 128), F32),
                pltpu.VMEM((rows_dev - 2, 5, 8, 128), F32),
                pltpu.VMEM((rows_dev - 2, 5, 8, 128), F32),
                small, small, small, small,
                dma((8,)), dma((6,)),
                regular((2,)), regular((2,)), regular((4,)),
            ],
            compiler_params=pltpu.CompilerParams(
                collective_id=0, has_side_effects=True, vmem_limit_bytes=48 * 1024 * 1024
            ),
        )(
            *(
                pltpu.with_memory_space_constraint(value, pltpu.HBM)
                for value in (
                    zonal_length,
                    zonal_state.reshape(nv * lev * wid, 2, rows_dev // 2, cells),
                    zonal_courant.reshape(lev * rows_dev, cells),
                    zonal_owner,
                    merid_state.reshape(flat, cells),
                    merid_courant.reshape(lev * rows_dev, cells),
                    mixing.reshape(nv * lev, lev),
                )
            )
        )
        zo, mo, co = pl.pallas_call(
            functools.partial(finish, cells, rows_dev),
            out_shape=(
                shape((nv * lev, wid, rows_dev, cells), F32),
                shape((nv * lev, wid, rows_dev, cells), F32),
                shape((GLON_DEV, rows_dev, nv * lev), F32),
            ),
            in_specs=[vmem] * 7,
            out_specs=(hbm,) * 3,
            scratch_shapes=[
                pltpu.VMEM((wid, nv * lev, rows_dev, cells), F32),
                pltpu.VMEM((wid, nv * lev, rows_dev, cells), F32),
                pltpu.VMEM((GLON_DEV, rows_dev, nv * lev), F32),
                pltpu.VMEM(seam, F32), pltpu.VMEM(seam, F32), products, dma((7,)),
            ],
            compiler_params=pltpu.CompilerParams(vmem_limit_bytes=40 * 1024 * 1024),
        )(*held)
        return zo.reshape(zonal_state.shape), mo.reshape(merid_state.shape), co

    return jax.shard_map(
        shards,
        mesh=mesh,
        in_specs=(
            P(None, None, None, "lat", "lon"),
            P(None, "lat", "lon"),
            P("lat"),
            P("lat", "lon"),
            P(None, None, None, "lon", "lat"),
            P(None, "lon", "lat"),
            P(),
        ),
        out_specs=(
            P(None, None, None, "lat", "lon"),
            P(None, None, None, "lon", "lat"),
            P("lon", "lat", None),
        ),
        check_vma=False,
    )
```
